256 devices in a mesh: tile: 32 (over z_lo, y, core), img: 8 (over x, z_hi).
Axes of the slice: x: 4, y: 4, z: 8 (z_hi: 2, z_lo: 4; z = z_hi * 4 + z_lo), core: 2. Of those that a mesh axis runs over, the one named last changes fastest.
Arguments:
- tower: bfloat16 [8, 64, 128, 256], P('img', 'tile'), may hold values from -6 to 6
- cls_weight: bfloat16 [720, 2304], replicated, may hold values from -0.125 to 0.125
- cls_bias: float32 [720], replicated, may hold values from -5.5 to -3.5
- box_weight: bfloat16 [36, 2304], replicated, may hold values from -0.125 to 0.125
- box_bias: float32 [36], replicated, may hold values from -0.5 to 0.5
- labels: int32 [8, 9, 64, 128], P('img', None, 'tile'), may hold values from -2 to 79, as said below
- target_index: int32 [8, 9, 64, 128], P('img', None, 'tile'), may hold values from 0 to 99
- boxes: float32 [8, 4, 100], P('img'), may hold values from -320 to 1344, as said below
Outputs:
- loss: float32 [], replicated
- cls_weight_grad: float32 [720, 2304], replicated
- cls_bias_grad: float32 [720], replicated
- box_weight_grad: float32 [36, 2304], replicated
- box_bias_grad: float32 [36], replicated
- tower_grad: bfloat16 [8, 64, 128, 256], P('img', 'tile')
The draws below stay inside these ranges and needn't reach their ends.
Inputs may be any that keep to these rules, and one draw needn't show every extreme that they name: `labels`: -1 marks background and -2 an ignored anchor, other values are classes; every image has at least one anchor with a class. `boxes`: x1 < x2 and y1 < y2 in every box; sides between 8 and 640 pixels.
All inputs are finite; a program needn't handle non-finite values.
Results may differ from the reference program's by a relative error of at most 0.0053.
Values may be sent and summed in bfloat16 or wider, within the bound.
No kernel may reach another device: no remote copies, remote signals or barrier semaphores. Data moves between devices by JAX's collectives and lax.ppermute only.
A program may use at most 64 MiB of HBM per device.

```python
import jax
import jax.numpy as jnp
from jax import lax

CHANNELS = 256
CLASSES = 80
ANCHORS = 9
STRIDE = 8
COLUMNS = 128
MAX_BOXES = 100
ROWS = 64
IMAGES = 8


def draw_labels(key, part):
    dims = (IMAGES, ANCHORS, ROWS, COLUMNS)
    key_pick = jax.random.fold_in(key, 11)
    key_class = jax.random.fold_in(key, 12)
    rolled = jax.random.randint(key_pick, dims, 0, 1000)
    row_ids = lax.broadcasted_iota(jnp.int32, dims, 2)
    col_ids = lax.broadcasted_iota(jnp.int32, dims, 3)
    anchor_ids = lax.broadcasted_iota(jnp.int32, dims, 1)
    positive_limit = 30 + 60 * row_ids // ROWS
    ignore_limit = positive_limit + 50
    classes = jax.random.randint(key_class, dims, 0, CLASSES)
    labels = jnp.where(rolled < positive_limit, classes, jnp.where(rolled < ignore_limit, -2, -1))
    forced = (anchor_ids == 0) & (row_ids == 0) & (col_ids == 0)
    return jnp.where(forced, classes, labels).astype(jnp.int32)


def draw_boxes(key, part):
    dims = (IMAGES, MAX_BOXES)
    centre_x = jax.random.uniform(jax.random.fold_in(key, 21), dims, jnp.float32, 0.0, COLUMNS * STRIDE * 1.0)
    centre_y = jax.random.uniform(jax.random.fold_in(key, 22), dims, jnp.float32, 0.0, ROWS * STRIDE * 1.0)
    widths = jnp.exp(jax.random.uniform(jax.random.fold_in(key, 23), dims, jnp.float32, jnp.log(16.0), jnp.log(512.0)))
    heights = jnp.exp(jax.random.uniform(jax.random.fold_in(key, 24), dims, jnp.float32, jnp.log(16.0), jnp.log(512.0)))
    corners = jnp.stack([centre_x - 0.5 * widths, centre_y - 0.5 * heights, centre_x + 0.5 * widths, centre_y + 0.5 * heights], axis=1)
    return corners.astype(jnp.float32)


def place_ends(result, stream_key, smallest, high):
    place = [jax.random.randint(jax.random.fold_in(stream_key, axis), (), 0, length) for axis, length in enumerate(result.shape)]
    widest = result.shape.index(max(result.shape))
    next_to = place[:widest] + [(place[widest] + 1) % result.shape[widest]] + place[widest + 1:]
    return result.at[tuple(place)].set(smallest).at[tuple(next_to)].set(high)


def levels(rng, shape, shards, smallest, high):
    loudness, own = 1.0, jax.random.fold_in(rng, 6)
    for position, blocks in shards:
        steps = jnp.exp(jax.random.uniform(jax.random.fold_in(own, position), (blocks,), jnp.float32, smallest / len(shards), high / len(shards)))
        loudness = loudness * jnp.repeat(steps, shape[position] // blocks).reshape([-1 if axis == position else 1 for axis in range(len(shape))])
    return loudness


def noise(rng, shape, spread, most, split=(), dtype=jnp.bfloat16):
    loudness = levels(rng, shape, split, -0.22, 0.18) if split else 1.0
    values = jax.random.normal(rng, shape, jnp.float32) * spread * loudness
    return jnp.minimum(jnp.maximum(values, -most), most).astype(dtype)


def setup_inputs(seed: int = 0) -> dict:
    arg_keys = jax.random.split(jax.random.key(seed), 9)
    return {
        "tower": noise(arg_keys[0], (IMAGES, ROWS, COLUMNS, CHANNELS), 1.0, 6.0, ((0, 8), (1, 32))),
        "cls_weight": noise(arg_keys[1], (ANCHORS * CLASSES, 9 * CHANNELS), (9 * CHANNELS) ** -0.5, 0.125),
        "cls_bias": jnp.clip(jax.random.uniform(arg_keys[2], (ANCHORS * CLASSES,), jnp.float32, -5.5, -3.5), -5.5, -3.5),
        "box_weight": noise(arg_keys[3], (ANCHORS * 4, 9 * CHANNELS), (9 * CHANNELS) ** -0.5, 0.125),
        "box_bias": jnp.clip(jax.random.uniform(arg_keys[4], (ANCHORS * 4,), jnp.float32, -0.5, 0.5), -0.5, 0.5),
        "labels": draw_labels(jax.random.fold_in(arg_keys[8], 71), 0),
        "target_index": place_ends(jax.random.randint(arg_keys[6], (IMAGES, ANCHORS, ROWS, COLUMNS), 0, MAX_BOXES), jax.random.fold_in(arg_keys[6], 1), 0, MAX_BOXES - 1).astype(jnp.int32),
        "boxes": draw_boxes(jax.random.fold_in(arg_keys[8], 71), 0),
    }


FOCAL_ALPHA = 0.25
NORM_EPS = 1e-06

def build_patches(extended):
    rows_here = extended.shape[1] - 2
    columns = extended.shape[2]
    padded = jnp.pad(extended, ((0, 0), (0, 0), (1, 1), (0, 0)))
    pieces = []
    for row_tap in range(3):
        for col_tap in range(3):
            pieces.append(padded[:, row_tap:row_tap + rows_here, col_tap:col_tap + columns, :])
    return jnp.concatenate(pieces, axis=3)

def taps_back(dpatch, rows_lo, rows_out):
    images_here, rows_in, columns, width_all = dpatch.shape
    channels = width_all // 9
    pieces = dpatch.reshape(images_here, rows_in, columns, 9, channels)
    accumulated = jnp.zeros((images_here, rows_in + 2, columns + 2, channels), jnp.float32)
    for row_tap in range(3):
        for col_tap in range(3):
            accumulated = accumulated.at[:, row_tap:row_tap + rows_in, col_tap:col_tap + columns, :].add(pieces[:, :, :, row_tap * 3 + col_tap, :])
    return accumulated[:, rows_lo:rows_lo + rows_out, 1:columns + 1, :]

def head_terms(logits, deltas, labels, target_index, boxes, first_row):
    images_here = labels.shape[0]
    rows_here = labels.shape[2]
    columns = labels.shape[3]
    scores = logits.reshape(ANCHORS, CLASSES, images_here, rows_here, columns)
    assigned = jnp.transpose(labels, (1, 0, 2, 3))
    classes = lax.broadcasted_iota(jnp.int32, (1, CLASSES, 1, 1, 1), 1)
    target = (assigned[:, None] == classes).astype(jnp.float32)
    counted = (assigned >= -1).astype(jnp.float32)[:, None]
    probability = jax.nn.sigmoid(scores)
    hit_term = -FOCAL_ALPHA * (1.0 - probability) * (1.0 - probability) * jax.nn.log_sigmoid(scores)
    miss_term = -(1.0 - FOCAL_ALPHA) * probability * probability * jax.nn.log_sigmoid(-scores)
    focal_sum = jnp.sum(counted * (target * hit_term + (1.0 - target) * miss_term))
    offsets = deltas.reshape(ANCHORS, 4, images_here, rows_here, columns)
    anchor_ids = lax.broadcasted_iota(jnp.int32, (ANCHORS, 1, 1, 1), 0)
    scale_step = (anchor_ids // 3).astype(jnp.float32)
    ratio_step = (anchor_ids % 3 - 1).astype(jnp.float32)
    anchor_base = 4.0 * STRIDE * jnp.exp2(scale_step / 3.0)
    anchor_w = anchor_base * jnp.exp2(-ratio_step / 2.0)
    anchor_h = anchor_base * jnp.exp2(ratio_step / 2.0)
    row_ids = first_row + lax.broadcasted_iota(jnp.int32, (1, 1, rows_here, 1), 2)
    col_ids = lax.broadcasted_iota(jnp.int32, (1, 1, 1, columns), 3)
    centre_y = (row_ids.astype(jnp.float32) + 0.5) * STRIDE
    centre_x = (col_ids.astype(jnp.float32) + 0.5) * STRIDE
    middle_x = centre_x + offsets[:, 0] * anchor_w
    middle_y = centre_y + offsets[:, 1] * anchor_h
    pred_width = anchor_w * jnp.exp(offsets[:, 2])
    pred_height = anchor_h * jnp.exp(offsets[:, 3])
    pred_left = middle_x - 0.5 * pred_width
    pred_right = middle_x + 0.5 * pred_width
    pred_top = middle_y - 0.5 * pred_height
    pred_bottom = middle_y + 0.5 * pred_height
    flat_index = target_index.reshape(images_here, -1)
    picked = jnp.take_along_axis(boxes, jnp.broadcast_to(flat_index[:, None, :], (images_here, 4, flat_index.shape[1])), axis=2)
    picked = jnp.transpose(picked.reshape(images_here, 4, ANCHORS, rows_here, columns), (1, 2, 0, 3, 4))
    true_left, true_top, true_right, true_bottom = (picked[0], picked[1], picked[2], picked[3])
    crossing_w = jnp.maximum(jnp.minimum(pred_right, true_right) - jnp.maximum(pred_left, true_left), 0.0)
    crossing_h = jnp.maximum(jnp.minimum(pred_bottom, true_bottom) - jnp.maximum(pred_top, true_top), 0.0)
    crossing = crossing_w * crossing_h
    union_area = pred_width * pred_height + (true_right - true_left) * (true_bottom - true_top) - crossing
    outer_w = jnp.maximum(pred_right, true_right) - jnp.minimum(pred_left, true_left)
    outer_h = jnp.maximum(pred_bottom, true_bottom) - jnp.minimum(pred_top, true_top)
    outer_area = outer_w * outer_h
    giou_value = crossing / union_area - (outer_area - union_area) / outer_area
    positive = (assigned >= 0).astype(jnp.float32)
    giou_sum = jnp.sum(positive * (1.0 - giou_value))
    return (focal_sum, giou_sum)

def reference(tower, cls_weight, cls_bias, box_weight, box_bias, labels, target_index, boxes):
    weight_all = jnp.concatenate([cls_weight, box_weight], axis=0)
    bias_all = jnp.concatenate([cls_bias, box_bias])
    split_at = cls_weight.shape[0]

    def one_image(carry, inputs):
        weight_sum, bias_sum, focal_total, giou_total, positives = carry
        image, image_labels, image_index, image_boxes = inputs
        extended = jnp.pad(image[None], ((0, 0), (1, 1), (0, 0), (0, 0)))
        patches = build_patches(extended)
        flat_patches = patches.reshape(-1, patches.shape[3])
        outputs = lax.dot_general(weight_all, flat_patches, (((1,), (1,)), ((), ())), preferred_element_type=jnp.float32)
        outputs = (outputs + bias_all[:, None]).reshape(weight_all.shape[0], 1, ROWS, COLUMNS)

        def loss_pair(scores, offsets):
            return head_terms(scores, offsets, image_labels[None], image_index[None], image_boxes[None], 0)
        loss_terms, pullback = jax.vjp(loss_pair, outputs[:split_at], outputs[split_at:])
        grad_scores, grad_offsets = pullback((jnp.ones((), jnp.float32), jnp.ones((), jnp.float32)))
        grad_out = jnp.concatenate([grad_scores, grad_offsets], axis=0)
        grad_low = grad_out.astype(jnp.bfloat16)
        grad_flat = grad_low.reshape(grad_low.shape[0], -1)
        weight_sum = weight_sum + jnp.dot(grad_flat, flat_patches, preferred_element_type=jnp.float32)
        bias_sum = bias_sum + lax.optimization_barrier(jnp.sum(grad_out, axis=(1, 2, 3)))
        dpatch = lax.dot_general(grad_flat, weight_all, (((0,), (0,)), ((), ())), preferred_element_type=jnp.float32)
        dpatch = dpatch.reshape(1, ROWS, COLUMNS, weight_all.shape[1])
        image_grad = taps_back(dpatch, 1, ROWS)[0].astype(jnp.bfloat16)
        positives = positives + jnp.sum((image_labels >= 0).astype(jnp.float32))
        focal_total = focal_total + loss_terms[0]
        giou_total = giou_total + loss_terms[1]
        return ((weight_sum, bias_sum, focal_total, giou_total, positives), image_grad)
    initial = (jnp.zeros(weight_all.shape, jnp.float32), jnp.zeros(bias_all.shape, jnp.float32), jnp.zeros((), jnp.float32), jnp.zeros((), jnp.float32), jnp.zeros((), jnp.float32))
    finals, tower_grad = lax.scan(one_image, initial, (tower, labels, target_index, boxes))
    weight_sum, bias_sum, focal_total, giou_total, positives = finals
    loss = (focal_total + giou_total) / positives
    entries = weight_all.shape[0] * (weight_all.shape[1] + 1)
    squares = jnp.sum(weight_sum * weight_sum) + jnp.sum(bias_sum * bias_sum)
    scale = lax.rsqrt(squares / entries + NORM_EPS)
    weight_norm = weight_sum * scale
    bias_norm = bias_sum * scale
    return (loss, weight_norm[:split_at], bias_norm[:split_at], weight_norm[split_at:], bias_norm[split_at:], tower_grad)
```

```python
import jax
import jax.numpy as jnp
from jax import lax
from jax.experimental import pallas as pl
from jax.experimental.pallas import tpu as pltpu
from jax.sharding import Mesh, PartitionSpec as P

CLASSES = 80
ANCHORS = 9
STRIDE = 8
FOCAL_ALPHA = 0.25
NORM_EPS = 1e-06

ROWS_ALL = 768
VALID = 756
HALF = 384
BLOCK = 24
TILES = 56
PIECE = 448

TILE_AXES = ("zlo", "y", "core")
IMG_AXES = ("x", "zhi")

f32 = jnp.float32
bf16 = jnp.bfloat16


def dot(a, b, dims):
    return lax.dot_general(a, b, (dims, ((), ())), preferred_element_type=f32)


def shifted(x, j):
    if j == 1:
        return x
    ids = lax.broadcasted_iota(jnp.int32, x.shape, 0)
    if j == 0:
        return jnp.where(ids == 0, 0.0, pltpu.roll(x, 1, 0))
    return jnp.where(ids == x.shape[0] - 1, 0.0, pltpu.roll(x, x.shape[0] - 1, 0))


def fill_patches(rows, p_ref, base):
    for e, row in enumerate(rows):
        x = row.astype(f32)
        for j in range(3):
            v = shifted(x, j).astype(bf16)
            for i in range(3):
                r = e - i
                if 0 <= r < 2:
                    p_ref[base + r * 128 : base + r * 128 + 128, (3 * i + j) * 256 : (3 * i + j) * 256 + 256] = v


def anchor_sizes(shape):
    ids = lax.broadcasted_iota(jnp.int32, shape, 0)
    w = jnp.ones(shape, f32)
    h = jnp.ones(shape, f32)
    for a in range(ANCHORS):
        base = 4.0 * STRIDE * 2.0 ** ((a // 3) / 3.0)
        ratio = a % 3 - 1
        w = jnp.where(ids == a, base * 2.0 ** (-ratio / 2.0), w)
        h = jnp.where(ids == a, base * 2.0 ** (ratio / 2.0), h)
    return w, h


def giou_terms(o0, o1, o2, o3, aw, ah, cx, cy, tl, tt, tr, tb):
    mx = cx + o0 * aw
    my = cy + o1 * ah
    pw = aw * jnp.exp(o2)
    ph = ah * jnp.exp(o3)
    left = mx - 0.5 * pw
    right = mx + 0.5 * pw
    top = my - 0.5 * ph
    bottom = my + 0.5 * ph
    iw = jnp.maximum(jnp.minimum(right, tr) - jnp.maximum(left, tl), 0.0)
    ih = jnp.maximum(jnp.minimum(bottom, tb) - jnp.maximum(top, tt), 0.0)
    inter = iw * ih
    union = pw * ph + (tr - tl) * (tb - tt) - inter
    ow = jnp.maximum(right, tr) - jnp.minimum(left, tl)
    oh = jnp.maximum(bottom, tb) - jnp.minimum(top, tt)
    outer = ow * oh
    return 1.0 - (inter / union - (outer - union) / outer)


def head_kernel(first, before, own, after, cw, bw, cb, bb, lab, idx, box, g_ref, p_ref, o_ref, b_ref, gb_ref):
    fill_patches([before[0], own[0], own[1], after[0]], p_ref, 0)
    p = p_ref[...]
    o_ref[...] = dot(cw[...], p, ((1,), (1,))) + cb[...]
    small_out = dot(bw[...], p, ((1,), (1,))) + bb[...]
    for r in range(2):
        b_ref[r * 64 : r * 64 + 48, :] = small_out[:, r * 128 : r * 128 + 128]
        b_ref[r * 64 + 48 : r * 64 + 64, :] = jnp.zeros((16, 128), f32)
    cls = lax.broadcasted_iota(jnp.int32, (CLASSES, 128), 0)

    def one_anchor(a, carry):
        sums = []
        at = pl.multiple_of(a * CLASSES, 16)
        for r in range(2):
            label = lab[r, pl.ds(a, 1), :]
            x = o_ref[pl.ds(at, CLASSES), r * 128 : r * 128 + 128]
            hit = label == cls
            z = jnp.where(hit, -x, x)
            e = jnp.exp(-jnp.abs(z))
            soft = jnp.maximum(z, 0.0) + jnp.log1p(e)
            big = 1.0 / (1.0 + e)
            small = e * big
            up = z >= 0.0
            q = jnp.where(up, big, small)
            rest = jnp.where(up, small, big)
            counted = (label >= -1).astype(f32)
            w = jnp.where(hit, FOCAL_ALPHA, 1.0 - FOCAL_ALPHA) * counted
            wq = w * q * q
            dz = wq * (q + 2.0 * rest * soft)
            g_ref[pl.ds(at, CLASSES), r * 128 : r * 128 + 128] = jnp.where(hit, -dz, dz).astype(bf16)
            sums.append(carry[r] + jnp.sum(wq * soft, axis=0, keepdims=True))
        return tuple(sums)

    zero = jnp.zeros((1, 128), f32)
    focal = lax.fori_loop(0, ANCHORS, one_anchor, (zero, zero))

    aw, ah = anchor_sizes((16, 128))
    cx = (lax.broadcasted_iota(jnp.int32, (16, 128), 1).astype(f32) + 0.5) * STRIDE
    live = lax.broadcasted_iota(jnp.int32, (16, 128), 0) < ANCHORS
    for r in range(2):
        cy = (jnp.full((16, 128), first[0] + r, jnp.int32).astype(f32) + 0.5) * STRIDE
        which = idx[r]
        corner = [
            jnp.take_along_axis(jnp.broadcast_to(box[k : k + 1, :], (16, 128)), which, axis=1) for k in range(4)
        ]
        positive = lab[r] >= 0
        o = [b_ref[pl.ds(r * 64 + k, 16, stride=4), :] for k in range(4)]
        value, pull = jax.vjp(
            lambda o0, o1, o2, o3: giou_terms(o0, o1, o2, o3, aw, ah, cx, cy, *corner), *o
        )
        grads = pull(jnp.ones((16, 128), f32))
        for k in range(4):
            gb_ref[pl.ds(r * 64 + k, 16, stride=4), :] = jnp.where(positive, grads[k], 0.0)
        giou = jnp.sum(jnp.where(positive, value, 0.0), axis=0, keepdims=True)
        count = jnp.sum(positive.astype(f32), axis=0, keepdims=True)
        rows = []
        for v in (focal[r], giou):
            hi = v.astype(bf16).astype(f32)
            rows += [hi, v - hi]
        rows.append(count)
        for n, v in enumerate(rows):
            gb_ref[r * 64 + 36 + n : r * 64 + 37 + n, :] = v
        g_ref[720:768, r * 128 : r * 128 + 128] = gb_ref[r * 64 : r * 64 + 48, :].astype(bf16)


def tower_kernel(g, cw, bw, mid, up, down, w_ref, sem):
    copy = pltpu.make_async_copy(cw, w_ref.at[pl.ds(0, 720)], sem)
    copy.start()
    w_ref[720:768, :] = bw[...]
    gt = g[...].astype(f32).T
    gj = []
    for j in range(3):
        gj.append(
            jnp.concatenate([shifted(gt[r * 128 : r * 128 + 128], 2 - j) for r in range(2)], axis=0).astype(bf16)
        )
    copy.wait()
    t = []
    for i in range(3):
        acc = jnp.zeros((256, 256), f32)
        for j in range(3):
            at = (3 * i + j) * 256
            acc = acc + dot(gj[j], w_ref[:, at : at + 256], ((1,), (0,)))
        t.append(acc)
    up[0] = t[0][0:128].astype(bf16)
    mid[0] = t[1][0:128] + t[0][128:256]
    mid[1] = t[1][128:256] + t[2][0:128]
    down[0] = t[2][128:256].astype(bf16)


def weight_kernel(ga, gb, ea, eb, m_ref, p_ref):
    fill_patches([ea[k] for k in range(4)], p_ref, 0)
    fill_patches([eb[k] for k in range(4)], p_ref, 256)
    a = ga[...]
    b = gb[...]
    for tap in range(9):
        at = tap * 256
        acc = dot(a, p_ref[0:256, at : at + 256], ((1,), (0,))) + dot(b, p_ref[256:512, at : at + 256], ((1,), (0,)))
        for m in range(16):
            for rb in range(3):
                row = m * BLOCK + rb * 8
                both = jnp.concatenate([acc[row : row + 8, 0:128], acc[row : row + 8, 128:256]], axis=0)
                v = (rb * 18 + 2 * tap) * 8
                m_ref[m, v : v + 16, :] = both.astype(bf16)
    bias = jnp.sum(a.astype(f32) + b.astype(f32), axis=1, keepdims=True)
    lane = lax.broadcasted_iota(jnp.int32, (8, 128), 1)
    for m in range(16):
        e = jnp.zeros((8, 128), f32)
        for rb in range(3):
            row = m * BLOCK + rb * 8
            e = jnp.where(lane == rb, bias[row : row + 8], e)
        hi = e.astype(bf16).astype(f32)
        m_ref[m, 432:448, :] = jnp.concatenate([hi, e - hi], axis=0).astype(bf16)


def sum_kernel(m_ref, s_ref):
    acc = m_ref[0].astype(f32)
    for m in range(1, 16):
        acc = acc + m_ref[m].astype(f32)
    for z in range(8):
        if z < 7:
            s_ref[z] = acc[z * 56 : z * 56 + 56]
        else:
            s_ref[z, 0:40] = acc[392:432]
            s_ref[z, 40:48] = acc[432:440] + acc[440:448]
            s_ref[z, 48:56] = jnp.zeros((8, 128), f32)


def piece_kernel(zi, s_ref, c_ref):
    acc = s_ref[0]
    for z in range(1, 8):
        acc = acc + s_ref[z]
    e = acc[40:48]
    hi = e.astype(bf16).astype(f32)
    last = jnp.full((8, 128), zi[0], jnp.int32) == 7
    out = jnp.concatenate([acc[0:48], jnp.where(last, e - hi, acc[48:56])], axis=0).astype(bf16)
    for z in range(8):
        c_ref[z] = out


def final_kernel(core, mine, other, cw_out, bw_out, b_out, loss, w_ref, e_ref, sem):
    srow = lax.broadcasted_iota(jnp.int32, (8, 128), 0)
    lane = lax.broadcasted_iota(jnp.int32, (8, 128), 1)
    c = core[0]

    def squares(src, half):
        def one(m, total):
            base = half * HALF + m * BLOCK
            for rb in range(3):
                acc = jnp.zeros((16, 128), f32)
                for k in range(9):
                    v = src[m, (rb * 9 + k) * 16 : (rb * 9 + k) * 16 + 16, :].astype(f32)
                    acc = acc + v * v
                ok = base + rb * 8 + srow < VALID
                total = total + jnp.where(ok, acc[0:8] + acc[8:16], 0.0)
            e = src[m, 432:448, :].astype(f32)
            e = e[0:8] + e[8:16]
            e_ref[half * 16 + m] = e
            ok = (base + lane * 8 + srow < VALID) & (lane < 3)
            return total + jnp.where(ok, e * e, 0.0)

        return one

    total = jnp.zeros((8, 128), f32)
    total = lax.fori_loop(0, 16, squares(mine, c), total)
    total = lax.fori_loop(0, 16, squares(other, 1 - c), total)
    mean = jnp.sum(total) * (1.0 / (VALID * 2305))
    scale = lax.rsqrt(jnp.full((8, 128), mean + NORM_EPS, f32))

    def write(src, half):
        def one(m, carry):
            base = half * HALF + m * BLOCK
            for rb in range(3):
                row = pl.multiple_of(base + rb * 8, 8)
                for k in range(9):
                    v = src[m, (rb * 9 + k) * 16 : (rb * 9 + k) * 16 + 16, :].astype(f32)
                    w_ref[pl.ds(row, 8), k * 256 : k * 256 + 128] = v[0:8] * scale
                    w_ref[pl.ds(row, 8), k * 256 + 128 : k * 256 + 256] = v[8:16] * scale
            b_out[half * 16 + m] = e_ref[half * 16 + m] * scale
            return carry

        return one

    lax.fori_loop(0, 16, write(mine, c), 0)
    lax.fori_loop(0, 16, write(other, 1 - c), 0)
    copy = pltpu.make_async_copy(w_ref.at[pl.ds(0, 720)], cw_out, sem)
    copy.start()
    bw_out[...] = w_ref[720:756, :]
    e = e_ref[31]
    sums = jnp.sum(jnp.where((lane == 1) & (srow >= 4), e, 0.0))
    count = jnp.sum(jnp.where((lane == 2) & (srow == 0), e, 0.0))
    loss[...] = jnp.full((8, 128), sums, f32) / jnp.full((8, 128), count, f32)
    copy.wait()


VMEM = pl.BlockSpec(memory_space=pltpu.VMEM)
SMEM = pl.BlockSpec(memory_space=pltpu.SMEM)
ANY = pl.BlockSpec(memory_space=pl.ANY)


def shape(*dims, dtype=f32):
    return jax.ShapeDtypeStruct(dims, dtype)


def head(first, before, own, after, cw, bw, cb, bb, lab, idx, box):
    return pl.pallas_call(
        head_kernel,
        out_shape=shape(ROWS_ALL, 256, dtype=bf16),
        in_specs=[SMEM] + [VMEM] * 10,
        out_specs=VMEM,
        scratch_shapes=[
            pltpu.VMEM((256, 2304), bf16),
            pltpu.VMEM((720, 256), f32),
            pltpu.VMEM((128, 128), f32),
            pltpu.VMEM((128, 128), f32),
        ],
        name="head",
    )(first, before, own, after, cw, bw, cb, bb, lab, idx, box)


def tower_terms(g, cw, bw):
    return pl.pallas_call(
        tower_kernel,
        out_shape=(
            shape(2, 128, 256),
            shape(1, 128, 256, dtype=bf16),
            shape(1, 128, 256, dtype=bf16),
        ),
        in_specs=[VMEM, ANY, VMEM],
        out_specs=(VMEM, VMEM, VMEM),
        scratch_shapes=[pltpu.VMEM((ROWS_ALL, 2304), bf16), pltpu.SemaphoreType.DMA],
        cost_estimate=pl.CostEstimate(flops=2 * 756 * 2304 * 256, transcendentals=0, bytes_accessed=4500000),
        name="tower_terms",
    )(g, cw, bw)


def weight_terms(ga, gb, ea, eb):
    return pl.pallas_call(
        weight_kernel,
        out_shape=shape(16, PIECE, 128, dtype=bf16),
        in_specs=[VMEM] * 4,
        out_specs=VMEM,
        scratch_shapes=[pltpu.VMEM((512, 2304), bf16)],
        name="weight_terms",
    )(ga, gb, ea, eb)


def block_sum(m):
    return pl.pallas_call(
        sum_kernel, out_shape=shape(8, 56, 128), in_specs=[VMEM], out_specs=VMEM, name="block_sum"
    )(m)


def piece_sum(zi, s):
    return pl.pallas_call(
        piece_kernel,
        out_shape=shape(8, 56, 128, dtype=bf16),
        in_specs=[SMEM, VMEM],
        out_specs=VMEM,
        name="piece_sum",
    )(zi, s)


def finish(core, mine, other):
    return pl.pallas_call(
        final_kernel,
        out_shape=(shape(720, 2304), shape(36, 2304), shape(32, 8, 128), shape(8, 128)),
        in_specs=[SMEM, VMEM, VMEM],
        out_specs=(ANY, VMEM, VMEM, VMEM),
        scratch_shapes=[
            pltpu.VMEM((ROWS_ALL, 2304), f32),
            pltpu.VMEM((32, 8, 128), f32),
            pltpu.SemaphoreType.DMA,
        ],
        name="finish",
    )(core, mine, other)


def swap(value):
    return lax.ppermute(value, "core", [(0, 1), (1, 0)])


def per_device(tower, cls_weight, cls_bias, box_weight, box_bias, labels, target_index, boxes):
    own = tower[0]
    tiles = 32
    up = [(t, t + 1) for t in range(tiles - 1)]
    down = [(t + 1, t) for t in range(tiles - 1)]
    before = lax.ppermute(own[1:2], TILE_AXES, up)
    after = lax.ppermute(own[0:1], TILE_AXES, down)
    core = lax.axis_index("core")
    tile = lax.axis_index(TILE_AXES)
    zi = lax.axis_index("zhi") * 4 + lax.axis_index("zlo")
    first = (tile * 2).reshape(1)
    bw = jnp.pad(box_weight, ((0, 12), (0, 0)))
    cb = cls_bias.reshape(720, 1)
    bb = jnp.pad(box_bias, (0, 12)).reshape(48, 1)
    lab = jnp.pad(jnp.transpose(labels[0], (1, 0, 2)), ((0, 0), (0, 7), (0, 0)), constant_values=-2)
    idx = jnp.pad(jnp.transpose(target_index[0], (1, 0, 2)), ((0, 0), (0, 7), (0, 0)))
    box = jnp.pad(boxes[0], ((0, 4), (0, 28)))
    g = head(first, before, own, after, cls_weight, bw, cb, bb, lab, idx, box)

    ext = jnp.concatenate([before, own, after], axis=0)
    ext_other = swap(ext)
    keep = lax.dynamic_slice_in_dim(g, core * HALF, HALF, axis=0)
    send = lax.dynamic_slice_in_dim(g, (1 - core) * HALF, HALF, axis=0)
    g_other = swap(send)

    mid, to_up, to_down = tower_terms(g, cls_weight, bw)
    from_down = lax.ppermute(to_up, TILE_AXES, down)
    from_up = lax.ppermute(to_down, TILE_AXES, up)
    tower_grad = jnp.concatenate(
        [mid[0:1] + from_up.astype(f32), mid[1:2] + from_down.astype(f32)], axis=0
    ).astype(bf16)[None]

    blocks = weight_terms(keep, g_other, ext, ext_other)
    blocks = lax.all_to_all(blocks, ("y", "x"), 0, 0, tiled=True)
    pieces = lax.all_to_all(block_sum(blocks), ("zhi", "zlo"), 0, 0, tiled=True)
    copies = lax.all_to_all(piece_sum(zi.reshape(1), pieces), ("zhi", "zlo"), 0, 0, tiled=True)
    block = copies.reshape(PIECE, 128)
    mine = lax.all_to_all(jnp.broadcast_to(block[None], (16, PIECE, 128)), ("y", "x"), 0, 0, tiled=True)
    other = swap(mine)
    cw_grad, bw_grad, bias, loss = finish(core.reshape(1), mine, other)
    bias = jnp.transpose(bias[:, :, :3], (0, 2, 1)).reshape(ROWS_ALL)
    return loss[0, 0], cw_grad, bias[:720], bw_grad, bias[720:VALID], tower_grad


def solution(mesh):
    fine = Mesh(mesh.devices.reshape(4, 4, 2, 4, 2), ("zlo", "y", "core", "x", "zhi"))
    placed = (
        P(IMG_AXES, TILE_AXES, None, None),
        P(),
        P(),
        P(),
        P(),
        P(IMG_AXES, None, TILE_AXES, None),
        P(IMG_AXES, None, TILE_AXES, None),
        P(IMG_AXES, None, None),
    )
    return jax.shard_map(
        per_device,
        mesh=fine,
        in_specs=placed,
        out_specs=(P(), P(), P(), P(), P(), P(IMG_AXES, TILE_AXES, None, None)),
        check_vma=False,
    )
```

```python
import jax
import jax.numpy as jnp
from jax import lax
from jax.experimental import pallas as pl
from jax.experimental.pallas import tpu as pltpu
from jax.sharding import Mesh, PartitionSpec as P

CLASSES = 80
ANCHORS = 9
STRIDE = 8
FOCAL_ALPHA = 0.25
NORM_EPS = 1e-06

ROWS_ALL = 768
VALID = 756
HALF = 384
GROUP_ROWS = 96
BLOCK = 24
TILES = 56
PIECE = 448

TILE_AXES = ("zlo", "y", "core")
IMG_AXES = ("x", "zhi")

f32 = jnp.float32
bf16 = jnp.bfloat16


def dot(a, b, dims):
    return lax.dot_general(a, b, (dims, ((), ())), preferred_element_type=f32)


def shifted(x, j):
    if j == 1:
        return x
    ids = lax.broadcasted_iota(jnp.int32, x.shape, 0)
    if j == 0:
        return jnp.where(ids == 0, 0.0, pltpu.roll(x, 1, 0))
    return jnp.where(ids == x.shape[0] - 1, 0.0, pltpu.roll(x, x.shape[0] - 1, 0))


def fill_patches(rows, p_ref, base):
    for e, row in enumerate(rows):
        x = row.astype(f32)
        for j in range(3):
            v = shifted(x, j).astype(bf16)
            for i in range(3):
                r = e - i
                if 0 <= r < 2:
                    p_ref[base + r * 128 : base + r * 128 + 128, (3 * i + j) * 256 : (3 * i + j) * 256 + 256] = v


def anchor_sizes(shape):
    ids = lax.broadcasted_iota(jnp.int32, shape, 0)
    w = jnp.ones(shape, f32)
    h = jnp.ones(shape, f32)
    for a in range(ANCHORS):
        base = 4.0 * STRIDE * 2.0 ** ((a // 3) / 3.0)
        ratio = a % 3 - 1
        w = jnp.where(ids == a, base * 2.0 ** (-ratio / 2.0), w)
        h = jnp.where(ids == a, base * 2.0 ** (ratio / 2.0), h)
    return w, h


def giou_terms(o0, o1, o2, o3, aw, ah, cx, cy, tl, tt, tr, tb):
    mx = cx + o0 * aw
    my = cy + o1 * ah
    pw = aw * jnp.exp(o2)
    ph = ah * jnp.exp(o3)
    left = mx - 0.5 * pw
    right = mx + 0.5 * pw
    top = my - 0.5 * ph
    bottom = my + 0.5 * ph
    iw = jnp.maximum(jnp.minimum(right, tr) - jnp.maximum(left, tl), 0.0)
    ih = jnp.maximum(jnp.minimum(bottom, tb) - jnp.maximum(top, tt), 0.0)
    inter = iw * ih
    union = pw * ph + (tr - tl) * (tb - tt) - inter
    ow = jnp.maximum(right, tr) - jnp.minimum(left, tl)
    oh = jnp.maximum(bottom, tb) - jnp.minimum(top, tt)
    outer = ow * oh
    return 1.0 - (inter / union - (outer - union) / outer)


def head_kernel(first, yi, ci, before, own, after, cw, bw, cb, bb, lab, idx, box, *refs):
    g_out = refs[0]
    blocks = refs[1:9]
    p_ref, o_ref, b_ref, gb_ref, g_ref, row_ref, box_ref, lab_ref, idx_ref = refs[9:]
    fill_patches([before[0], own[0], own[1], after[0]], p_ref, 0)
    row_ref[0:1, 0:720] = cb[...]
    row_ref[8:9, 0:36] = bb[...]
    column = row_ref[0:8, :].T[:, 0:1]
    box_column = row_ref[8:16, 0:128].T[:, 0:1]
    box_ref[0:4, 0:100] = box[...]
    lab_ref[...] = jnp.full((32, 128), -2, jnp.int32)
    idx_ref[...] = jnp.zeros((32, 128), jnp.int32)
    for r in range(2):
        for a in range(ANCHORS):
            lab_ref[r * 16 + a : r * 16 + a + 1, :] = lab[a, r : r + 1, :]
            idx_ref[r * 16 + a : r * 16 + a + 1, :] = idx[a, r : r + 1, :]
    p = p_ref[...]
    o_ref[...] = dot(cw[...], p, ((1,), (1,))) + column[0:720]
    small_out = dot(bw[...], p, ((1,), (1,))) + box_column[0:36]
    for r in range(2):
        b_ref[r * 64 + 32 : r * 64 + 64, :] = jnp.zeros((32, 128), f32)
        b_ref[r * 64 : r * 64 + 36, :] = small_out[:, r * 128 : r * 128 + 128]
    cls = lax.broadcasted_iota(jnp.int32, (CLASSES, 128), 0)

    def one_anchor(a, carry):
        sums = []
        at = pl.multiple_of(a * CLASSES, 16)
        for r in range(2):
            label = lab_ref[pl.ds(r * 16 + a, 1), :]
            x = o_ref[pl.ds(at, CLASSES), r * 128 : r * 128 + 128]
            hit = label == cls
            z = jnp.where(hit, -x, x)
            e = jnp.exp(-jnp.abs(z))
            soft = jnp.maximum(z, 0.0) + jnp.log1p(e)
            big = 1.0 / (1.0 + e)
            small = e * big
            up = z >= 0.0
            q = jnp.where(up, big, small)
            rest = jnp.where(up, small, big)
            counted = (label >= -1).astype(f32)
            w = jnp.where(hit, FOCAL_ALPHA, 1.0 - FOCAL_ALPHA) * counted
            wq = w * q * q
            dz = wq * (q + 2.0 * rest * soft)
            g_ref[pl.ds(at, CLASSES), r * 128 : r * 128 + 128] = jnp.where(hit, -dz, dz).astype(bf16)
            sums.append(carry[r] + jnp.sum(wq * soft, axis=0, keepdims=True))
        return tuple(sums)

    zero = jnp.zeros((1, 128), f32)
    focal = lax.fori_loop(0, ANCHORS, one_anchor, (zero, zero))

    aw, ah = anchor_sizes((16, 128))
    cx = (lax.broadcasted_iota(jnp.int32, (16, 128), 1).astype(f32) + 0.5) * STRIDE
    for r in range(2):
        cy = (jnp.full((16, 128), first[0] + r, jnp.int32).astype(f32) + 0.5) * STRIDE
        which = idx_ref[r * 16 : r * 16 + 16, :]
        corner = [
            jnp.take_along_axis(jnp.broadcast_to(box_ref[k : k + 1, :], (16, 128)), which, axis=1) for k in range(4)
        ]
        positive = lab_ref[r * 16 : r * 16 + 16, :] >= 0
        o = [b_ref[pl.ds(r * 64 + k, 16, stride=4), :] for k in range(4)]
        value, pull = jax.vjp(
            lambda o0, o1, o2, o3: giou_terms(o0, o1, o2, o3, aw, ah, cx, cy, *corner), *o
        )
        grads = pull(jnp.ones((16, 128), f32))
        for k in range(4):
            gb_ref[pl.ds(r * 64 + k, 16, stride=4), :] = jnp.where(positive, grads[k], 0.0)
        giou = jnp.sum(jnp.where(positive, value, 0.0), axis=0, keepdims=True)
        count = jnp.sum(positive.astype(f32), axis=0, keepdims=True)
        rows = []
        for v in (focal[r], giou):
            hi = v.astype(bf16).astype(f32)
            rows += [hi, v - hi]
        rows.append(count)
        for n, v in enumerate(rows):
            gb_ref[r * 64 + 36 + n : r * 64 + 37 + n, :] = v
        g_ref[720:768, r * 128 : r * 128 + 128] = gb_ref[r * 64 : r * 64 + 48, :].astype(bf16)
    g_out[...] = g_ref[...]
    for k in range(4):
        y = (yi[0] + k) & 3
        for other in range(2):
            c = ci[0] if other == 0 else 1 - ci[0]
            at = pl.multiple_of(c * HALF + y * GROUP_ROWS, 16)
            blocks[other * 4 + k][...] = g_ref[pl.ds(at, GROUP_ROWS), :]


def tower_kernel(g, cw, bw, mid, up, down, w_ref, sem):
    copy = pltpu.make_async_copy(cw, w_ref.at[pl.ds(0, 720)], sem)
    copy.start()
    w_ref[752:768, :] = jnp.zeros((16, 2304), bf16)
    w_ref[720:756, :] = bw[...]
    gt = g[...].astype(f32).T
    gj = []
    for j in range(3):
        gj.append(
            jnp.concatenate([shifted(gt[r * 128 : r * 128 + 128], 2 - j) for r in range(2)], axis=0).astype(bf16)
        )
    copy.wait()
    t = []
    for i in range(3):
        acc = jnp.zeros((256, 256), f32)
        for j in range(3):
            at = (3 * i + j) * 256
            acc = acc + dot(gj[j], w_ref[:, at : at + 256], ((1,), (0,)))
        t.append(acc)
    up[0] = t[0][0:128].astype(bf16)
    mid[0] = t[1][0:128] + t[0][128:256]
    mid[1] = t[1][128:256] + t[2][0:128]
    down[0] = t[2][128:256].astype(bf16)


def tower_end_kernel(mid, above, below, t_ref):
    t_ref[0, 0] = (mid[0] + above[0].astype(f32)).astype(bf16)
    t_ref[0, 1] = (mid[1] + below[0].astype(f32)).astype(bf16)


def weight_kernel(yi, ci, *refs):
    g = refs[0:8]
    near = refs[8:12]
    far = refs[12:16]
    m_ref, t_ref, s_ref, g_ref = refs[17:]

    def place(row, k, c):
        y = (yi[0] - k) & 3
        t_ref[1 + y * 4 + c * 2] = row(0)
        t_ref[2 + y * 4 + c * 2] = row(1)

        @pl.when((y == 0) & (c == 0))
        def _():
            t_ref[0] = row(2)

        @pl.when((y == 3) & (c == 1))
        def _():
            t_ref[17] = row(2)

    for k in range(4):
        place(lambda r, k=k: near[k][r], k, ci[0])
        place(lambda r, k=k: far[k][r], k, 1 - ci[0])
        y = (yi[0] - k) & 3
        g_ref[y * 2 + ci[0]] = g[k][...]
        g_ref[y * 2 + 1 - ci[0]] = g[4 + k][...]

    def shift(row, carry):
        x = t_ref[row].astype(f32)
        at = pl.multiple_of(row * 128, 128)
        for j in range(3):
            s_ref[j, pl.ds(at, 128), :] = shifted(x, j).astype(bf16)
        return carry

    lax.fori_loop(0, 18, shift, 0)
    lhs = jnp.concatenate([g_ref[n] for n in range(8)], axis=1)
    for tap in range(9):
        i, j = divmod(tap, 3)
        acc = dot(lhs, s_ref[j, i * 128 : i * 128 + 2048, :], ((1,), (0,)))
        for m in range(4):
            for rb in range(3):
                row = m * BLOCK + rb * 8
                both = jnp.concatenate([acc[row : row + 8, 0:128], acc[row : row + 8, 128:256]], axis=0)
                v = (rb * 18 + 2 * tap) * 8
                m_ref[m, v : v + 16, :] = both.astype(bf16)
    bias = dot(jnp.ones((8, 2048), bf16), lhs, ((1,), (1,)))
    bias = jnp.concatenate([bias, jnp.zeros((8, 32), f32)], axis=1)
    for m in range(4):
        e = bias if m == 0 else pltpu.roll(bias, 128 - m * BLOCK, 1)
        hi = e.astype(bf16).astype(f32)
        m_ref[m, 432:448, :] = jnp.concatenate([hi, e - hi], axis=0).astype(bf16)


def sum_kernel(zi, m_ref, unused, c_ref):
    acc = m_ref[0].astype(f32)
    for m in range(1, 32):
        acc = acc + m_ref[m].astype(f32)
    last = jnp.full((8, 128), zi[0], jnp.int32) == 7
    e = acc[40:48] + acc[48:56]
    hi = e.astype(bf16).astype(f32)
    out = jnp.concatenate(
        [acc[0:40], jnp.where(last, hi, acc[40:48]), jnp.where(last, e - hi, acc[48:56])], axis=0
    ).astype(bf16)
    for z in range(8):
        c_ref[z] = out


def final_kernel(core, mine, other, cw_out, bw_out, cb_out, bb_out, loss, w_ref, e_ref, row_ref, sem):
    srow = lax.broadcasted_iota(jnp.int32, (8, 128), 0)
    lane = lax.broadcasted_iota(jnp.int32, (8, 128), 1)
    c = core[0]

    def squares(src, half):
        def one(m, total):
            base = half * HALF + m * BLOCK
            for rb in range(3):
                acc = jnp.zeros((16, 128), f32)
                for k in range(9):
                    v = src[m, (rb * 9 + k) * 16 : (rb * 9 + k) * 16 + 16, :].astype(f32)
                    acc = acc + v * v
                ok = base + rb * 8 + srow < VALID
                total = total + jnp.where(ok, acc[0:8] + acc[8:16], 0.0)
            e = src[m, 432:448, :].astype(f32)
            e = e[0:8] + e[8:16]
            e_ref[half * 16 + m] = e
            ok = (base + lane < VALID) & (lane < BLOCK) & (srow == 0)
            return total + jnp.where(ok, e * e, 0.0)

        return one

    total = jnp.zeros((8, 128), f32)
    total = lax.fori_loop(0, 16, squares(mine, c), total)
    total = lax.fori_loop(0, 16, squares(other, 1 - c), total)
    mean = jnp.sum(total) * (1.0 / (VALID * 2305))
    scale = lax.rsqrt(jnp.full((8, 128), mean + NORM_EPS, f32))

    def chunk(block):
        rows = pl.ds(pl.multiple_of(block * BLOCK, 8), BLOCK)
        return pltpu.make_async_copy(w_ref.at[rows], cw_out.at[rows], sem)

    def write(src, half):
        def one(m, carry):
            block = half * 16 + m
            for rb in range(3):
                row = pl.multiple_of(block * BLOCK + rb * 8, 8)
                for k in range(9):
                    v = src[m, (rb * 9 + k) * 16 : (rb * 9 + k) * 16 + 16, :].astype(f32)
                    w_ref[pl.ds(row, 8), k * 256 : k * 256 + 128] = v[0:8] * scale
                    w_ref[pl.ds(row, 8), k * 256 + 128 : k * 256 + 256] = v[8:16] * scale

            @pl.when(block < 30)
            def _():
                chunk(block).start()

            return carry

        return one

    lax.fori_loop(0, 16, write(mine, c), 0)
    lax.fori_loop(0, 16, write(other, 1 - c), 0)
    bw_out[...] = w_ref[720:756, :]
    row_ref[...] = jnp.zeros((8, 896), f32)
    for block in range(32):
        tile, off = divmod(block * BLOCK, 128)
        e = e_ref[block] * scale
        e = e if off == 0 else pltpu.roll(e, off, 1)
        here = (lane >= off) & (lane < off + BLOCK)
        row_ref[:, tile * 128 : tile * 128 + 128] = jnp.where(here, e, row_ref[:, tile * 128 : tile * 128 + 128])
        if off + BLOCK > 128:
            past = lane < off + BLOCK - 128
            row_ref[:, tile * 128 + 128 : tile * 128 + 256] = jnp.where(past, e, 0.0)
    cb_out[...] = row_ref[0:1, 0:720]
    bb_out[...] = pltpu.roll(row_ref[:, 640:768], 128 - 80, 1)[0:1, 0:36]
    e = jnp.where(srow == 0, e_ref[31], 0.0)
    sums = jnp.sum(jnp.where((lane >= 12) & (lane < 16), e, 0.0))
    count = jnp.sum(jnp.where(lane == 16, e, 0.0))
    loss[...] = jnp.full((1, 128), sums, f32) / jnp.full((1, 128), count, f32)

    def drain(k, carry):
        chunk(k).wait()
        return carry

    lax.fori_loop(0, 30, drain, 0)


VMEM = pl.BlockSpec(memory_space=pltpu.VMEM)
SMEM = pl.BlockSpec(memory_space=pltpu.SMEM)
ANY = pl.BlockSpec(memory_space=pl.ANY)


def shape(*dims, dtype=f32):
    return jax.ShapeDtypeStruct(dims, dtype)


def head(first, yi, ci, before, own, after, cw, bw, cb, bb, lab, idx, box):
    return pl.pallas_call(
        head_kernel,
        out_shape=[shape(ROWS_ALL, 256, dtype=bf16)] + [shape(GROUP_ROWS, 256, dtype=bf16)] * 8,
        in_specs=[SMEM] * 3 + [VMEM] * 10,
        out_specs=[VMEM] * 9,
        scratch_shapes=[
            pltpu.VMEM((256, 2304), bf16),
            pltpu.VMEM((720, 256), f32),
            pltpu.VMEM((128, 128), f32),
            pltpu.VMEM((128, 128), f32),
            pltpu.VMEM((ROWS_ALL, 256), bf16),
            pltpu.VMEM((16, 768), f32),
            pltpu.VMEM((8, 128), f32),
            pltpu.VMEM((32, 128), jnp.int32),
            pltpu.VMEM((32, 128), jnp.int32),
        ],
        name="head",
    )(first, yi, ci, before, own, after, cw, bw, cb, bb, lab, idx, box)


def tower_terms(g, cw, bw):
    return pl.pallas_call(
        tower_kernel,
        out_shape=(
            shape(2, 128, 256),
            shape(1, 128, 256, dtype=bf16),
            shape(1, 128, 256, dtype=bf16),
        ),
        in_specs=[VMEM, ANY, VMEM],
        out_specs=(VMEM, VMEM, VMEM),
        scratch_shapes=[pltpu.VMEM((ROWS_ALL, 2304), bf16), pltpu.SemaphoreType.DMA],
        cost_estimate=pl.CostEstimate(flops=2 * 756 * 2304 * 256, transcendentals=0, bytes_accessed=4500000),
        name="tower_terms",
    )(g, cw, bw)


def tower_end(mid, above, below):
    return pl.pallas_call(
        tower_end_kernel,
        out_shape=shape(1, 2, 128, 256, dtype=bf16),
        in_specs=[VMEM] * 3,
        out_specs=VMEM,
        name="tower_end",
    )(mid, above, below)


def weight_terms(yi, ci, g, near, far, after):
    return pl.pallas_call(
        weight_kernel,
        out_shape=shape(4, PIECE, 128, dtype=bf16),
        in_specs=[SMEM] * 2 + [VMEM] * 16 + [ANY],
        out_specs=VMEM,
        scratch_shapes=[
            pltpu.VMEM((18, 128, 256), bf16),
            pltpu.VMEM((3, 2304, 256), bf16),
            pltpu.VMEM((8, GROUP_ROWS, 256), bf16),
        ],
        name="weight_terms",
    )(yi, ci, *g, *near, *far, after)


def block_sum(zi, m, after):
    return pl.pallas_call(
        sum_kernel,
        out_shape=shape(8, 56, 128, dtype=bf16),
        in_specs=[SMEM, VMEM, ANY],
        out_specs=VMEM,
        name="block_sum",
    )(zi, m, after)


def finish(core, mine, other):
    return pl.pallas_call(
        final_kernel,
        out_shape=(shape(720, 2304), shape(36, 2304), shape(1, 720), shape(1, 36), shape(1, 128)),
        in_specs=[SMEM, VMEM, VMEM],
        out_specs=(ANY, VMEM, VMEM, VMEM, VMEM),
        scratch_shapes=[
            pltpu.VMEM((ROWS_ALL, 2304), f32),
            pltpu.VMEM((32, 8, 128), f32),
            pltpu.VMEM((8, 896), f32),
            pltpu.SemaphoreType.DMA,
        ],
        name="finish",
    )(core, mine, other)


def swap(value):
    return lax.ppermute(value, "core", [(0, 1), (1, 0)])


def ahead(value, k, other):
    pairs = [(y * 2 + c, ((y + k) % 4) * 2 + (1 - c if other else c)) for y in range(4) for c in range(2)]
    return lax.ppermute(value, ("y", "core"), pairs)


def per_device(tower, cls_weight, cls_bias, box_weight, box_bias, labels, target_index, boxes):
    own = tower[0]
    tiles = 32
    up = [(t, t + 1) for t in range(tiles - 1)]
    down = [(t + 1, t) for t in range(tiles - 1)]
    before = lax.ppermute(own[1:2], TILE_AXES, up)
    after = lax.ppermute(own[0:1], TILE_AXES, down)
    ci = lax.axis_index("core").reshape(1)
    yi = lax.axis_index("y").reshape(1)
    zi = (lax.axis_index("zhi") * 4 + lax.axis_index("zlo")).reshape(1)
    first = (lax.axis_index(TILE_AXES) * 2).reshape(1)

    edge = jnp.where(lax.axis_index("core") == 0, before, after)
    rows = jnp.concatenate([own, edge], axis=0)
    near = [rows] + [ahead(rows, k, False) for k in (1, 2, 3)]

    g, *blocks = head(
        first, yi, ci, before, own, after, cls_weight, box_weight,
        cls_bias.reshape(1, 720), box_bias.reshape(1, 36), labels[0], target_index[0], boxes[0],
    )
    g, *near = lax.optimization_barrier((g, *near))
    far = [swap(v) for v in near]
    blocks = [blocks[0]] + [ahead(blocks[k], k, False) for k in (1, 2, 3)] + [
        ahead(blocks[4 + k], k, True) for k in range(4)
    ]

    mid, to_up, to_down = tower_terms(g, cls_weight, box_weight)
    below = lax.ppermute(to_up, TILE_AXES, down)
    above = lax.ppermute(to_down, TILE_AXES, up)
    tower_grad = tower_end(mid, above, below)

    terms = weight_terms(yi, ci, blocks, near, far, mid).reshape(32, 56, 128)
    terms = lax.all_to_all(terms, ("x", "zhi", "zlo"), 0, 0, tiled=True)
    copies = lax.all_to_all(block_sum(zi, terms, tower_grad), ("zhi", "zlo"), 0, 0, tiled=True)
    block = copies.reshape(PIECE, 128)
    mine = lax.all_to_all(jnp.broadcast_to(block[None], (16, PIECE, 128)), ("y", "x"), 0, 0, tiled=True)
    other = swap(mine)
    cw_grad, bw_grad, cb_grad, bb_grad, loss = finish(ci, mine, other)
    return loss[0, 0], cw_grad, cb_grad.reshape(720), bw_grad, bb_grad.reshape(36), tower_grad


def solution(mesh):
    fine = Mesh(mesh.devices.reshape(4, 4, 2, 4, 2), ("zlo", "y", "core", "x", "zhi"))
    placed = (
        P(IMG_AXES, TILE_AXES, None, None),
        P(),
        P(),
        P(),
        P(),
        P(IMG_AXES, None, TILE_AXES, None),
        P(IMG_AXES, None, TILE_AXES, None),
        P(IMG_AXES, None, None),
    )
    return jax.shard_map(
        per_device,
        mesh=fine,
        in_specs=placed,
        out_specs=(P(), P(), P(), P(), P(), P(IMG_AXES, TILE_AXES, None, None)),
        check_vma=False,
    )
```

```python
import jax
import jax.numpy as jnp
from jax import lax
from jax.experimental import pallas as pl
from jax.experimental.pallas import tpu as pltpu
from jax.sharding import Mesh, PartitionSpec as P

CLASSES = 80
ANCHORS = 9
STRIDE = 8
FOCAL_ALPHA = 0.25
NORM_EPS = 1e-06

ROWS_ALL = 768
VALID = 756
HALF = 384
GROUP_ROWS = 96
BLOCK = 24
TILES = 56
PIECE = 448

LIMIT = 24 << 20

TILE_AXES = ("zlo", "y", "core")
IMG_AXES = ("x", "zhi")

f32 = jnp.float32
bf16 = jnp.bfloat16


def dot(a, b, dims):
    return lax.dot_general(a, b, (dims, ((), ())), preferred_element_type=f32)


def shifted(x, j):
    if j == 1:
        return x
    ids = lax.broadcasted_iota(jnp.int32, x.shape, 0)
    if j == 0:
        return jnp.where(ids == 0, 0.0, pltpu.roll(x, 1, 0))
    return jnp.where(ids == x.shape[0] - 1, 0.0, pltpu.roll(x, x.shape[0] - 1, 0))


def fill_patches(rows, p_ref, base):
    for e, row in enumerate(rows):
        x = row.astype(f32)
        for j in range(3):
            v = shifted(x, j).astype(bf16)
            for i in range(3):
                r = e - i
                if 0 <= r < 2:
                    p_ref[base + r * 128 : base + r * 128 + 128, (3 * i + j) * 256 : (3 * i + j) * 256 + 256] = v


def anchor_sizes(shape):
    ids = lax.broadcasted_iota(jnp.int32, shape, 0)
    w = jnp.ones(shape, f32)
    h = jnp.ones(shape, f32)
    for a in range(ANCHORS):
        base = 4.0 * STRIDE * 2.0 ** ((a // 3) / 3.0)
        ratio = a % 3 - 1
        w = jnp.where(ids == a, base * 2.0 ** (-ratio / 2.0), w)
        h = jnp.where(ids == a, base * 2.0 ** (ratio / 2.0), h)
    return w, h


def giou_terms(o0, o1, o2, o3, aw, ah, cx, cy, tl, tt, tr, tb):
    mx = cx + o0 * aw
    my = cy + o1 * ah
    pw = aw * jnp.exp(o2)
    ph = ah * jnp.exp(o3)
    left = mx - 0.5 * pw
    right = mx + 0.5 * pw
    top = my - 0.5 * ph
    bottom = my + 0.5 * ph
    iw = jnp.maximum(jnp.minimum(right, tr) - jnp.maximum(left, tl), 0.0)
    ih = jnp.maximum(jnp.minimum(bottom, tb) - jnp.maximum(top, tt), 0.0)
    inter = iw * ih
    union = pw * ph + (tr - tl) * (tb - tt) - inter
    ow = jnp.maximum(right, tr) - jnp.minimum(left, tl)
    oh = jnp.maximum(bottom, tb) - jnp.minimum(top, tt)
    outer = ow * oh
    return 1.0 - (inter / union - (outer - union) / outer)


def head_kernel(first, yi, ci, before, own, after, cw, bw, cb, bb, lab, idx, box, *refs):
    g_out = refs[0]
    blocks = refs[1:9]
    p_ref, o_ref, b_ref, gb_ref, g_ref, row_ref, box_ref, lab_ref, idx_ref = refs[9:]
    fill_patches([before[0], own[0], own[1], after[0]], p_ref, 0)
    row_ref[0, 0:720] = cb[...]
    row_ref[8, 0:36] = bb[...]
    column = row_ref[0:8, :].T[:, 0:1]
    box_column = row_ref[8:16, 0:128].T[:, 0:1]
    box_ref[0:4, 0:100] = box[...]
    lab_ref[...] = jnp.full((32, 128), -2, jnp.int32)
    idx_ref[...] = jnp.zeros((32, 128), jnp.int32)
    for r in range(2):
        for a in range(ANCHORS):
            lab_ref[r * 16 + a : r * 16 + a + 1, :] = lab[a, r : r + 1, :]
            idx_ref[r * 16 + a : r * 16 + a + 1, :] = idx[a, r : r + 1, :]
    p = p_ref[...]
    o_ref[...] = dot(cw[...], p, ((1,), (1,))) + column[0:720]
    small_out = dot(bw[...], p, ((1,), (1,))) + box_column[0:36]
    for r in range(2):
        b_ref[r * 64 + 32 : r * 64 + 64, :] = jnp.zeros((32, 128), f32)
        b_ref[r * 64 : r * 64 + 36, :] = small_out[:, r * 128 : r * 128 + 128]
    cls = lax.broadcasted_iota(jnp.int32, (CLASSES, 128), 0)

    def one_anchor(a, carry):
        sums = []
        at = pl.multiple_of(a * CLASSES, 16)
        for r in range(2):
            label = lab_ref[pl.ds(r * 16 + a, 1), :]
            x = o_ref[pl.ds(at, CLASSES), r * 128 : r * 128 + 128]
            hit = label == cls
            z = jnp.where(hit, -x, x)
            e = jnp.exp(-jnp.abs(z))
            soft = jnp.maximum(z, 0.0) + jnp.log1p(e)
            big = 1.0 / (1.0 + e)
            small = e * big
            up = z >= 0.0
            q = jnp.where(up, big, small)
            rest = jnp.where(up, small, big)
            counted = (label >= -1).astype(f32)
            w = jnp.where(hit, FOCAL_ALPHA, 1.0 - FOCAL_ALPHA) * counted
            wq = w * q * q
            dz = wq * (q + 2.0 * rest * soft)
            g_ref[pl.ds(at, CLASSES), r * 128 : r * 128 + 128] = jnp.where(hit, -dz, dz).astype(bf16)
            sums.append(carry[r] + jnp.sum(wq * soft, axis=0, keepdims=True))
        return tuple(sums)

    zero = jnp.zeros((1, 128), f32)
    focal = lax.fori_loop(0, ANCHORS, one_anchor, (zero, zero))

    aw, ah = anchor_sizes((16, 128))
    cx = (lax.broadcasted_iota(jnp.int32, (16, 128), 1).astype(f32) + 0.5) * STRIDE
    for r in range(2):
        cy = (jnp.full((16, 128), first[0] + r, jnp.int32).astype(f32) + 0.5) * STRIDE
        which = idx_ref[r * 16 : r * 16 + 16, :]
        corner = [
            jnp.take_along_axis(jnp.broadcast_to(box_ref[k : k + 1, :], (16, 128)), which, axis=1) for k in range(4)
        ]
        positive = lab_ref[r * 16 : r * 16 + 16, :] >= 0
        o = [b_ref[pl.ds(r * 64 + k, 16, stride=4), :] for k in range(4)]
        value, pull = jax.vjp(
            lambda o0, o1, o2, o3: giou_terms(o0, o1, o2, o3, aw, ah, cx, cy, *corner), *o
        )
        grads = pull(jnp.ones((16, 128), f32))
        for k in range(4):
            gb_ref[pl.ds(r * 64 + k, 16, stride=4), :] = jnp.where(positive, grads[k], 0.0)
        giou = jnp.sum(jnp.where(positive, value, 0.0), axis=0, keepdims=True)
        count = jnp.sum(positive.astype(f32), axis=0, keepdims=True)
        rows = []
        for v in (focal[r], giou):
            hi = v.astype(bf16).astype(f32)
            rows += [hi, v - hi]
        rows.append(count)
        for n, v in enumerate(rows):
            gb_ref[r * 64 + 36 + n : r * 64 + 37 + n, :] = v
        g_ref[720:768, r * 128 : r * 128 + 128] = gb_ref[r * 64 : r * 64 + 48, :].astype(bf16)
    g_out[...] = g_ref[...]
    for k in range(4):
        y = (yi[0] + k) & 3
        for other in range(2):
            c = ci[0] if other == 0 else 1 - ci[0]
            at = pl.multiple_of(c * HALF + y * GROUP_ROWS, 16)
            blocks[other * 4 + k][...] = g_ref[pl.ds(at, GROUP_ROWS), :]


def tower_kernel(g, cw, bw, unused, mid, up, down, token, w_ref, sem):
    token[...] = jnp.zeros((8, 128), f32)
    copy = pltpu.make_async_copy(cw, w_ref.at[pl.ds(0, 720)], sem)
    copy.start()
    w_ref[752:768, :] = jnp.zeros((16, 2304), bf16)
    w_ref[720:756, :] = bw[...]
    gt = g[...].astype(f32).T
    gj = []
    for j in range(3):
        gj.append(
            jnp.concatenate([shifted(gt[r * 128 : r * 128 + 128], 2 - j) for r in range(2)], axis=0).astype(bf16)
        )
    copy.wait()
    t = []
    for i in range(3):
        acc = jnp.zeros((256, 256), f32)
        for j in range(3):
            at = (3 * i + j) * 256
            acc = acc + dot(gj[j], w_ref[:, at : at + 256], ((1,), (0,)))
        t.append(acc)
    up[0] = t[0][0:128].astype(bf16)
    mid[0] = t[1][0:128] + t[0][128:256]
    mid[1] = t[1][128:256] + t[2][0:128]
    down[0] = t[2][128:256].astype(bf16)


def tower_end_kernel(mid, above, below, t_ref, token):
    token[...] = jnp.zeros((8, 128), f32)
    t_ref[0, 0] = (mid[0] + above[0].astype(f32)).astype(bf16)
    t_ref[0, 1] = (mid[1] + below[0].astype(f32)).astype(bf16)


def weight_kernel(yi, ci, xi, *refs):
    g = refs[0:8]
    near = refs[8:12]
    far = refs[12:16]
    edge_lo, edge_hi = refs[16:18]
    outs = refs[18:22]
    t_ref, s_ref, g_ref, m_ref = refs[23:]
    t_ref[0] = edge_lo[0]
    t_ref[17] = edge_hi[0]
    for k in range(4):
        y = (yi[0] - k) & 3
        for src, c in ((near, ci[0]), (far, 1 - ci[0])):
            for r in range(2):
                t_ref[1 + r + y * 4 + c * 2] = src[k][r]
        g_ref[y * 2 + ci[0]] = g[k][...]
        g_ref[y * 2 + 1 - ci[0]] = g[4 + k][...]

    def shift(row, carry):
        x = t_ref[row].astype(f32)
        at = pl.multiple_of(row * 128, 128)
        for j in range(3):
            s_ref[j, pl.ds(at, 128), :] = shifted(x, j).astype(bf16)
        return carry

    lax.fori_loop(0, 18, shift, 0)
    lhs = jnp.concatenate([g_ref[n] for n in range(8)], axis=1)
    for tap in range(9):
        i, j = divmod(tap, 3)
        acc = dot(lhs, s_ref[j, i * 128 : i * 128 + 2048, :], ((1,), (0,)))
        for m in range(4):
            for rb in range(3):
                row = m * BLOCK + rb * 8
                both = jnp.concatenate([acc[row : row + 8, 0:128], acc[row : row + 8, 128:256]], axis=0)
                v = (rb * 18 + 2 * tap) * 8
                m_ref[m, v : v + 16, :] = both.astype(bf16)
    bias = dot(jnp.ones((8, 2048), bf16), lhs, ((1,), (1,)))
    bias = jnp.concatenate([bias, jnp.zeros((8, 32), f32)], axis=1)
    for m in range(4):
        e = bias if m == 0 else pltpu.roll(bias, 128 - m * BLOCK, 1)
        hi = e.astype(bf16).astype(f32)
        m_ref[m, 432:448, :] = jnp.concatenate([hi, e - hi], axis=0).astype(bf16)
    refs[22][...] = jnp.zeros((8, 128), f32)
    for k in range(4):
        outs[k][...] = m_ref[(xi[0] + k) & 3]


def block_sum_kernel(a, b, c, d, unused, s_ref):
    acc = (a[...].astype(f32) + b[...].astype(f32)) + (c[...].astype(f32) + d[...].astype(f32))
    e = acc[432:440] + acc[440:448]
    hi = e.astype(bf16).astype(f32)
    s_ref[0:432, :] = acc[0:432].astype(bf16)
    s_ref[432:448, :] = jnp.concatenate([hi, e - hi], axis=0).astype(bf16)


def piece_sum_kernel(zi, m_ref, c_ref):
    acc = m_ref[0].astype(f32)
    for m in range(1, 8):
        acc = acc + m_ref[m].astype(f32)
    last = jnp.full((8, 128), zi[0], jnp.int32) == 7
    e = acc[40:48] + acc[48:56]
    hi = e.astype(bf16).astype(f32)
    out = jnp.concatenate(
        [acc[0:40], jnp.where(last, hi, acc[40:48]), jnp.where(last, e - hi, acc[48:56])], axis=0
    ).astype(bf16)
    for z in range(8):
        c_ref[z] = out


def join_kernel(a, b, c, d, o_ref):
    for k, ref in enumerate((a, b, c, d)):
        o_ref[k] = ref[...]


def final_kernel(yi, xi, ci, *refs):
    sources = refs[0:8]
    cw_out, bw_out, cb_out, bb_out, loss, w_ref, e_ref, row_ref, sem = refs[9:]
    srow = lax.broadcasted_iota(jnp.int32, (8, 128), 0)
    lane = lax.broadcasted_iota(jnp.int32, (8, 128), 1)

    def block_of(n, k):
        c = ci[0] if n < 4 else 1 - ci[0]
        far = n % 4
        y = (yi[0] - jnp.where(c == 0, far, k)) & 3
        x = (xi[0] - jnp.where(c == 0, k, far)) & 3
        return c * 16 + y * 4 + x

    def squares(n):
        src = sources[n]

        def one(k, total):
            block = block_of(n, k)
            base = block * BLOCK
            for rb in range(3):
                acc = jnp.zeros((16, 128), f32)
                for t in range(9):
                    v = src[k, (rb * 9 + t) * 16 : (rb * 9 + t) * 16 + 16, :].astype(f32)
                    acc = acc + v * v
                ok = base + rb * 8 + srow < VALID
                total = total + jnp.where(ok, acc[0:8] + acc[8:16], 0.0)
            e = src[k, 432:448, :].astype(f32)
            e = e[0:8] + e[8:16]
            e_ref[block] = e
            ok = (base + lane < VALID) & (lane < BLOCK) & (srow == 0)
            return total + jnp.where(ok, e * e, 0.0)

        return one

    total = jnp.zeros((8, 128), f32)
    for n in range(8):
        total = lax.fori_loop(0, 4, squares(n), total)
    mean = jnp.sum(total) * (1.0 / (VALID * 2305))
    scale = lax.rsqrt(jnp.full((8, 128), mean + NORM_EPS, f32))

    def chunk(block):
        rows = pl.ds(pl.multiple_of(block * BLOCK, 8), BLOCK)
        return pltpu.make_async_copy(w_ref.at[rows], cw_out.at[rows], sem)

    def write(n):
        src = sources[n]

        def one(k, carry):
            block = block_of(n, k)
            for rb in range(3):
                row = pl.multiple_of(block * BLOCK + rb * 8, 8)
                for t in range(9):
                    v = src[k, (rb * 9 + t) * 16 : (rb * 9 + t) * 16 + 16, :].astype(f32)
                    w_ref[pl.ds(row, 8), t * 256 : t * 256 + 128] = v[0:8] * scale
                    w_ref[pl.ds(row, 8), t * 256 + 128 : t * 256 + 256] = v[8:16] * scale

            @pl.when(block < 30)
            def _():
                chunk(block).start()

            return carry

        return one

    for n in range(8):
        lax.fori_loop(0, 4, write(n), 0)
    bw_out[...] = w_ref[720:756, :]
    row_ref[...] = jnp.zeros((8, 896), f32)
    for block in range(32):
        tile, off = divmod(block * BLOCK, 128)
        e = e_ref[block] * scale
        e = e if off == 0 else pltpu.roll(e, off, 1)
        here = (lane >= off) & (lane < off + BLOCK)
        row_ref[:, tile * 128 : tile * 128 + 128] = jnp.where(here, e, row_ref[:, tile * 128 : tile * 128 + 128])
        if off + BLOCK > 128:
            past = lane < off + BLOCK - 128
            row_ref[:, tile * 128 + 128 : tile * 128 + 256] = jnp.where(past, e, 0.0)
    cb_out[...] = row_ref[0, 0:720]
    bb_out[...] = pltpu.roll(row_ref[:, 640:768], 128 - 80, 1)[0, 0:36]
    e = jnp.where(srow == 0, e_ref[31], 0.0)
    sums = jnp.sum(jnp.where((lane >= 12) & (lane < 16), e, 0.0))
    count = jnp.sum(jnp.where(lane == 16, e, 0.0))
    loss[...] = jnp.full((1, 128), sums, f32) / jnp.full((1, 128), count, f32)

    def drain(k, carry):
        chunk(k).wait()
        return carry

    lax.fori_loop(0, 30, drain, 0)


VMEM = pl.BlockSpec(memory_space=pltpu.VMEM)
SMEM = pl.BlockSpec(memory_space=pltpu.SMEM)
ANY = pl.BlockSpec(memory_space=pl.ANY)


def near_memory(arrays):
    return [pltpu.with_memory_space_constraint(v, pltpu.VMEM) for v in arrays]


def shape(*dims, dtype=f32):
    return jax.ShapeDtypeStruct(dims, dtype)


def head(first, yi, ci, before, own, after, cw, bw, cb, bb, lab, idx, box):
    return pl.pallas_call(
        head_kernel,
        out_shape=[pltpu.VMEM((ROWS_ALL, 256), bf16)] + [pltpu.VMEM((GROUP_ROWS, 256), bf16)] * 8,
        in_specs=[SMEM] * 3 + [VMEM] * 10,
        out_specs=[VMEM] * 9,
        scratch_shapes=[
            pltpu.VMEM((256, 2304), bf16),
            pltpu.VMEM((720, 256), f32),
            pltpu.VMEM((128, 128), f32),
            pltpu.VMEM((128, 128), f32),
            pltpu.VMEM((ROWS_ALL, 256), bf16),
            pltpu.VMEM((16, 768), f32),
            pltpu.VMEM((8, 128), f32),
            pltpu.VMEM((32, 128), jnp.int32),
            pltpu.VMEM((32, 128), jnp.int32),
        ],
        compiler_params=pltpu.CompilerParams(vmem_limit_bytes=LIMIT),
        name="head",
    )(first, yi, ci, *near_memory([before, own, after, cw, bw, cb, bb, lab, idx, box]))


def tower_terms(g, cw, bw, after):
    return pl.pallas_call(
        tower_kernel,
        out_shape=(
            pltpu.VMEM((2, 128, 256), f32),
            pltpu.VMEM((1, 128, 256), bf16),
            pltpu.VMEM((1, 128, 256), bf16),
            shape(8, 128),
        ),
        in_specs=[VMEM, VMEM, VMEM, ANY],
        out_specs=(VMEM, VMEM, VMEM, VMEM),
        scratch_shapes=[pltpu.VMEM((ROWS_ALL, 2304), bf16), pltpu.SemaphoreType.DMA],
        cost_estimate=pl.CostEstimate(flops=2 * 756 * 2304 * 256, transcendentals=0, bytes_accessed=4500000),
        compiler_params=pltpu.CompilerParams(vmem_limit_bytes=LIMIT),
        name="tower_terms",
    )(*near_memory([g, cw, bw]), after)


def tower_end(mid, above, below):
    return pl.pallas_call(
        tower_end_kernel,
        out_shape=(shape(1, 2, 128, 256, dtype=bf16), shape(8, 128)),
        in_specs=[VMEM] * 3,
        out_specs=(VMEM, VMEM),
        compiler_params=pltpu.CompilerParams(vmem_limit_bytes=LIMIT),
        name="tower_end",
    )(*near_memory([mid, above, below]))


def weight_terms(yi, ci, xi, g, near, far, edges):
    return pl.pallas_call(
        weight_kernel,
        out_shape=[pltpu.VMEM((PIECE, 128), bf16)] * 4 + [shape(8, 128)],
        in_specs=[SMEM] * 3 + [VMEM] * 18,
        out_specs=[VMEM] * 5,
        scratch_shapes=[
            pltpu.VMEM((18, 128, 256), bf16),
            pltpu.VMEM((3, 2304, 256), bf16),
            pltpu.VMEM((8, GROUP_ROWS, 256), bf16),
            pltpu.VMEM((4, PIECE, 128), bf16),
        ],
        compiler_params=pltpu.CompilerParams(vmem_limit_bytes=LIMIT),
        name="weight_terms",
    )(yi, ci, xi, *near_memory([*g, *near, *far, *edges]))


def block_sum(parts, after):
    return pl.pallas_call(
        block_sum_kernel,
        out_shape=pltpu.VMEM((PIECE, 128), bf16),
        in_specs=[VMEM] * 4 + [ANY],
        out_specs=VMEM,
        compiler_params=pltpu.CompilerParams(vmem_limit_bytes=LIMIT),
        name="block_sum",
    )(*near_memory(parts), after)


def piece_sum(zi, m):
    return pl.pallas_call(
        piece_sum_kernel,
        out_shape=pltpu.VMEM((8, 56, 128), bf16),
        in_specs=[SMEM, VMEM],
        out_specs=VMEM,
        compiler_params=pltpu.CompilerParams(vmem_limit_bytes=LIMIT),
        name="piece_sum",
    )(zi, *near_memory([m]))


def join(parts):
    return pl.pallas_call(
        join_kernel,
        out_shape=pltpu.VMEM((4, PIECE, 128), bf16),
        in_specs=[VMEM] * 4,
        out_specs=VMEM,
        compiler_params=pltpu.CompilerParams(vmem_limit_bytes=LIMIT),
        name="join",
    )(*near_memory(parts))


def finish(yi, xi, ci, mine, other, after):
    return pl.pallas_call(
        final_kernel,
        out_shape=(shape(720, 2304), shape(36, 2304), shape(720), shape(36), shape(1, 128)),
        in_specs=[SMEM] * 3 + [VMEM] * 8 + [ANY],
        out_specs=(ANY, VMEM, VMEM, VMEM, VMEM),
        scratch_shapes=[
            pltpu.VMEM((ROWS_ALL, 2304), f32),
            pltpu.VMEM((32, 8, 128), f32),
            pltpu.VMEM((8, 896), f32),
            pltpu.SemaphoreType.DMA,
        ],
        compiler_params=pltpu.CompilerParams(vmem_limit_bytes=LIMIT),
        name="finish",
    )(yi, xi, ci, *near_memory([*mine, *other]), after)


def swap(value):
    return lax.ppermute(value, "core", [(0, 1), (1, 0)])


def ahead(value, k, other):
    pairs = [(y * 2 + c, ((y + k) % 4) * 2 + (1 - c if other else c)) for y in range(4) for c in range(2)]
    return lax.ppermute(value, ("y", "core"), pairs)


def along(value, k, first_axis):
    pairs = []
    for y in range(4):
        for c in range(2):
            for x in range(4):
                dx = k if (first_axis == "x") == (c == 0) else 0
                dy = k - dx
                pairs.append(((y * 2 + c) * 4 + x, (((y + dy) % 4) * 2 + c) * 4 + (x + dx) % 4))
    return lax.ppermute(value, ("y", "core", "x"), pairs)


def per_device(tower, cls_weight, cls_bias, box_weight, box_bias, labels, target_index, boxes):
    own = tower[0]
    tiles = 32
    up = [(t, t + 1) for t in range(tiles - 1)]
    down = [(t + 1, t) for t in range(tiles - 1)]
    before = lax.ppermute(own[1:2], TILE_AXES, up)
    after = lax.ppermute(own[0:1], TILE_AXES, down)
    near = [own] + [ahead(own, k, False) for k in (1, 2, 3)]
    core = lax.axis_index("core")
    y = lax.axis_index("y")
    ci = core.reshape(1)
    yi = y.reshape(1)
    xi = lax.axis_index("x").reshape(1)
    zi = (lax.axis_index("zhi") * 4 + lax.axis_index("zlo")).reshape(1)
    first = (lax.axis_index(TILE_AXES) * 2).reshape(1)

    g, *blocks = head(
        first, yi, ci, before, own, after, cls_weight, box_weight,
        cls_bias, box_bias, labels[0], target_index[0], boxes[0],
    )
    g, *near = lax.optimization_barrier((g, *near))
    far = [swap(v) for v in near]
    blocks = [blocks[0]] + [ahead(blocks[k], k, False) for k in (1, 2, 3)] + [
        ahead(blocks[4 + k], k, True) for k in range(4)
    ]
    row_0 = near[0][0:1] * 0
    row_15 = row_0
    for k in range(4):
        for src, c in ((near[k], core), (far[k], 1 - core)):
            row_0 = jnp.where((y == k) & (c == 0), src[0:1], row_0)
            row_15 = jnp.where((y == (k + 3) % 4) & (c == 1), src[1:2], row_15)
    edges = [
        lax.ppermute(row_15, "zlo", [(z, z + 1) for z in range(3)]),
        lax.ppermute(row_0, "zlo", [(z + 1, z) for z in range(3)]),
    ]

    *parts, token = weight_terms(yi, ci, xi, blocks, near, far, edges)
    mid, to_up, to_down, tower_token = tower_terms(g, cls_weight, box_weight, token)
    parts = [parts[0]] + [
        lax.ppermute(parts[k], "x", [(i, (i + k) % 4) for i in range(4)]) for k in (1, 2, 3)
    ]
    terms = block_sum(parts, tower_token).reshape(8, 56, 128)
    terms = lax.all_to_all(terms, ("zhi", "zlo"), 0, 0, tiled=True)
    copies = lax.all_to_all(piece_sum(zi, terms), ("zhi", "zlo"), 0, 0, tiled=True)
    block = copies.reshape(PIECE, 128)
    row = join([block] + [along(block, k, "x") for k in (1, 2, 3)])
    row, to_up, to_down = lax.optimization_barrier((row, to_up, to_down))
    mine = [row] + [along(row, k, "y") for k in (1, 2, 3)]
    other = [swap(v) for v in mine]
    below = lax.ppermute(to_up, TILE_AXES, down)
    above = lax.ppermute(to_down, TILE_AXES, up)
    tower_grad, end_token = tower_end(mid, above, below)
    cw_grad, bw_grad, cb_grad, bb_grad, loss = finish(yi, xi, ci, mine, other, end_token)
    return loss[0, 0], cw_grad, cb_grad, bw_grad, bb_grad, tower_grad


def solution(mesh):
    fine = Mesh(mesh.devices.reshape(4, 4, 2, 4, 2), ("zlo", "y", "core", "x", "zhi"))
    placed = (
        P(IMG_AXES, TILE_AXES, None, None),
        P(),
        P(),
        P(),
        P(),
        P(IMG_AXES, None, TILE_AXES, None),
        P(IMG_AXES, None, TILE_AXES, None),
        P(IMG_AXES, None, None),
    )
    return jax.shard_map(
        per_device,
        mesh=fine,
        in_specs=placed,
        out_specs=(P(), P(), P(), P(), P(), P(IMG_AXES, TILE_AXES, None, None)),
        check_vma=False,
    )
```

```python
import jax
import jax.numpy as jnp
from jax import lax
from jax.experimental import pallas as pl
from jax.experimental.pallas import tpu as pltpu
from jax.sharding import Mesh, PartitionSpec as P

CLASSES = 80
ANCHORS = 9
STRIDE = 8
FOCAL_ALPHA = 0.25
NORM_EPS = 1e-06

ROWS_ALL = 768
VALID = 756
HALF = 384
GROUP_ROWS = 96
BLOCK = 24
TILES = 56
PIECE = 448

LIMIT = 24 << 20

TILE_AXES = ("zlo", "y", "core")
IMG_AXES = ("x", "zhi")

f32 = jnp.float32
bf16 = jnp.bfloat16


def dot(a, b, dims):
    return lax.dot_general(a, b, (dims, ((), ())), preferred_element_type=f32)


def shifted(x, j):
    if j == 1:
        return x
    ids = lax.broadcasted_iota(jnp.int32, x.shape, 0)
    if j == 0:
        return jnp.where(ids == 0, 0.0, pltpu.roll(x, 1, 0))
    return jnp.where(ids == x.shape[0] - 1, 0.0, pltpu.roll(x, x.shape[0] - 1, 0))


def fill_patches(rows, p_ref, base):
    for e, row in enumerate(rows):
        x = row.astype(f32)
        for j in range(3):
            v = shifted(x, j).astype(bf16)
            for i in range(3):
                r = e - i
                if 0 <= r < 2:
                    p_ref[base + r * 128 : base + r * 128 + 128, (3 * i + j) * 256 : (3 * i + j) * 256 + 256] = v


def anchor_sizes(shape):
    ids = lax.broadcasted_iota(jnp.int32, shape, 0)
    w = jnp.ones(shape, f32)
    h = jnp.ones(shape, f32)
    for a in range(ANCHORS):
        base = 4.0 * STRIDE * 2.0 ** ((a // 3) / 3.0)
        ratio = a % 3 - 1
        w = jnp.where(ids == a, base * 2.0 ** (-ratio / 2.0), w)
        h = jnp.where(ids == a, base * 2.0 ** (ratio / 2.0), h)
    return w, h


def giou_terms(o0, o1, o2, o3, aw, ah, cx, cy, tl, tt, tr, tb):
    mx = cx + o0 * aw
    my = cy + o1 * ah
    pw = aw * jnp.exp(o2)
    ph = ah * jnp.exp(o3)
    left = mx - 0.5 * pw
    right = mx + 0.5 * pw
    top = my - 0.5 * ph
    bottom = my + 0.5 * ph
    iw = jnp.maximum(jnp.minimum(right, tr) - jnp.maximum(left, tl), 0.0)
    ih = jnp.maximum(jnp.minimum(bottom, tb) - jnp.maximum(top, tt), 0.0)
    inter = iw * ih
    union = pw * ph + (tr - tl) * (tb - tt) - inter
    ow = jnp.maximum(right, tr) - jnp.minimum(left, tl)
    oh = jnp.maximum(bottom, tb) - jnp.minimum(top, tt)
    outer = ow * oh
    return 1.0 - (inter / union - (outer - union) / outer)


def stage_kernel(cw, bw, w_ref, sem):
    copy = pltpu.make_async_copy(cw, w_ref.at[pl.ds(0, 720)], sem)
    copy.start()
    w_ref[752:768, :] = jnp.zeros((16, 2304), bf16)
    w_ref[720:756, :] = bw[...]
    copy.wait()


def head_kernel(first, ci, before, own, after, w, cb, bb, lab, idx, box, *refs):
    g_out, keep, send, edge = refs[0:4]
    p_ref, o_ref, b_ref, gb_ref, g_ref, row_ref, box_ref, lab_ref, idx_ref = refs[4:]
    edge[...] = jnp.where(jnp.full((1, 128, 256), ci[0], jnp.int32) == 0, before[...], after[...])
    fill_patches([before[0], own[0], own[1], after[0]], p_ref, 0)
    row_ref[0, 0:720] = cb[...]
    row_ref[8, 0:36] = bb[...]
    column = row_ref[0:8, :].T[:, 0:1]
    box_column = row_ref[8:16, 0:128].T[:, 0:1]
    box_ref[0:4, 0:100] = box[...]
    lab_ref[...] = jnp.full((32, 128), -2, jnp.int32)
    idx_ref[...] = jnp.zeros((32, 128), jnp.int32)
    for r in range(2):
        for a in range(ANCHORS):
            lab_ref[r * 16 + a : r * 16 + a + 1, :] = lab[a, r : r + 1, :]
            idx_ref[r * 16 + a : r * 16 + a + 1, :] = idx[a, r : r + 1, :]
    p = p_ref[...]
    out = dot(w[...], p, ((1,), (1,)))
    o_ref[...] = out[0:720] + column[0:720]
    small_out = out[720:756] + box_column[0:36]
    for r in range(2):
        b_ref[r * 64 + 32 : r * 64 + 64, :] = jnp.zeros((32, 128), f32)
        b_ref[r * 64 : r * 64 + 36, :] = small_out[:, r * 128 : r * 128 + 128]
    cls = lax.broadcasted_iota(jnp.int32, (CLASSES, 128), 0)

    def one_anchor(a, carry):
        sums = []
        at = pl.multiple_of(a * CLASSES, 16)
        for r in range(2):
            label = lab_ref[pl.ds(r * 16 + a, 1), :]
            x = o_ref[pl.ds(at, CLASSES), r * 128 : r * 128 + 128]
            hit = label == cls
            z = jnp.where(hit, -x, x)
            e = jnp.exp(-jnp.abs(z))
            soft = jnp.maximum(z, 0.0) + jnp.log1p(e)
            big = 1.0 / (1.0 + e)
            small = e * big
            up = z >= 0.0
            q = jnp.where(up, big, small)
            rest = jnp.where(up, small, big)
            counted = (label >= -1).astype(f32)
            w = jnp.where(hit, FOCAL_ALPHA, 1.0 - FOCAL_ALPHA) * counted
            wq = w * q * q
            dz = wq * (q + 2.0 * rest * soft)
            g_ref[pl.ds(at, CLASSES), r * 128 : r * 128 + 128] = jnp.where(hit, -dz, dz).astype(bf16)
            sums.append(carry[r] + jnp.sum(wq * soft, axis=0, keepdims=True))
        return tuple(sums)

    zero = jnp.zeros((1, 128), f32)
    focal = lax.fori_loop(0, ANCHORS, one_anchor, (zero, zero))

    aw, ah = anchor_sizes((16, 128))
    cx = (lax.broadcasted_iota(jnp.int32, (16, 128), 1).astype(f32) + 0.5) * STRIDE
    for r in range(2):
        cy = (jnp.full((16, 128), first[0] + r, jnp.int32).astype(f32) + 0.5) * STRIDE
        which = idx_ref[r * 16 : r * 16 + 16, :]
        corner = [
            jnp.take_along_axis(jnp.broadcast_to(box_ref[k : k + 1, :], (16, 128)), which, axis=1) for k in range(4)
        ]
        positive = lab_ref[r * 16 : r * 16 + 16, :] >= 0
        o = [b_ref[pl.ds(r * 64 + k, 16, stride=4), :] for k in range(4)]
        value, pull = jax.vjp(
            lambda o0, o1, o2, o3: giou_terms(o0, o1, o2, o3, aw, ah, cx, cy, *corner), *o
        )
        grads = pull(jnp.ones((16, 128), f32))
        for k in range(4):
            gb_ref[pl.ds(r * 64 + k, 16, stride=4), :] = jnp.where(positive, grads[k], 0.0)
        giou = jnp.sum(jnp.where(positive, value, 0.0), axis=0, keepdims=True)
        count = jnp.sum(positive.astype(f32), axis=0, keepdims=True)
        rows = []
        for v in (focal[r], giou):
            hi = v.astype(bf16).astype(f32)
            rows += [hi, v - hi]
        rows.append(count)
        for n, v in enumerate(rows):
            gb_ref[r * 64 + 36 + n : r * 64 + 37 + n, :] = v
        g_ref[720:768, r * 128 : r * 128 + 128] = gb_ref[r * 64 : r * 64 + 48, :].astype(bf16)
    g_out[...] = g_ref[...]
    keep[...] = g_ref[pl.ds(pl.multiple_of(ci[0] * HALF, 16), HALF), :]
    send[...] = g_ref[pl.ds(pl.multiple_of((1 - ci[0]) * HALF, 16), HALF), :]


def tower_kernel(g, w_ref, unused, mid, up, down, token):
    token[...] = jnp.zeros((8, 128), f32)
    gt = g[...].astype(f32).T
    gj = []
    for j in range(3):
        gj.append(
            jnp.concatenate([shifted(gt[r * 128 : r * 128 + 128], 2 - j) for r in range(2)], axis=0).astype(bf16)
        )
    t = []
    for i in range(3):
        acc = jnp.zeros((256, 256), f32)
        for j in range(3):
            at = (3 * i + j) * 256
            acc = acc + dot(gj[j], w_ref[:, at : at + 256], ((1,), (0,)))
        t.append(acc)
    up[0] = t[0][0:128].astype(bf16)
    mid[0] = t[1][0:128] + t[0][128:256]
    mid[1] = t[1][128:256] + t[2][0:128]
    down[0] = t[2][128:256].astype(bf16)


def tower_end_kernel(mid, above, below, t_ref, token):
    token[...] = jnp.zeros((8, 128), f32)
    t_ref[0, 0] = (mid[0] + above[0].astype(f32)).astype(bf16)
    t_ref[0, 1] = (mid[1] + below[0].astype(f32)).astype(bf16)


def weight_kernel(yi, xi, ci, keep, got, own, other, edge, other_edge, *refs):
    outs = refs[0:4]
    token, t_ref, s_ref, g_ref, m_ref = refs[4:]
    token[...] = jnp.zeros((8, 128), f32)
    c = ci[0]
    t_ref[5 * c] = edge[0]
    t_ref[5 - 5 * c] = other_edge[0]
    for r in range(2):
        t_ref[1 + 2 * c + r] = own[r]
        t_ref[3 - 2 * c + r] = other[r]
    g_ref[c] = keep[...]
    g_ref[1 - c] = got[...]

    def shift(row, carry):
        x = t_ref[row].astype(f32)
        at = pl.multiple_of(row * 128, 128)
        for j in range(3):
            s_ref[j, pl.ds(at, 128), :] = shifted(x, j).astype(bf16)
        return carry

    lax.fori_loop(0, 6, shift, 0)
    lhs = jnp.concatenate([g_ref[0], g_ref[1]], axis=1)
    for tap in range(9):
        i, j = divmod(tap, 3)
        acc = dot(lhs, s_ref[j, i * 128 : i * 128 + 512, :], ((1,), (0,)))
        for m in range(16):
            for rb in range(3):
                row = m * BLOCK + rb * 8
                both = jnp.concatenate([acc[row : row + 8, 0:128], acc[row : row + 8, 128:256]], axis=0)
                v = (rb * 18 + 2 * tap) * 8
                m_ref[m, v : v + 16, :] = both.astype(bf16)
    bias = dot(jnp.ones((8, 512), bf16), lhs, ((1,), (1,)))
    for m in range(16):
        tile, off = divmod(m * BLOCK, 128)
        e = bias[:, tile * 128 : tile * 128 + 128]
        e = e if off == 0 else pltpu.roll(e, 128 - off, 1)
        if off + BLOCK > 128:
            past = pltpu.roll(bias[:, tile * 128 + 128 : tile * 128 + 256], 128 - off, 1)
            lane = lax.broadcasted_iota(jnp.int32, (8, 128), 1)
            e = jnp.where(lane < 128 - off, e, past)
        hi = e.astype(bf16).astype(f32)
        m_ref[m, 432:448, :] = jnp.concatenate([hi, e - hi], axis=0).astype(bf16)
    for k in range(4):
        for q in range(4):
            outs[k][q] = m_ref[jnp.where(c == 0, ((yi[0] + k) & 3) * 4 + q, q * 4 + ((xi[0] + k) & 3))]


def row_sum_kernel(yi, xi, ci, *refs):
    parts = refs[0:4]
    outs = refs[5:9]
    here = jnp.where(ci[0] == 0, xi[0], yi[0])
    for k in range(4):
        q = (here + k) & 3
        acc = parts[0][q].astype(f32)
        for n in range(1, 4):
            acc = acc + parts[n][q].astype(f32)
        e = acc[432:440] + acc[440:448]
        hi = e.astype(bf16).astype(f32)
        outs[k][0:432, :] = acc[0:432].astype(bf16)
        outs[k][432:448, :] = jnp.concatenate([hi, e - hi], axis=0).astype(bf16)


def block_sum_kernel(a, b, c, d, s_ref):
    acc = (a[...].astype(f32) + b[...].astype(f32)) + (c[...].astype(f32) + d[...].astype(f32))
    e = acc[432:440] + acc[440:448]
    hi = e.astype(bf16).astype(f32)
    s_ref[0:432, :] = acc[0:432].astype(bf16)
    s_ref[432:448, :] = jnp.concatenate([hi, e - hi], axis=0).astype(bf16)


def piece_sum_kernel(zi, m_ref, c_ref):
    acc = m_ref[0].astype(f32)
    for m in range(1, 8):
        acc = acc + m_ref[m].astype(f32)
    last = jnp.full((8, 128), zi[0], jnp.int32) == 7
    e = acc[40:48] + acc[48:56]
    hi = e.astype(bf16).astype(f32)
    out = jnp.concatenate(
        [acc[0:40], jnp.where(last, hi, acc[40:48]), jnp.where(last, e - hi, acc[48:56])], axis=0
    ).astype(bf16)
    for z in range(8):
        c_ref[z] = out


def join_kernel(a, b, c, d, o_ref):
    for k, ref in enumerate((a, b, c, d)):
        o_ref[k] = ref[...]


def final_kernel(yi, xi, ci, *refs):
    sources = refs[0:8]
    cw_out, bw_out, cb_out, bb_out, loss, w_ref, e_ref, row_ref, sem = refs[8:]
    srow = lax.broadcasted_iota(jnp.int32, (8, 128), 0)
    lane = lax.broadcasted_iota(jnp.int32, (8, 128), 1)

    def block_of(n, k):
        c = ci[0] if n < 4 else 1 - ci[0]
        far = n % 4
        y = (yi[0] - jnp.where(c == 0, far, k)) & 3
        x = (xi[0] - jnp.where(c == 0, k, far)) & 3
        return c * 16 + y * 4 + x

    def squares(n):
        src = sources[n]

        def one(k, total):
            block = block_of(n, k)
            base = block * BLOCK
            for rb in range(3):
                acc = jnp.zeros((16, 128), f32)
                for t in range(9):
                    v = src[k, (rb * 9 + t) * 16 : (rb * 9 + t) * 16 + 16, :].astype(f32)
                    acc = acc + v * v
                ok = base + rb * 8 + srow < VALID
                total = total + jnp.where(ok, acc[0:8] + acc[8:16], 0.0)
            e = src[k, 432:448, :].astype(f32)
            e = e[0:8] + e[8:16]
            e_ref[block] = e
            ok = (base + lane < VALID) & (lane < BLOCK) & (srow == 0)
            return total + jnp.where(ok, e * e, 0.0)

        return one

    total = jnp.zeros((8, 128), f32)
    for n in range(8):
        total = lax.fori_loop(0, 4, squares(n), total)
    mean = jnp.sum(total) * (1.0 / (VALID * 2305))
    scale = lax.rsqrt(jnp.full((8, 128), mean + NORM_EPS, f32))

    def chunk(block):
        rows = pl.ds(pl.multiple_of(block * BLOCK, 8), BLOCK)
        return pltpu.make_async_copy(w_ref.at[rows], cw_out.at[rows], sem)

    def write(n):
        src = sources[n]

        def one(k, carry):
            block = block_of(n, k)
            for rb in range(3):
                row = pl.multiple_of(block * BLOCK + rb * 8, 8)
                for t in range(9):
                    v = src[k, (rb * 9 + t) * 16 : (rb * 9 + t) * 16 + 16, :].astype(f32)
                    w_ref[pl.ds(row, 8), t * 256 : t * 256 + 128] = v[0:8] * scale
                    w_ref[pl.ds(row, 8), t * 256 + 128 : t * 256 + 256] = v[8:16] * scale

            @pl.when(block < 30)
            def _():
                chunk(block).start()

            return carry

        return one

    for n in range(8):
        lax.fori_loop(0, 4, write(n), 0)
    bw_out[...] = w_ref[720:756, :]
    row_ref[...] = jnp.zeros((8, 896), f32)
    for block in range(32):
        tile, off = divmod(block * BLOCK, 128)
        e = e_ref[block] * scale
        e = e if off == 0 else pltpu.roll(e, off, 1)
        here = (lane >= off) & (lane < off + BLOCK)
        row_ref[:, tile * 128 : tile * 128 + 128] = jnp.where(here, e, row_ref[:, tile * 128 : tile * 128 + 128])
        if off + BLOCK > 128:
            past = lane < off + BLOCK - 128
            row_ref[:, tile * 128 + 128 : tile * 128 + 256] = jnp.where(past, e, 0.0)
    cb_out[...] = row_ref[0, 0:720]
    bb_out[...] = pltpu.roll(row_ref[:, 640:768], 128 - 80, 1)[0, 0:36]
    e = jnp.where(srow == 0, e_ref[31], 0.0)
    sums = jnp.sum(jnp.where((lane >= 12) & (lane < 16), e, 0.0))
    count = jnp.sum(jnp.where(lane == 16, e, 0.0))
    loss[...] = jnp.full((1, 128), sums, f32) / jnp.full((1, 128), count, f32)

    def drain(k, carry):
        chunk(k).wait()
        return carry

    lax.fori_loop(0, 30, drain, 0)


VMEM = pl.BlockSpec(memory_space=pltpu.VMEM)
SMEM = pl.BlockSpec(memory_space=pltpu.SMEM)
ANY = pl.BlockSpec(memory_space=pl.ANY)


def near_memory(arrays):
    return [pltpu.with_memory_space_constraint(v, pltpu.VMEM) for v in arrays]


def far_memory(arrays):
    return [pltpu.with_memory_space_constraint(v, pltpu.HBM) for v in arrays]


def shape(*dims, dtype=f32):
    return jax.ShapeDtypeStruct(dims, dtype)


def stage(cw, bw):
    return pl.pallas_call(
        stage_kernel,
        out_shape=pltpu.VMEM((ROWS_ALL, 2304), bf16),
        in_specs=[ANY, VMEM],
        out_specs=VMEM,
        scratch_shapes=[pltpu.SemaphoreType.DMA],
        compiler_params=pltpu.CompilerParams(vmem_limit_bytes=LIMIT),
        name="stage",
    )(*far_memory([cw, bw]))


def head(first, ci, before, own, after, w, cb, bb, lab, idx, box):
    return pl.pallas_call(
        head_kernel,
        out_shape=[
            pltpu.HBM((ROWS_ALL, 256), bf16),
            pltpu.HBM((HALF, 256), bf16),
            pltpu.HBM((HALF, 256), bf16),
            pltpu.VMEM((1, 128, 256), bf16),
        ],
        in_specs=[SMEM] * 2 + [VMEM] * 9,
        out_specs=[VMEM] * 4,
        scratch_shapes=[
            pltpu.VMEM((256, 2304), bf16),
            pltpu.VMEM((720, 256), f32),
            pltpu.VMEM((128, 128), f32),
            pltpu.VMEM((128, 128), f32),
            pltpu.VMEM((ROWS_ALL, 256), bf16),
            pltpu.VMEM((16, 768), f32),
            pltpu.VMEM((8, 128), f32),
            pltpu.VMEM((32, 128), jnp.int32),
            pltpu.VMEM((32, 128), jnp.int32),
        ],
        compiler_params=pltpu.CompilerParams(vmem_limit_bytes=LIMIT),
        name="head",
    )(first, ci, *near_memory([before]), own, *near_memory([after, w]), *far_memory([cb, bb, lab, idx, box]))


def tower_terms(g, w, after):
    return pl.pallas_call(
        tower_kernel,
        out_shape=(
            pltpu.VMEM((2, 128, 256), f32),
            pltpu.VMEM((1, 128, 256), bf16),
            pltpu.VMEM((1, 128, 256), bf16),
            shape(8, 128),
        ),
        in_specs=[VMEM, VMEM, ANY],
        out_specs=(VMEM, VMEM, VMEM, VMEM),
        compiler_params=pltpu.CompilerParams(vmem_limit_bytes=LIMIT),
        name="tower_terms",
        cost_estimate=pl.CostEstimate(flops=2 * 756 * 2304 * 256, transcendentals=0, bytes_accessed=4500000),
    )(*far_memory([g]), *near_memory([w]), after)


def tower_end(mid, above, below):
    return pl.pallas_call(
        tower_end_kernel,
        out_shape=(shape(1, 2, 128, 256, dtype=bf16), shape(8, 128)),
        in_specs=[VMEM] * 3,
        out_specs=(VMEM, VMEM),
        compiler_params=pltpu.CompilerParams(vmem_limit_bytes=LIMIT),
        name="tower_end",
    )(*near_memory([mid, above, below]))


def weight_terms(yi, xi, ci, keep, got, own, other, edge, other_edge):
    return pl.pallas_call(
        weight_kernel,
        out_shape=[pltpu.VMEM((4, PIECE, 128), bf16)] * 4 + [shape(8, 128)],
        in_specs=[SMEM] * 3 + [VMEM] * 6,
        out_specs=[VMEM] * 5,
        scratch_shapes=[
            pltpu.VMEM((6, 128, 256), bf16),
            pltpu.VMEM((3, 768, 256), bf16),
            pltpu.VMEM((2, HALF, 256), bf16),
            pltpu.VMEM((16, PIECE, 128), bf16),
        ],
        compiler_params=pltpu.CompilerParams(vmem_limit_bytes=LIMIT),
        name="weight_terms",
    )(yi, xi, ci, *far_memory([keep, got, own, other]), edge, other_edge)


def row_sum(yi, xi, ci, parts, after):
    return pl.pallas_call(
        row_sum_kernel,
        out_shape=[pltpu.VMEM((PIECE, 128), bf16)] * 4,
        in_specs=[SMEM] * 3 + [VMEM] * 4 + [ANY],
        out_specs=[VMEM] * 4,
        compiler_params=pltpu.CompilerParams(vmem_limit_bytes=LIMIT),
        name="row_sum",
    )(yi, xi, ci, *near_memory(parts), after)


def block_sum(parts):
    return pl.pallas_call(
        block_sum_kernel,
        out_shape=pltpu.VMEM((PIECE, 128), bf16),
        in_specs=[VMEM] * 4,
        out_specs=VMEM,
        compiler_params=pltpu.CompilerParams(vmem_limit_bytes=LIMIT),
        name="block_sum",
    )(*near_memory(parts))


def piece_sum(zi, m):
    return pl.pallas_call(
        piece_sum_kernel,
        out_shape=pltpu.VMEM((8, 56, 128), bf16),
        in_specs=[SMEM, VMEM],
        out_specs=VMEM,
        compiler_params=pltpu.CompilerParams(vmem_limit_bytes=LIMIT),
        name="piece_sum",
    )(zi, *near_memory([m]))


def join(parts):
    return pl.pallas_call(
        join_kernel,
        out_shape=pltpu.VMEM((4, PIECE, 128), bf16),
        in_specs=[VMEM] * 4,
        out_specs=VMEM,
        compiler_params=pltpu.CompilerParams(vmem_limit_bytes=LIMIT),
        name="join",
    )(*near_memory(parts))


def finish(yi, xi, ci, mine, other):
    return pl.pallas_call(
        final_kernel,
        out_shape=(shape(720, 2304), shape(36, 2304), shape(720), shape(36), shape(1, 128)),
        in_specs=[SMEM] * 3 + [VMEM] * 8,
        out_specs=(ANY, VMEM, VMEM, VMEM, VMEM),
        scratch_shapes=[
            pltpu.VMEM((ROWS_ALL, 2304), f32),
            pltpu.VMEM((32, 8, 128), f32),
            pltpu.VMEM((8, 896), f32),
            pltpu.SemaphoreType.DMA,
        ],
        compiler_params=pltpu.CompilerParams(vmem_limit_bytes=LIMIT),
        name="finish",
    )(yi, xi, ci, *near_memory([*mine, *other]))


def swap(value):
    return lax.ppermute(value, "core", [(0, 1), (1, 0)])


def along(value, k, first_axis):
    pairs = []
    for y in range(4):
        for c in range(2):
            for x in range(4):
                dx = k if (first_axis == "x") == (c == 0) else 0
                dy = k - dx
                pairs.append(((y * 2 + c) * 4 + x, (((y + dy) % 4) * 2 + c) * 4 + (x + dx) % 4))
    return lax.ppermute(value, ("y", "core", "x"), pairs)


def per_device(tower, cls_weight, cls_bias, box_weight, box_bias, labels, target_index, boxes):
    own = tower[0]
    tiles = 32
    up = [(t, t + 1) for t in range(tiles - 1)]
    down = [(t + 1, t) for t in range(tiles - 1)]
    before = lax.ppermute(own[1:2], TILE_AXES, up)
    after = lax.ppermute(own[0:1], TILE_AXES, down)
    own_other = swap(own)
    ci = lax.axis_index("core").reshape(1)
    yi = lax.axis_index("y").reshape(1)
    xi = lax.axis_index("x").reshape(1)
    zi = (lax.axis_index("zhi") * 4 + lax.axis_index("zlo")).reshape(1)
    first = (lax.axis_index(TILE_AXES) * 2).reshape(1)

    w = stage(cls_weight, box_weight)
    g, keep, send, edge = head(
        first, ci, before, own, after, w, cls_bias, box_bias, labels[0], target_index[0], boxes[0]
    )
    *parts, token = weight_terms(yi, xi, ci, keep, swap(send), own, own_other, edge, swap(edge))

    mid, to_up, to_down, _ = tower_terms(g, w, token)
    below = lax.ppermute(to_up, TILE_AXES, down)
    above = lax.ppermute(to_down, TILE_AXES, up)
    tower_grad, end_token = tower_end(mid, above, below)

    parts = [parts[0]] + [along(parts[k], k, "y") for k in (1, 2, 3)]
    parts = row_sum(yi, xi, ci, parts, end_token)
    parts = [parts[0]] + [along(parts[k], k, "x") for k in (1, 2, 3)]
    terms = lax.all_to_all(block_sum(parts).reshape(8, 56, 128), ("zhi", "zlo"), 0, 0, tiled=True)
    copies = lax.all_to_all(piece_sum(zi, terms), ("zhi", "zlo"), 0, 0, tiled=True)
    block = copies.reshape(PIECE, 128)
    row = join([block] + [along(block, k, "x") for k in (1, 2, 3)])
    mine = [row] + [along(row, k, "y") for k in (1, 2, 3)]
    other = [swap(v) for v in mine]
    cw_grad, bw_grad, cb_grad, bb_grad, loss = finish(yi, xi, ci, mine, other)
    return loss[0, 0], cw_grad, cb_grad, bw_grad, bb_grad, tower_grad


def solution(mesh):
    fine = Mesh(mesh.devices.reshape(4, 4, 2, 4, 2), ("zlo", "y", "core", "x", "zhi"))
    placed = (
        P(IMG_AXES, TILE_AXES, None, None),
        P(),
        P(),
        P(),
        P(),
        P(IMG_AXES, None, TILE_AXES, None),
        P(IMG_AXES, None, TILE_AXES, None),
        P(IMG_AXES, None, None),
    )
    return jax.shard_map(
        per_device,
        mesh=fine,
        in_specs=placed,
        out_specs=(P(), P(), P(), P(), P(), P(IMG_AXES, TILE_AXES, None, None)),
        check_vma=False,
    )
```

```python
import jax
import jax.numpy as jnp
from jax import lax
from jax.experimental import pallas as pl
from jax.experimental.pallas import tpu as pltpu
from jax.sharding import Mesh, PartitionSpec as P

CLASSES = 80
ANCHORS = 9
STRIDE = 8
FOCAL_ALPHA = 0.25
NORM_EPS = 1e-06

ROWS_ALL = 768
VALID = 756
HALF = 384
GROUP_ROWS = 96
BLOCK = 24
TILES = 56
PIECE = 448

LIMIT = 24 << 20

TILE_AXES = ("zlo", "y", "core")
IMG_AXES = ("x", "zhi")

f32 = jnp.float32
bf16 = jnp.bfloat16


def dot(a, b, dims):
    return lax.dot_general(a, b, (dims, ((), ())), preferred_element_type=f32)


def shifted(x, j):
    if j == 1:
        return x
    ids = lax.broadcasted_iota(jnp.int32, x.shape, 0)
    if j == 0:
        return jnp.where(ids == 0, 0.0, pltpu.roll(x, 1, 0))
    return jnp.where(ids == x.shape[0] - 1, 0.0, pltpu.roll(x, x.shape[0] - 1, 0))


def fill_patches(rows, p_ref, base):
    for e, row in enumerate(rows):
        x = row.astype(f32)
        for j in range(3):
            v = shifted(x, j).astype(bf16)
            for i in range(3):
                r = e - i
                if 0 <= r < 2:
                    p_ref[base + r * 128 : base + r * 128 + 128, (3 * i + j) * 256 : (3 * i + j) * 256 + 256] = v


def anchor_sizes(shape):
    ids = lax.broadcasted_iota(jnp.int32, shape, 0)
    w = jnp.ones(shape, f32)
    h = jnp.ones(shape, f32)
    for a in range(ANCHORS):
        base = 4.0 * STRIDE * 2.0 ** ((a // 3) / 3.0)
        ratio = a % 3 - 1
        w = jnp.where(ids == a, base * 2.0 ** (-ratio / 2.0), w)
        h = jnp.where(ids == a, base * 2.0 ** (ratio / 2.0), h)
    return w, h


def giou_terms(o0, o1, o2, o3, aw, ah, cx, cy, tl, tt, tr, tb):
    mx = cx + o0 * aw
    my = cy + o1 * ah
    pw = aw * jnp.exp(o2)
    ph = ah * jnp.exp(o3)
    left = mx - 0.5 * pw
    right = mx + 0.5 * pw
    top = my - 0.5 * ph
    bottom = my + 0.5 * ph
    iw = jnp.maximum(jnp.minimum(right, tr) - jnp.maximum(left, tl), 0.0)
    ih = jnp.maximum(jnp.minimum(bottom, tb) - jnp.maximum(top, tt), 0.0)
    inter = iw * ih
    union = pw * ph + (tr - tl) * (tb - tt) - inter
    ow = jnp.maximum(right, tr) - jnp.minimum(left, tl)
    oh = jnp.maximum(bottom, tb) - jnp.minimum(top, tt)
    outer = ow * oh
    return 1.0 - (inter / union - (outer - union) / outer)


def stage_kernel(cw, bw, w_ref, sem):
    copy = pltpu.make_async_copy(cw, w_ref.at[pl.ds(0, 720)], sem)
    copy.start()
    w_ref[752:768, :] = jnp.zeros((16, 2304), bf16)
    w_ref[720:756, :] = bw[...]
    copy.wait()


def head_kernel(first, ci, before, own, after, w, cb, bb, lab, idx, box, *refs):
    g_out, keep, send, edge = refs[0:4]
    p_ref, o_ref, b_ref, gb_ref, g_ref, row_ref, box_ref, lab_ref, idx_ref = refs[4:]
    edge[0] = jnp.where(jnp.full((128, 256), ci[0], jnp.int32) == 0, before[1], after[0])
    fill_patches([before[1], own[0], own[1], after[0]], p_ref, 0)
    row_ref[0, 0:720] = cb[...]
    row_ref[8, 0:36] = bb[...]
    column = row_ref[0:8, :].T[:, 0:1]
    box_column = row_ref[8:16, 0:128].T[:, 0:1]
    box_ref[0:4, 0:100] = box[...]
    lab_ref[...] = jnp.full((32, 128), -2, jnp.int32)
    idx_ref[...] = jnp.zeros((32, 128), jnp.int32)
    for r in range(2):
        for a in range(ANCHORS):
            lab_ref[r * 16 + a : r * 16 + a + 1, :] = lab[a, r : r + 1, :]
            idx_ref[r * 16 + a : r * 16 + a + 1, :] = idx[a, r : r + 1, :]
    p = p_ref[...]
    out = dot(w[...], p, ((1,), (1,)))
    o_ref[...] = out[0:720] + column[0:720]
    small_out = out[720:756] + box_column[0:36]
    for r in range(2):
        b_ref[r * 64 + 32 : r * 64 + 64, :] = jnp.zeros((32, 128), f32)
        b_ref[r * 64 : r * 64 + 36, :] = small_out[:, r * 128 : r * 128 + 128]
    cls = lax.broadcasted_iota(jnp.int32, (CLASSES, 128), 0)

    def one_anchor(a, carry):
        sums = []
        at = pl.multiple_of(a * CLASSES, 16)
        for r in range(2):
            label = lab_ref[pl.ds(r * 16 + a, 1), :]
            x = o_ref[pl.ds(at, CLASSES), r * 128 : r * 128 + 128]
            hit = label == cls
            z = jnp.where(hit, -x, x)
            e = jnp.exp(-jnp.abs(z))
            soft = jnp.maximum(z, 0.0) + jnp.log1p(e)
            big = 1.0 / (1.0 + e)
            small = e * big
            up = z >= 0.0
            q = jnp.where(up, big, small)
            rest = jnp.where(up, small, big)
            counted = (label >= -1).astype(f32)
            w = jnp.where(hit, FOCAL_ALPHA, 1.0 - FOCAL_ALPHA) * counted
            wq = w * q * q
            dz = wq * (q + 2.0 * rest * soft)
            g_ref[pl.ds(at, CLASSES), r * 128 : r * 128 + 128] = jnp.where(hit, -dz, dz).astype(bf16)
            sums.append(carry[r] + jnp.sum(wq * soft, axis=0, keepdims=True))
        return tuple(sums)

    zero = jnp.zeros((1, 128), f32)
    focal = lax.fori_loop(0, ANCHORS, one_anchor, (zero, zero))

    aw, ah = anchor_sizes((16, 128))
    cx = (lax.broadcasted_iota(jnp.int32, (16, 128), 1).astype(f32) + 0.5) * STRIDE
    for r in range(2):
        cy = (jnp.full((16, 128), first[0] + r, jnp.int32).astype(f32) + 0.5) * STRIDE
        which = idx_ref[r * 16 : r * 16 + 16, :]
        corner = [
            jnp.take_along_axis(jnp.broadcast_to(box_ref[k : k + 1, :], (16, 128)), which, axis=1) for k in range(4)
        ]
        positive = lab_ref[r * 16 : r * 16 + 16, :] >= 0
        o = [b_ref[pl.ds(r * 64 + k, 16, stride=4), :] for k in range(4)]
        value, pull = jax.vjp(
            lambda o0, o1, o2, o3: giou_terms(o0, o1, o2, o3, aw, ah, cx, cy, *corner), *o
        )
        grads = pull(jnp.ones((16, 128), f32))
        for k in range(4):
            gb_ref[pl.ds(r * 64 + k, 16, stride=4), :] = jnp.where(positive, grads[k], 0.0)
        giou = jnp.sum(jnp.where(positive, value, 0.0), axis=0, keepdims=True)
        count = jnp.sum(positive.astype(f32), axis=0, keepdims=True)
        rows = []
        for v in (focal[r], giou):
            hi = v.astype(bf16).astype(f32)
            rows += [hi, v - hi]
        rows.append(count)
        for n, v in enumerate(rows):
            gb_ref[r * 64 + 36 + n : r * 64 + 37 + n, :] = v
        g_ref[720:768, r * 128 : r * 128 + 128] = gb_ref[r * 64 : r * 64 + 48, :].astype(bf16)
    g_out[...] = g_ref[...]
    keep[...] = g_ref[pl.ds(pl.multiple_of(ci[0] * HALF, 16), HALF), :]
    send[...] = g_ref[pl.ds(pl.multiple_of((1 - ci[0]) * HALF, 16), HALF), :]


def tower_kernel(g, w_ref, unused, mid, up, down, token):
    token[...] = jnp.zeros((8, 128), f32)
    gt = g[...].astype(f32).T
    gj = []
    for j in range(3):
        gj.append(
            jnp.concatenate([shifted(gt[r * 128 : r * 128 + 128], 2 - j) for r in range(2)], axis=0).astype(bf16)
        )
    t = []
    for i in range(3):
        acc = jnp.zeros((256, 256), f32)
        for j in range(3):
            at = (3 * i + j) * 256
            acc = acc + dot(gj[j], w_ref[:, at : at + 256], ((1,), (0,)))
        t.append(acc)
    up[0] = t[0][0:128].astype(bf16)
    mid[0] = t[1][0:128] + t[0][128:256]
    mid[1] = t[1][128:256] + t[2][0:128]
    down[0] = t[2][128:256].astype(bf16)


def tower_end_kernel(mid, above, below, t_ref, token):
    token[...] = jnp.zeros((8, 128), f32)
    t_ref[0, 0] = (mid[0] + above[0].astype(f32)).astype(bf16)
    t_ref[0, 1] = (mid[1] + below[0].astype(f32)).astype(bf16)


def weight_kernel(yi, xi, ci, keep, got, before, own, after, other_edge, *refs):
    outs = refs[0:4]
    token, t_ref, s_ref, g_ref, m_ref = refs[4:]
    token[...] = jnp.zeros((8, 128), f32)
    c = ci[0]
    t_ref[5 - 5 * c] = other_edge[0]
    for r in range(2):
        t_ref[1 + 2 * c + r] = own[r]

    @pl.when(c == 0)
    def _():
        t_ref[0] = before[1]
        t_ref[3] = after[0]
        t_ref[4] = after[1]

    @pl.when(c == 1)
    def _():
        t_ref[1] = before[0]
        t_ref[2] = before[1]
        t_ref[5] = after[0]

    g_ref[c] = keep[...]
    g_ref[1 - c] = got[...]

    def shift(row, carry):
        x = t_ref[row].astype(f32)
        at = pl.multiple_of(row * 128, 128)
        for j in range(3):
            s_ref[j, pl.ds(at, 128), :] = shifted(x, j).astype(bf16)
        return carry

    lax.fori_loop(0, 6, shift, 0)
    lhs = jnp.concatenate([g_ref[0], g_ref[1]], axis=1)
    for tap in range(9):
        i, j = divmod(tap, 3)
        acc = dot(lhs, s_ref[j, i * 128 : i * 128 + 512, :], ((1,), (0,)))
        for m in range(16):
            for rb in range(3):
                row = m * BLOCK + rb * 8
                both = jnp.concatenate([acc[row : row + 8, 0:128], acc[row : row + 8, 128:256]], axis=0)
                v = (rb * 18 + 2 * tap) * 8
                m_ref[m, v : v + 16, :] = both.astype(bf16)
    bias = dot(jnp.ones((8, 512), bf16), lhs, ((1,), (1,)))
    for m in range(16):
        tile, off = divmod(m * BLOCK, 128)
        e = bias[:, tile * 128 : tile * 128 + 128]
        e = e if off == 0 else pltpu.roll(e, 128 - off, 1)
        if off + BLOCK > 128:
            past = pltpu.roll(bias[:, tile * 128 + 128 : tile * 128 + 256], 128 - off, 1)
            lane = lax.broadcasted_iota(jnp.int32, (8, 128), 1)
            e = jnp.where(lane < 128 - off, e, past)
        hi = e.astype(bf16).astype(f32)
        m_ref[m, 432:448, :] = jnp.concatenate([hi, e - hi], axis=0).astype(bf16)
    for k in range(4):
        for q in range(4):
            outs[k][q] = m_ref[jnp.where(c == 0, ((yi[0] + k) & 3) * 4 + q, q * 4 + ((xi[0] + k) & 3))]


def row_sum_kernel(yi, xi, ci, *refs):
    parts = refs[0:4]
    outs = refs[5:9]
    here = jnp.where(ci[0] == 0, xi[0], yi[0])
    for k in range(4):
        q = (here + k) & 3
        acc = parts[0][q].astype(f32)
        for n in range(1, 4):
            acc = acc + parts[n][q].astype(f32)
        e = acc[432:440] + acc[440:448]
        hi = e.astype(bf16).astype(f32)
        outs[k][0:432, :] = acc[0:432].astype(bf16)
        outs[k][432:448, :] = jnp.concatenate([hi, e - hi], axis=0).astype(bf16)


def block_sum_kernel(zi, a, b, c, d, unused, s_ref):
    acc = (a[...].astype(f32) + b[...].astype(f32)) + (c[...].astype(f32) + d[...].astype(f32))
    e = acc[432:440] + acc[440:448]
    hi = e.astype(bf16).astype(f32)
    s_ref[0:432, :] = acc[0:432].astype(bf16)
    s_ref[432:448, :] = jnp.concatenate([hi, e - hi], axis=0).astype(bf16)


def piece_sum_kernel(zi, m_ref, c_ref):
    acc = m_ref[0].astype(f32)
    for m in range(1, 8):
        acc = acc + m_ref[m].astype(f32)
    last = jnp.full((8, 128), zi[0], jnp.int32) == 7
    e = acc[40:48] + acc[48:56]
    hi = e.astype(bf16).astype(f32)
    out = jnp.concatenate(
        [acc[0:40], jnp.where(last, hi, acc[40:48]), jnp.where(last, e - hi, acc[48:56])], axis=0
    ).astype(bf16)
    for z in range(8):
        c_ref[z] = out


def join_kernel(a, b, c, d, o_ref):
    for k, ref in enumerate((a, b, c, d)):
        o_ref[k] = ref[...]


LAST = 5


def block_of(yi, xi, ci, n, k):
    c = ci[0] if n < 4 else 1 - ci[0]
    far = n % 4
    y = (yi[0] - jnp.where(c == 0, far, k)) & 3
    x = (xi[0] - jnp.where(c == 0, k, far)) & 3
    return c * 16 + y * 4 + x


def squares(yi, xi, ci, n, src):
    srow = lax.broadcasted_iota(jnp.int32, (8, 128), 0)
    lane = lax.broadcasted_iota(jnp.int32, (8, 128), 1)

    def one(k, total):
        base = block_of(yi, xi, ci, n, k) * BLOCK
        for rb in range(3):
            acc = jnp.zeros((16, 128), f32)
            for t in range(9):
                v = src[k, (rb * 9 + t) * 16 : (rb * 9 + t) * 16 + 16, :].astype(f32)
                acc = acc + v * v
            ok = base + rb * 8 + srow < VALID
            total = total + jnp.where(ok, acc[0:8] + acc[8:16], 0.0)
        e = src[k, 432:448, :].astype(f32)
        e = e[0:8] + e[8:16]
        ok = (base + lane < VALID) & (lane < BLOCK) & (srow == 0)
        return total + jnp.where(ok, e * e, 0.0)

    return one


def squares_kernel(yi, xi, ci, *refs):
    total = jnp.zeros((8, 128), f32)
    for n, src in zip([n for n in range(8) if n != LAST], refs[:7]):
        total = lax.fori_loop(0, 4, squares(yi, xi, ci, n, src), total)
    refs[7][...] = total


def final_kernel(yi, xi, ci, *refs):
    sources = refs[0:8]
    partial, cw_out, bw_out, cb_out, bb_out, loss, w_ref, e_ref, row_ref, sem = refs[8:]
    srow = lax.broadcasted_iota(jnp.int32, (8, 128), 0)
    lane = lax.broadcasted_iota(jnp.int32, (8, 128), 1)
    total = lax.fori_loop(0, 4, squares(yi, xi, ci, LAST, sources[LAST]), partial[...])
    mean = jnp.sum(total) * (1.0 / (VALID * 2305))
    scale = lax.rsqrt(jnp.full((8, 128), mean + NORM_EPS, f32))

    def chunk(block):
        rows = pl.ds(pl.multiple_of(block * BLOCK, 8), BLOCK)
        return pltpu.make_async_copy(w_ref.at[rows], cw_out.at[rows], sem)

    def write(n):
        src = sources[n]

        def one(k, carry):
            block = block_of(yi, xi, ci, n, k)
            e = src[k, 432:448, :].astype(f32)
            e_ref[block] = e[0:8] + e[8:16]
            for rb in range(3):
                row = pl.multiple_of(block * BLOCK + rb * 8, 8)
                for t in range(9):
                    v = src[k, (rb * 9 + t) * 16 : (rb * 9 + t) * 16 + 16, :].astype(f32)
                    w_ref[pl.ds(row, 8), t * 256 : t * 256 + 128] = v[0:8] * scale
                    w_ref[pl.ds(row, 8), t * 256 + 128 : t * 256 + 256] = v[8:16] * scale

            @pl.when(block < 30)
            def _():
                chunk(block).start()

            return carry

        return one

    for n in range(8):
        lax.fori_loop(0, 4, write(n), 0)
    bw_out[...] = w_ref[720:756, :]
    row_ref[...] = jnp.zeros((8, 896), f32)
    for block in range(32):
        tile, off = divmod(block * BLOCK, 128)
        e = e_ref[block] * scale
        e = e if off == 0 else pltpu.roll(e, off, 1)
        here = (lane >= off) & (lane < off + BLOCK)
        row_ref[:, tile * 128 : tile * 128 + 128] = jnp.where(here, e, row_ref[:, tile * 128 : tile * 128 + 128])
        if off + BLOCK > 128:
            past = lane < off + BLOCK - 128
            row_ref[:, tile * 128 + 128 : tile * 128 + 256] = jnp.where(past, e, 0.0)
    cb_out[...] = row_ref[0, 0:720]
    bb_out[...] = pltpu.roll(row_ref[:, 640:768], 128 - 80, 1)[0, 0:36]
    e = jnp.where(srow == 0, e_ref[31], 0.0)
    sums = jnp.sum(jnp.where((lane >= 12) & (lane < 16), e, 0.0))
    count = jnp.sum(jnp.where(lane == 16, e, 0.0))
    loss[...] = jnp.full((1, 128), sums, f32) / jnp.full((1, 128), count, f32)

    def drain(k, carry):
        chunk(k).wait()
        return carry

    lax.fori_loop(0, 30, drain, 0)


VMEM = pl.BlockSpec(memory_space=pltpu.VMEM)
SMEM = pl.BlockSpec(memory_space=pltpu.SMEM)
ANY = pl.BlockSpec(memory_space=pl.ANY)


def near_memory(arrays):
    return [pltpu.with_memory_space_constraint(v, pltpu.VMEM) for v in arrays]


def far_memory(arrays):
    return [pltpu.with_memory_space_constraint(v, pltpu.HBM) for v in arrays]


def shape(*dims, dtype=f32):
    return jax.ShapeDtypeStruct(dims, dtype)


def stage(cw, bw):
    return pl.pallas_call(
        stage_kernel,
        out_shape=pltpu.VMEM((ROWS_ALL, 2304), bf16),
        in_specs=[ANY, VMEM],
        out_specs=VMEM,
        scratch_shapes=[pltpu.SemaphoreType.DMA],
        compiler_params=pltpu.CompilerParams(vmem_limit_bytes=LIMIT),
        name="stage",
    )(*far_memory([cw, bw]))


def head(first, ci, before, own, after, w, cb, bb, lab, idx, box):
    return pl.pallas_call(
        head_kernel,
        out_shape=[
            pltpu.HBM((ROWS_ALL, 256), bf16),
            pltpu.HBM((HALF, 256), bf16),
            pltpu.HBM((HALF, 256), bf16),
            pltpu.VMEM((1, 128, 256), bf16),
        ],
        in_specs=[SMEM] * 2 + [VMEM] * 9,
        out_specs=[VMEM] * 4,
        scratch_shapes=[
            pltpu.VMEM((256, 2304), bf16),
            pltpu.VMEM((720, 256), f32),
            pltpu.VMEM((128, 128), f32),
            pltpu.VMEM((128, 128), f32),
            pltpu.VMEM((ROWS_ALL, 256), bf16),
            pltpu.VMEM((16, 768), f32),
            pltpu.VMEM((8, 128), f32),
            pltpu.VMEM((32, 128), jnp.int32),
            pltpu.VMEM((32, 128), jnp.int32),
        ],
        compiler_params=pltpu.CompilerParams(vmem_limit_bytes=LIMIT),
        name="head",
    )(first, ci, *far_memory([before, own, after]), *near_memory([w]), *far_memory([cb, bb, lab, idx, box]))


def tower_terms(g, w, after):
    return pl.pallas_call(
        tower_kernel,
        out_shape=(
            pltpu.HBM((2, 128, 256), f32),
            pltpu.VMEM((1, 128, 256), bf16),
            pltpu.VMEM((1, 128, 256), bf16),
            shape(8, 128),
        ),
        in_specs=[VMEM, VMEM, ANY],
        out_specs=(VMEM, VMEM, VMEM, VMEM),
        compiler_params=pltpu.CompilerParams(vmem_limit_bytes=LIMIT),
        name="tower_terms",
        cost_estimate=pl.CostEstimate(flops=2 * 756 * 2304 * 256, transcendentals=0, bytes_accessed=4500000),
    )(*far_memory([g]), *near_memory([w]), after)


def tower_end(mid, above, below):
    return pl.pallas_call(
        tower_end_kernel,
        out_shape=(shape(1, 2, 128, 256, dtype=bf16), shape(8, 128)),
        in_specs=[VMEM] * 3,
        out_specs=(VMEM, VMEM),
        compiler_params=pltpu.CompilerParams(vmem_limit_bytes=LIMIT),
        name="tower_end",
    )(*far_memory([mid]), above, below)


def weight_terms(yi, xi, ci, keep, got, before, own, after, other_edge):
    return pl.pallas_call(
        weight_kernel,
        out_shape=[pltpu.VMEM((4, PIECE, 128), bf16)] * 4 + [shape(8, 128)],
        in_specs=[SMEM] * 3 + [VMEM] * 6,
        out_specs=[VMEM] * 5,
        scratch_shapes=[
            pltpu.VMEM((6, 128, 256), bf16),
            pltpu.VMEM((3, 768, 256), bf16),
            pltpu.VMEM((2, HALF, 256), bf16),
            pltpu.VMEM((16, PIECE, 128), bf16),
        ],
        compiler_params=pltpu.CompilerParams(vmem_limit_bytes=LIMIT),
        name="weight_terms",
    )(yi, xi, ci, *far_memory([keep, got, before, own, after]), other_edge)


def row_sum(yi, xi, ci, parts, after):
    return pl.pallas_call(
        row_sum_kernel,
        out_shape=[pltpu.VMEM((PIECE, 128), bf16)] * 4,
        in_specs=[SMEM] * 3 + [VMEM] * 4 + [ANY],
        out_specs=[VMEM] * 4,
        compiler_params=pltpu.CompilerParams(vmem_limit_bytes=LIMIT),
        name="row_sum",
    )(yi, xi, ci, *near_memory(parts), after)


def block_sum(zi, parts, after):
    return pl.pallas_call(
        block_sum_kernel,
        out_shape=pltpu.VMEM((PIECE, 128), bf16),
        in_specs=[SMEM] + [VMEM] * 4 + [ANY],
        out_specs=VMEM,
        compiler_params=pltpu.CompilerParams(vmem_limit_bytes=LIMIT),
        name="block_sum",
    )(zi, *near_memory(parts), after)


def piece_sum(zi, m):
    return pl.pallas_call(
        piece_sum_kernel,
        out_shape=pltpu.VMEM((8, 56, 128), bf16),
        in_specs=[SMEM, VMEM],
        out_specs=VMEM,
        compiler_params=pltpu.CompilerParams(vmem_limit_bytes=LIMIT),
        name="piece_sum",
    )(zi, *near_memory([m]))


def join(parts):
    return pl.pallas_call(
        join_kernel,
        out_shape=pltpu.VMEM((4, PIECE, 128), bf16),
        in_specs=[VMEM] * 4,
        out_specs=VMEM,
        compiler_params=pltpu.CompilerParams(vmem_limit_bytes=LIMIT),
        name="join",
    )(*near_memory(parts))


def squares_of(yi, xi, ci, pieces):
    return pl.pallas_call(
        squares_kernel,
        out_shape=pltpu.VMEM((8, 128), f32),
        in_specs=[SMEM] * 3 + [VMEM] * 7,
        out_specs=VMEM,
        compiler_params=pltpu.CompilerParams(vmem_limit_bytes=LIMIT),
        name="squares",
    )(yi, xi, ci, *near_memory(pieces))


def finish(yi, xi, ci, pieces, partial):
    return pl.pallas_call(
        final_kernel,
        out_shape=(shape(720, 2304), shape(36, 2304), shape(720), shape(36), shape(1, 128)),
        in_specs=[SMEM] * 3 + [VMEM] * 9,
        out_specs=(ANY, VMEM, VMEM, VMEM, VMEM),
        scratch_shapes=[
            pltpu.VMEM((ROWS_ALL, 2304), f32),
            pltpu.VMEM((32, 8, 128), f32),
            pltpu.VMEM((8, 896), f32),
            pltpu.SemaphoreType.DMA,
        ],
        compiler_params=pltpu.CompilerParams(vmem_limit_bytes=LIMIT),
        name="finish",
    )(yi, xi, ci, *near_memory([*pieces, partial]))


def swap(value):
    return lax.ppermute(value, "core", [(0, 1), (1, 0)])


def along(value, k, first_axis):
    pairs = []
    for y in range(4):
        for c in range(2):
            for x in range(4):
                dx = k if (first_axis == "x") == (c == 0) else 0
                dy = k - dx
                pairs.append(((y * 2 + c) * 4 + x, (((y + dy) % 4) * 2 + c) * 4 + (x + dx) % 4))
    return lax.ppermute(value, ("y", "core", "x"), pairs)


def per_device(tower, cls_weight, cls_bias, box_weight, box_bias, labels, target_index, boxes):
    own = tower[0]
    tiles = 32
    up = [(t, t + 1) for t in range(tiles - 1)]
    down = [(t + 1, t) for t in range(tiles - 1)]
    before = lax.ppermute(own, TILE_AXES, up)
    after = lax.ppermute(own, TILE_AXES, down)
    ci = lax.axis_index("core").reshape(1)
    yi = lax.axis_index("y").reshape(1)
    xi = lax.axis_index("x").reshape(1)
    zi = (lax.axis_index("zhi") * 4 + lax.axis_index("zlo")).reshape(1)
    first = (lax.axis_index(TILE_AXES) * 2).reshape(1)

    w = stage(cls_weight, box_weight)
    g, keep, send, edge = head(
        first, ci, before, own, after, w, cls_bias, box_bias, labels[0], target_index[0], boxes[0]
    )
    *parts, token = weight_terms(yi, xi, ci, keep, swap(send), before, own, after, swap(edge))

    mid, to_up, to_down, tower_token = tower_terms(g, w, token)
    below = lax.ppermute(to_up, TILE_AXES, down)
    above = lax.ppermute(to_down, TILE_AXES, up)
    tower_grad, end_token = tower_end(mid, above, below)

    parts = [parts[0]] + [along(parts[k], k, "y") for k in (1, 2, 3)]
    parts = row_sum(yi, xi, ci, parts, tower_token)
    parts = [parts[0]] + [along(parts[k], k, "x") for k in (1, 2, 3)]
    terms = lax.all_to_all(block_sum(zi, parts, end_token).reshape(8, 56, 128), ("zhi", "zlo"), 0, 0, tiled=True)
    copies = lax.all_to_all(piece_sum(zi, terms), ("zhi", "zlo"), 0, 0, tiled=True)
    block = copies.reshape(PIECE, 128)
    row = join([block] + [along(block, k, "x") for k in (1, 2, 3)])
    mine = [row] + [along(row, k, "y") for k in (1, 2, 3)]
    pieces = mine + [swap(v) for v in mine]
    partial = squares_of(yi, xi, ci, pieces[:LAST] + pieces[LAST + 1 :])
    cw_grad, bw_grad, cb_grad, bb_grad, loss = finish(yi, xi, ci, pieces, partial)
    return loss[0, 0], cw_grad, cb_grad, bw_grad, bb_grad, tower_grad


def solution(mesh):
    fine = Mesh(mesh.devices.reshape(4, 4, 2, 4, 2), ("zlo", "y", "core", "x", "zhi"))
    placed = (
        P(IMG_AXES, TILE_AXES, None, None),
        P(),
        P(),
        P(),
        P(),
        P(IMG_AXES, None, TILE_AXES, None),
        P(IMG_AXES, None, TILE_AXES, None),
        P(IMG_AXES, None, None),
    )
    return jax.shard_map(
        per_device,
        mesh=fine,
        in_specs=placed,
        out_specs=(P(), P(), P(), P(), P(), P(IMG_AXES, TILE_AXES, None, None)),
        check_vma=False,
    )
```

```python
import jax
import jax.numpy as jnp
from jax import lax
from jax.experimental import pallas as pl
from jax.experimental.pallas import tpu as pltpu
from jax.sharding import Mesh, PartitionSpec as P

CLASSES = 80
ANCHORS = 9
STRIDE = 8
FOCAL_ALPHA = 0.25
NORM_EPS = 1e-06

ROWS_ALL = 768
VALID = 756
HALF = 384
GROUP_ROWS = 96
BLOCK = 24
TILES = 56
PIECE = 448

LIMIT = 24 << 20

TILE_AXES = ("zlo", "y", "core")
IMG_AXES = ("x", "zhi")

f32 = jnp.float32
bf16 = jnp.bfloat16


def dot(a, b, dims):
    return lax.dot_general(a, b, (dims, ((), ())), preferred_element_type=f32)


def shifted(x, j):
    if j == 1:
        return x
    ids = lax.broadcasted_iota(jnp.int32, x.shape, 0)
    if j == 0:
        return jnp.where(ids == 0, 0.0, pltpu.roll(x, 1, 0))
    return jnp.where(ids == x.shape[0] - 1, 0.0, pltpu.roll(x, x.shape[0] - 1, 0))


def fill_patches(rows, p_ref, base):
    for e, row in enumerate(rows):
        x = row.astype(f32)
        for j in range(3):
            v = shifted(x, j).astype(bf16)
            for i in range(3):
                r = e - i
                if 0 <= r < 2:
                    p_ref[base + r * 128 : base + r * 128 + 128, (3 * i + j) * 256 : (3 * i + j) * 256 + 256] = v


def anchor_sizes(shape):
    ids = lax.broadcasted_iota(jnp.int32, shape, 0)
    w = jnp.ones(shape, f32)
    h = jnp.ones(shape, f32)
    for a in range(ANCHORS):
        base = 4.0 * STRIDE * 2.0 ** ((a // 3) / 3.0)
        ratio = a % 3 - 1
        w = jnp.where(ids == a, base * 2.0 ** (-ratio / 2.0), w)
        h = jnp.where(ids == a, base * 2.0 ** (ratio / 2.0), h)
    return w, h


def giou_terms(o0, o1, o2, o3, aw, ah, cx, cy, tl, tt, tr, tb):
    mx = cx + o0 * aw
    my = cy + o1 * ah
    pw = aw * jnp.exp(o2)
    ph = ah * jnp.exp(o3)
    left = mx - 0.5 * pw
    right = mx + 0.5 * pw
    top = my - 0.5 * ph
    bottom = my + 0.5 * ph
    iw = jnp.maximum(jnp.minimum(right, tr) - jnp.maximum(left, tl), 0.0)
    ih = jnp.maximum(jnp.minimum(bottom, tb) - jnp.maximum(top, tt), 0.0)
    inter = iw * ih
    union = pw * ph + (tr - tl) * (tb - tt) - inter
    ow = jnp.maximum(right, tr) - jnp.minimum(left, tl)
    oh = jnp.maximum(bottom, tb) - jnp.minimum(top, tt)
    outer = ow * oh
    return 1.0 - (inter / union - (outer - union) / outer)


def stage_kernel(cw, bw, w_ref, sem):
    copy = pltpu.make_async_copy(cw, w_ref.at[pl.ds(0, 720)], sem)
    copy.start()
    w_ref[752:768, :] = jnp.zeros((16, 2304), bf16)
    w_ref[720:756, :] = bw[...]
    copy.wait()


def head_kernel(first, ci, outer, own, inner, w, cb, bb, lab, idx, box, *refs):
    g_out, keep, send, edge = refs[0:4]
    p_ref, o_ref, b_ref, gb_ref, g_ref, row_ref, box_ref, lab_ref, idx_ref, ext_ref = refs[4:]
    c = ci[0]
    edge[0] = outer[1 - c]
    ext_ref[3 * c] = outer[1 - c]
    ext_ref[3 - 3 * c] = inner[c]
    fill_patches([ext_ref[0], own[0], own[1], ext_ref[3]], p_ref, 0)
    row_ref[0, 0:720] = cb[...]
    row_ref[8, 0:36] = bb[...]
    column = row_ref[0:8, :].T[:, 0:1]
    box_column = row_ref[8:16, 0:128].T[:, 0:1]
    box_ref[0:4, 0:100] = box[...]
    lab_ref[...] = jnp.full((32, 128), -2, jnp.int32)
    idx_ref[...] = jnp.zeros((32, 128), jnp.int32)
    for r in range(2):
        for a in range(ANCHORS):
            lab_ref[r * 16 + a : r * 16 + a + 1, :] = lab[a, r : r + 1, :]
            idx_ref[r * 16 + a : r * 16 + a + 1, :] = idx[a, r : r + 1, :]
    p = p_ref[...]
    out = dot(w[...], p, ((1,), (1,)))
    o_ref[...] = out[0:720] + column[0:720]
    small_out = out[720:756] + box_column[0:36]
    for r in range(2):
        b_ref[r * 64 + 32 : r * 64 + 64, :] = jnp.zeros((32, 128), f32)
        b_ref[r * 64 : r * 64 + 36, :] = small_out[:, r * 128 : r * 128 + 128]
    cls = lax.broadcasted_iota(jnp.int32, (CLASSES, 128), 0)

    def one_anchor(a, carry):
        sums = []
        at = pl.multiple_of(a * CLASSES, 16)
        for r in range(2):
            label = lab_ref[pl.ds(r * 16 + a, 1), :]
            x = o_ref[pl.ds(at, CLASSES), r * 128 : r * 128 + 128]
            hit = label == cls
            z = jnp.where(hit, -x, x)
            e = jnp.exp(-jnp.abs(z))
            soft = jnp.maximum(z, 0.0) + jnp.log1p(e)
            big = 1.0 / (1.0 + e)
            small = e * big
            up = z >= 0.0
            q = jnp.where(up, big, small)
            rest = jnp.where(up, small, big)
            counted = (label >= -1).astype(f32)
            w = jnp.where(hit, FOCAL_ALPHA, 1.0 - FOCAL_ALPHA) * counted
            wq = w * q * q
            dz = wq * (q + 2.0 * rest * soft)
            g_ref[pl.ds(at, CLASSES), r * 128 : r * 128 + 128] = jnp.where(hit, -dz, dz).astype(bf16)
            sums.append(carry[r] + jnp.sum(wq * soft, axis=0, keepdims=True))
        return tuple(sums)

    zero = jnp.zeros((1, 128), f32)
    focal = lax.fori_loop(0, ANCHORS, one_anchor, (zero, zero))

    aw, ah = anchor_sizes((16, 128))
    cx = (lax.broadcasted_iota(jnp.int32, (16, 128), 1).astype(f32) + 0.5) * STRIDE
    for r in range(2):
        cy = (jnp.full((16, 128), first[0] + r, jnp.int32).astype(f32) + 0.5) * STRIDE
        which = idx_ref[r * 16 : r * 16 + 16, :]
        corner = [
            jnp.take_along_axis(jnp.broadcast_to(box_ref[k : k + 1, :], (16, 128)), which, axis=1) for k in range(4)
        ]
        positive = lab_ref[r * 16 : r * 16 + 16, :] >= 0
        o = [b_ref[pl.ds(r * 64 + k, 16, stride=4), :] for k in range(4)]
        value, pull = jax.vjp(
            lambda o0, o1, o2, o3: giou_terms(o0, o1, o2, o3, aw, ah, cx, cy, *corner), *o
        )
        grads = pull(jnp.ones((16, 128), f32))
        for k in range(4):
            gb_ref[pl.ds(r * 64 + k, 16, stride=4), :] = jnp.where(positive, grads[k], 0.0)
        giou = jnp.sum(jnp.where(positive, value, 0.0), axis=0, keepdims=True)
        count = jnp.sum(positive.astype(f32), axis=0, keepdims=True)
        rows = []
        for v in (focal[r], giou):
            hi = v.astype(bf16).astype(f32)
            rows += [hi, v - hi]
        rows.append(count)
        for n, v in enumerate(rows):
            gb_ref[r * 64 + 36 + n : r * 64 + 37 + n, :] = v
        g_ref[720:768, r * 128 : r * 128 + 128] = gb_ref[r * 64 : r * 64 + 48, :].astype(bf16)
    g_out[...] = g_ref[...]
    keep[...] = g_ref[pl.ds(pl.multiple_of(ci[0] * HALF, 16), HALF), :]
    send[...] = g_ref[pl.ds(pl.multiple_of((1 - ci[0]) * HALF, 16), HALF), :]


def tower_kernel(ci, g, w_ref, unused, mid, outer, inner, token):
    token[...] = jnp.zeros((8, 128), f32)
    gt = g[...].astype(f32).T
    gj = []
    for j in range(3):
        gj.append(
            jnp.concatenate([shifted(gt[r * 128 : r * 128 + 128], 2 - j) for r in range(2)], axis=0).astype(bf16)
        )
    t = []
    for i in range(3):
        acc = jnp.zeros((256, 256), f32)
        for j in range(3):
            at = (3 * i + j) * 256
            acc = acc + dot(gj[j], w_ref[:, at : at + 256], ((1,), (0,)))
        t.append(acc)
    low = jnp.full((128, 256), ci[0], jnp.int32) == 0
    up = t[0][0:128]
    down = t[2][128:256]
    outer[0] = jnp.where(low, up, down).astype(bf16)
    inner[0] = jnp.where(low, down, up).astype(bf16)
    mid[0] = t[1][0:128] + t[0][128:256]
    mid[1] = t[1][128:256] + t[2][0:128]


def tower_end_kernel(ci, mid, outer, inner, t_ref, token):
    token[...] = jnp.zeros((8, 128), f32)
    c = ci[0]
    t_ref[0, c] = (mid[c] + outer[0].astype(f32)).astype(bf16)
    t_ref[0, 1 - c] = (mid[1 - c] + inner[0].astype(f32)).astype(bf16)


def weight_kernel(yi, xi, ci, keep, got, outer, own, inner, other_edge, *refs):
    outs = refs[0:4]
    token, t_ref, s_ref, g_ref, m_ref = refs[4:]
    token[...] = jnp.zeros((8, 128), f32)
    c = ci[0]
    t_ref[5 * c] = outer[1 - c]
    t_ref[5 - 5 * c] = other_edge[0]
    for r in range(2):
        t_ref[1 + 2 * c + r] = own[r]
        t_ref[3 - 2 * c + r] = inner[r]
    g_ref[c] = keep[...]
    g_ref[1 - c] = got[...]

    def shift(row, carry):
        x = t_ref[row].astype(f32)
        at = pl.multiple_of(row * 128, 128)
        for j in range(3):
            s_ref[j, pl.ds(at, 128), :] = shifted(x, j).astype(bf16)
        return carry

    lax.fori_loop(0, 6, shift, 0)
    lhs = jnp.concatenate([g_ref[0], g_ref[1]], axis=1)
    for tap in range(9):
        i, j = divmod(tap, 3)
        acc = dot(lhs, s_ref[j, i * 128 : i * 128 + 512, :], ((1,), (0,)))
        for m in range(16):
            for rb in range(3):
                row = m * BLOCK + rb * 8
                both = jnp.concatenate([acc[row : row + 8, 0:128], acc[row : row + 8, 128:256]], axis=0)
                v = (rb * 18 + 2 * tap) * 8
                m_ref[m, v : v + 16, :] = both.astype(bf16)
    bias = dot(jnp.ones((8, 512), bf16), lhs, ((1,), (1,)))
    for m in range(16):
        tile, off = divmod(m * BLOCK, 128)
        e = bias[:, tile * 128 : tile * 128 + 128]
        e = e if off == 0 else pltpu.roll(e, 128 - off, 1)
        if off + BLOCK > 128:
            past = pltpu.roll(bias[:, tile * 128 + 128 : tile * 128 + 256], 128 - off, 1)
            lane = lax.broadcasted_iota(jnp.int32, (8, 128), 1)
            e = jnp.where(lane < 128 - off, e, past)
        hi = e.astype(bf16).astype(f32)
        m_ref[m, 432:448, :] = jnp.concatenate([hi, e - hi], axis=0).astype(bf16)
    for k in range(4):
        for q in range(4):
            outs[k][q] = m_ref[jnp.where(c == 0, ((yi[0] + k) & 3) * 4 + q, q * 4 + ((xi[0] + k) & 3))]


def row_sum_kernel(yi, xi, ci, *refs):
    parts = refs[0:4]
    outs = refs[5:9]
    here = jnp.where(ci[0] == 0, xi[0], yi[0])
    for k in range(4):
        q = (here + k) & 3
        acc = parts[0][q].astype(f32)
        for n in range(1, 4):
            acc = acc + parts[n][q].astype(f32)
        e = acc[432:440] + acc[440:448]
        hi = e.astype(bf16).astype(f32)
        outs[k][0:432, :] = acc[0:432].astype(bf16)
        outs[k][432:448, :] = jnp.concatenate([hi, e - hi], axis=0).astype(bf16)


def block_sum_kernel(zi, a, b, c, d, s_ref):
    acc = (a[...].astype(f32) + b[...].astype(f32)) + (c[...].astype(f32) + d[...].astype(f32))
    e = acc[432:440] + acc[440:448]
    hi = e.astype(bf16).astype(f32)
    s_ref[0:432, :] = acc[0:432].astype(bf16)
    s_ref[432:448, :] = jnp.concatenate([hi, e - hi], axis=0).astype(bf16)


def piece_sum_kernel(zi, m_ref, c_ref):
    acc = m_ref[0].astype(f32)
    for m in range(1, 8):
        acc = acc + m_ref[m].astype(f32)
    last = jnp.full((8, 128), zi[0], jnp.int32) == 7
    e = acc[40:48] + acc[48:56]
    hi = e.astype(bf16).astype(f32)
    out = jnp.concatenate(
        [acc[0:40], jnp.where(last, hi, acc[40:48]), jnp.where(last, e - hi, acc[48:56])], axis=0
    ).astype(bf16)
    for z in range(8):
        c_ref[z] = out


def join_kernel(a, b, c, d, o_ref):
    for k, ref in enumerate((a, b, c, d)):
        o_ref[k] = ref[...]


LAST = 5


def block_of(yi, xi, ci, n, k):
    c = ci[0] if n < 4 else 1 - ci[0]
    far = n % 4
    y = (yi[0] - jnp.where(c == 0, far, k)) & 3
    x = (xi[0] - jnp.where(c == 0, k, far)) & 3
    return c * 16 + y * 4 + x


def squares(yi, xi, ci, n, src):
    srow = lax.broadcasted_iota(jnp.int32, (8, 128), 0)
    lane = lax.broadcasted_iota(jnp.int32, (8, 128), 1)

    def one(k, total):
        base = block_of(yi, xi, ci, n, k) * BLOCK
        for rb in range(3):
            acc = jnp.zeros((16, 128), f32)
            for t in range(9):
                v = src[k, (rb * 9 + t) * 16 : (rb * 9 + t) * 16 + 16, :].astype(f32)
                acc = acc + v * v
            ok = base + rb * 8 + srow < VALID
            total = total + jnp.where(ok, acc[0:8] + acc[8:16], 0.0)
        e = src[k, 432:448, :].astype(f32)
        e = e[0:8] + e[8:16]
        ok = (base + lane < VALID) & (lane < BLOCK) & (srow == 0)
        return total + jnp.where(ok, e * e, 0.0)

    return one


def squares_kernel(yi, xi, ci, *refs):
    total = jnp.zeros((8, 128), f32)
    for n, src in zip([n for n in range(8) if n != LAST], refs[:7]):
        total = lax.fori_loop(0, 4, squares(yi, xi, ci, n, src), total)
    refs[7][...] = total


def final_kernel(yi, xi, ci, *refs):
    sources = refs[0:8]
    partial, cw_out, bw_out, cb_out, bb_out, loss, w_ref, e_ref, row_ref, sem = refs[8:]
    srow = lax.broadcasted_iota(jnp.int32, (8, 128), 0)
    lane = lax.broadcasted_iota(jnp.int32, (8, 128), 1)
    total = lax.fori_loop(0, 4, squares(yi, xi, ci, LAST, sources[LAST]), partial[...])
    mean = jnp.sum(total) * (1.0 / (VALID * 2305))
    scale = lax.rsqrt(jnp.full((8, 128), mean + NORM_EPS, f32))

    def chunk(block):
        rows = pl.ds(pl.multiple_of(block * BLOCK, 8), BLOCK)
        return pltpu.make_async_copy(w_ref.at[rows], cw_out.at[rows], sem)

    def write(n):
        src = sources[n]

        def one(k, carry):
            block = block_of(yi, xi, ci, n, k)
            e = src[k, 432:448, :].astype(f32)
            e_ref[block] = e[0:8] + e[8:16]
            for rb in range(3):
                row = pl.multiple_of(block * BLOCK + rb * 8, 8)
                for t in range(9):
                    v = src[k, (rb * 9 + t) * 16 : (rb * 9 + t) * 16 + 16, :].astype(f32)
                    w_ref[pl.ds(row, 8), t * 256 : t * 256 + 128] = v[0:8] * scale
                    w_ref[pl.ds(row, 8), t * 256 + 128 : t * 256 + 256] = v[8:16] * scale

            @pl.when(block < 30)
            def _():
                chunk(block).start()

            return carry

        return one

    for n in range(8):
        lax.fori_loop(0, 4, write(n), 0)
    bw_out[...] = w_ref[720:756, :]
    row_ref[...] = jnp.zeros((8, 896), f32)
    for block in range(32):
        tile, off = divmod(block * BLOCK, 128)
        e = e_ref[block] * scale
        e = e if off == 0 else pltpu.roll(e, off, 1)
        here = (lane >= off) & (lane < off + BLOCK)
        row_ref[:, tile * 128 : tile * 128 + 128] = jnp.where(here, e, row_ref[:, tile * 128 : tile * 128 + 128])
        if off + BLOCK > 128:
            past = lane < off + BLOCK - 128
            row_ref[:, tile * 128 + 128 : tile * 128 + 256] = jnp.where(past, e, 0.0)
    cb_out[...] = row_ref[0, 0:720]
    bb_out[...] = pltpu.roll(row_ref[:, 640:768], 128 - 80, 1)[0, 0:36]
    e = jnp.where(srow == 0, e_ref[31], 0.0)
    sums = jnp.sum(jnp.where((lane >= 12) & (lane < 16), e, 0.0))
    count = jnp.sum(jnp.where(lane == 16, e, 0.0))
    loss[...] = jnp.full((1, 128), sums, f32) / jnp.full((1, 128), count, f32)

    def drain(k, carry):
        chunk(k).wait()
        return carry

    lax.fori_loop(0, 30, drain, 0)


VMEM = pl.BlockSpec(memory_space=pltpu.VMEM)
SMEM = pl.BlockSpec(memory_space=pltpu.SMEM)
ANY = pl.BlockSpec(memory_space=pl.ANY)


def near_memory(arrays):
    return [pltpu.with_memory_space_constraint(v, pltpu.VMEM) for v in arrays]


def far_memory(arrays):
    return [pltpu.with_memory_space_constraint(v, pltpu.HBM) for v in arrays]


def shape(*dims, dtype=f32):
    return jax.ShapeDtypeStruct(dims, dtype)


def stage(cw, bw):
    return pl.pallas_call(
        stage_kernel,
        out_shape=pltpu.VMEM((ROWS_ALL, 2304), bf16),
        in_specs=[ANY, VMEM],
        out_specs=VMEM,
        scratch_shapes=[pltpu.SemaphoreType.DMA],
        compiler_params=pltpu.CompilerParams(vmem_limit_bytes=LIMIT),
        name="stage",
    )(*far_memory([cw, bw]))


def head(first, ci, outer, own, inner, w, cb, bb, lab, idx, box):
    return pl.pallas_call(
        head_kernel,
        out_shape=[
            pltpu.HBM((ROWS_ALL, 256), bf16),
            pltpu.HBM((HALF, 256), bf16),
            pltpu.HBM((HALF, 256), bf16),
            pltpu.VMEM((1, 128, 256), bf16),
        ],
        in_specs=[SMEM] * 2 + [VMEM] * 9,
        out_specs=[VMEM] * 4,
        scratch_shapes=[
            pltpu.VMEM((256, 2304), bf16),
            pltpu.VMEM((720, 256), f32),
            pltpu.VMEM((128, 128), f32),
            pltpu.VMEM((128, 128), f32),
            pltpu.VMEM((ROWS_ALL, 256), bf16),
            pltpu.VMEM((16, 768), f32),
            pltpu.VMEM((8, 128), f32),
            pltpu.VMEM((32, 128), jnp.int32),
            pltpu.VMEM((32, 128), jnp.int32),
            pltpu.VMEM((4, 128, 256), bf16),
        ],
        compiler_params=pltpu.CompilerParams(vmem_limit_bytes=LIMIT),
        name="head",
    )(first, ci, *far_memory([outer, own, inner]), *near_memory([w]), *far_memory([cb, bb, lab, idx, box]))


def tower_terms(ci, g, w, after):
    return pl.pallas_call(
        tower_kernel,
        out_shape=(
            pltpu.HBM((2, 128, 256), f32),
            pltpu.VMEM((1, 128, 256), bf16),
            pltpu.VMEM((1, 128, 256), bf16),
            shape(8, 128),
        ),
        in_specs=[SMEM, VMEM, VMEM, ANY],
        out_specs=(VMEM, VMEM, VMEM, VMEM),
        compiler_params=pltpu.CompilerParams(vmem_limit_bytes=LIMIT),
        name="tower_terms",
        cost_estimate=pl.CostEstimate(flops=2 * 756 * 2304 * 256, transcendentals=0, bytes_accessed=4500000),
    )(ci, *far_memory([g]), *near_memory([w]), after)


def tower_end(ci, mid, outer, inner):
    return pl.pallas_call(
        tower_end_kernel,
        out_shape=(shape(1, 2, 128, 256, dtype=bf16), shape(8, 128)),
        in_specs=[SMEM] + [VMEM] * 3,
        out_specs=(VMEM, VMEM),
        compiler_params=pltpu.CompilerParams(vmem_limit_bytes=LIMIT),
        name="tower_end",
    )(ci, *far_memory([mid]), outer, inner)


def weight_terms(yi, xi, ci, keep, got, outer, own, inner, other_edge):
    return pl.pallas_call(
        weight_kernel,
        out_shape=[pltpu.VMEM((4, PIECE, 128), bf16)] * 4 + [shape(8, 128)],
        in_specs=[SMEM] * 3 + [VMEM] * 6,
        out_specs=[VMEM] * 5,
        scratch_shapes=[
            pltpu.VMEM((6, 128, 256), bf16),
            pltpu.VMEM((3, 768, 256), bf16),
            pltpu.VMEM((2, HALF, 256), bf16),
            pltpu.VMEM((16, PIECE, 128), bf16),
        ],
        compiler_params=pltpu.CompilerParams(vmem_limit_bytes=LIMIT),
        name="weight_terms",
    )(yi, xi, ci, *far_memory([keep, got, outer, own, inner]), other_edge)


def row_sum(yi, xi, ci, parts, after):
    return pl.pallas_call(
        row_sum_kernel,
        out_shape=[pltpu.VMEM((PIECE, 128), bf16)] * 4,
        in_specs=[SMEM] * 3 + [VMEM] * 4 + [ANY],
        out_specs=[VMEM] * 4,
        compiler_params=pltpu.CompilerParams(vmem_limit_bytes=LIMIT),
        name="row_sum",
    )(yi, xi, ci, *near_memory(parts), after)


def block_sum(zi, parts):
    return pl.pallas_call(
        block_sum_kernel,
        out_shape=pltpu.VMEM((PIECE, 128), bf16),
        in_specs=[SMEM] + [VMEM] * 4,
        out_specs=VMEM,
        compiler_params=pltpu.CompilerParams(vmem_limit_bytes=LIMIT),
        name="block_sum",
    )(zi, *near_memory(parts))


def piece_sum(zi, m):
    return pl.pallas_call(
        piece_sum_kernel,
        out_shape=pltpu.VMEM((8, 56, 128), bf16),
        in_specs=[SMEM, VMEM],
        out_specs=VMEM,
        compiler_params=pltpu.CompilerParams(vmem_limit_bytes=LIMIT),
        name="piece_sum",
    )(zi, *near_memory([m]))


def join(parts):
    return pl.pallas_call(
        join_kernel,
        out_shape=pltpu.VMEM((4, PIECE, 128), bf16),
        in_specs=[VMEM] * 4,
        out_specs=VMEM,
        compiler_params=pltpu.CompilerParams(vmem_limit_bytes=LIMIT),
        name="join",
    )(*near_memory(parts))


def squares_of(yi, xi, ci, pieces):
    return pl.pallas_call(
        squares_kernel,
        out_shape=pltpu.VMEM((8, 128), f32),
        in_specs=[SMEM] * 3 + [VMEM] * 7,
        out_specs=VMEM,
        compiler_params=pltpu.CompilerParams(vmem_limit_bytes=LIMIT),
        name="squares",
    )(yi, xi, ci, *near_memory(pieces))


def finish(yi, xi, ci, pieces, partial):
    return pl.pallas_call(
        final_kernel,
        out_shape=(shape(720, 2304), shape(36, 2304), shape(720), shape(36), shape(1, 128)),
        in_specs=[SMEM] * 3 + [VMEM] * 9,
        out_specs=(ANY, VMEM, VMEM, VMEM, VMEM),
        scratch_shapes=[
            pltpu.VMEM((ROWS_ALL, 2304), f32),
            pltpu.VMEM((32, 8, 128), f32),
            pltpu.VMEM((8, 896), f32),
            pltpu.SemaphoreType.DMA,
        ],
        compiler_params=pltpu.CompilerParams(vmem_limit_bytes=LIMIT),
        name="finish",
    )(yi, xi, ci, *near_memory([*pieces, partial]))


def swap(value):
    return lax.ppermute(value, "core", [(0, 1), (1, 0)])


def across(value):
    pairs = [(t, t + 1) for t in range(1, 31, 2)]
    return lax.ppermute(value, TILE_AXES, pairs + [(b, a) for a, b in pairs])


def along(value, k, first_axis):
    pairs = []
    for y in range(4):
        for c in range(2):
            for x in range(4):
                dx = k if (first_axis == "x") == (c == 0) else 0
                dy = k - dx
                pairs.append(((y * 2 + c) * 4 + x, (((y + dy) % 4) * 2 + c) * 4 + (x + dx) % 4))
    return lax.ppermute(value, ("y", "core", "x"), pairs)


def per_device(tower, cls_weight, cls_bias, box_weight, box_bias, labels, target_index, boxes):
    own = tower[0]
    outer = across(own)
    inner = swap(own)
    ci = lax.axis_index("core").reshape(1)
    yi = lax.axis_index("y").reshape(1)
    xi = lax.axis_index("x").reshape(1)
    zi = (lax.axis_index("zhi") * 4 + lax.axis_index("zlo")).reshape(1)
    first = (lax.axis_index(TILE_AXES) * 2).reshape(1)

    w = stage(cls_weight, box_weight)
    g, keep, send, edge = head(
        first, ci, outer, own, inner, w, cls_bias, box_bias, labels[0], target_index[0], boxes[0]
    )
    *parts, token = weight_terms(yi, xi, ci, keep, swap(send), outer, own, inner, swap(edge))

    mid, to_outer, to_inner, _ = tower_terms(ci, g, w, token)
    tower_grad, end_token = tower_end(ci, mid, across(to_outer), swap(to_inner))

    parts = [parts[0]] + [along(parts[k], k, "y") for k in (1, 2, 3)]
    parts = row_sum(yi, xi, ci, parts, end_token)
    parts = [parts[0]] + [along(parts[k], k, "x") for k in (1, 2, 3)]
    terms = lax.all_to_all(block_sum(zi, parts).reshape(8, 56, 128), ("zhi", "zlo"), 0, 0, tiled=True)
    copies = lax.all_to_all(piece_sum(zi, terms), ("zhi", "zlo"), 0, 0, tiled=True)
    block = copies.reshape(PIECE, 128)
    row = join([block] + [along(block, k, "x") for k in (1, 2, 3)])
    mine = [row] + [along(row, k, "y") for k in (1, 2, 3)]
    pieces = mine + [swap(v) for v in mine]
    partial = squares_of(yi, xi, ci, pieces[:LAST] + pieces[LAST + 1 :])
    cw_grad, bw_grad, cb_grad, bb_grad, loss = finish(yi, xi, ci, pieces, partial)
    return loss[0, 0], cw_grad, cb_grad, bw_grad, bb_grad, tower_grad


def solution(mesh):
    fine = Mesh(mesh.devices.reshape(4, 4, 2, 4, 2), ("zlo", "y", "core", "x", "zhi"))
    placed = (
        P(IMG_AXES, TILE_AXES, None, None),
        P(),
        P(),
        P(),
        P(),
        P(IMG_AXES, None, TILE_AXES, None),
        P(IMG_AXES, None, TILE_AXES, None),
        P(IMG_AXES, None, None),
    )
    return jax.shard_map(
        per_device,
        mesh=fine,
        in_specs=placed,
        out_specs=(P(), P(), P(), P(), P(), P(IMG_AXES, TILE_AXES, None, None)),
        check_vma=False,
    )
```

```python
import jax
import jax.numpy as jnp
from jax import lax
from jax.experimental import pallas as pl
from jax.experimental.pallas import tpu as pltpu
from jax.sharding import Mesh, PartitionSpec as P

CLASSES = 80
ANCHORS = 9
STRIDE = 8
FOCAL_ALPHA = 0.25
NORM_EPS = 1e-06

ROWS_ALL = 768
VALID = 756
HALF = 384
GROUP_ROWS = 96
BLOCK = 24
TILES = 56
PIECE = 448
QUARTER = 112

LIMIT = 24 << 20

TILE_AXES = ("zlo", "y", "core")
IMG_AXES = ("x", "zhi")

f32 = jnp.float32
bf16 = jnp.bfloat16


def dot(a, b, dims):
    return lax.dot_general(a, b, (dims, ((), ())), preferred_element_type=f32)


def shifted(x, j):
    if j == 1:
        return x
    ids = lax.broadcasted_iota(jnp.int32, x.shape, 0)
    if j == 0:
        return jnp.where(ids == 0, 0.0, pltpu.roll(x, 1, 0))
    return jnp.where(ids == x.shape[0] - 1, 0.0, pltpu.roll(x, x.shape[0] - 1, 0))


def fill_patches(rows, p_ref, base):
    for e, row in enumerate(rows):
        x = row.astype(f32)
        for j in range(3):
            v = shifted(x, j).astype(bf16)
            for i in range(3):
                r = e - i
                if 0 <= r < 2:
                    p_ref[base + r * 128 : base + r * 128 + 128, (3 * i + j) * 256 : (3 * i + j) * 256 + 256] = v


def anchor_sizes(shape):
    ids = lax.broadcasted_iota(jnp.int32, shape, 0)
    w = jnp.ones(shape, f32)
    h = jnp.ones(shape, f32)
    for a in range(ANCHORS):
        base = 4.0 * STRIDE * 2.0 ** ((a // 3) / 3.0)
        ratio = a % 3 - 1
        w = jnp.where(ids == a, base * 2.0 ** (-ratio / 2.0), w)
        h = jnp.where(ids == a, base * 2.0 ** (ratio / 2.0), h)
    return w, h


def giou_terms(o0, o1, o2, o3, aw, ah, cx, cy, tl, tt, tr, tb):
    mx = cx + o0 * aw
    my = cy + o1 * ah
    pw = aw * jnp.exp(o2)
    ph = ah * jnp.exp(o3)
    left = mx - 0.5 * pw
    right = mx + 0.5 * pw
    top = my - 0.5 * ph
    bottom = my + 0.5 * ph
    iw = jnp.maximum(jnp.minimum(right, tr) - jnp.maximum(left, tl), 0.0)
    ih = jnp.maximum(jnp.minimum(bottom, tb) - jnp.maximum(top, tt), 0.0)
    inter = iw * ih
    union = pw * ph + (tr - tl) * (tb - tt) - inter
    ow = jnp.maximum(right, tr) - jnp.minimum(left, tl)
    oh = jnp.maximum(bottom, tb) - jnp.minimum(top, tt)
    outer = ow * oh
    return 1.0 - (inter / union - (outer - union) / outer)


def stage_kernel(cw, bw, w_ref, sem):
    copy = pltpu.make_async_copy(cw, w_ref.at[pl.ds(0, 720)], sem)
    copy.start()
    w_ref[752:768, :] = jnp.zeros((16, 2304), bf16)
    w_ref[720:756, :] = bw[...]
    copy.wait()


def head_kernel(first, ci, outer, own, inner, w, cb, bb, lab, idx, box, *refs):
    g_out, keep, send, edge = refs[0:4]
    p_ref, o_ref, b_ref, gb_ref, g_ref, row_ref, box_ref, lab_ref, idx_ref, ext_ref = refs[4:]
    c = ci[0]
    edge[0] = outer[1 - c]
    ext_ref[3 * c] = outer[1 - c]
    ext_ref[3 - 3 * c] = inner[c]
    fill_patches([ext_ref[0], own[0], own[1], ext_ref[3]], p_ref, 0)
    row_ref[0, 0:720] = cb[...]
    row_ref[8, 0:36] = bb[...]
    column = row_ref[0:8, :].T[:, 0:1]
    box_column = row_ref[8:16, 0:128].T[:, 0:1]
    box_ref[0:4, 0:100] = box[...]
    lab_ref[...] = jnp.full((32, 128), -2, jnp.int32)
    idx_ref[...] = jnp.zeros((32, 128), jnp.int32)
    for r in range(2):
        for a in range(ANCHORS):
            lab_ref[r * 16 + a : r * 16 + a + 1, :] = lab[a, r : r + 1, :]
            idx_ref[r * 16 + a : r * 16 + a + 1, :] = idx[a, r : r + 1, :]
    p = p_ref[...]
    out = dot(w[...], p, ((1,), (1,)))
    o_ref[...] = out[0:720] + column[0:720]
    small_out = out[720:756] + box_column[0:36]
    for r in range(2):
        b_ref[r * 64 + 32 : r * 64 + 64, :] = jnp.zeros((32, 128), f32)
        b_ref[r * 64 : r * 64 + 36, :] = small_out[:, r * 128 : r * 128 + 128]
    cls = lax.broadcasted_iota(jnp.int32, (CLASSES, 128), 0)

    def one_anchor(a, carry):
        sums = []
        at = pl.multiple_of(a * CLASSES, 16)
        for r in range(2):
            label = lab_ref[pl.ds(r * 16 + a, 1), :]
            x = o_ref[pl.ds(at, CLASSES), r * 128 : r * 128 + 128]
            hit = label == cls
            z = jnp.where(hit, -x, x)
            e = jnp.exp(-jnp.abs(z))
            soft = jnp.maximum(z, 0.0) + jnp.log1p(e)
            big = 1.0 / (1.0 + e)
            small = e * big
            up = z >= 0.0
            q = jnp.where(up, big, small)
            rest = jnp.where(up, small, big)
            counted = (label >= -1).astype(f32)
            w = jnp.where(hit, FOCAL_ALPHA, 1.0 - FOCAL_ALPHA) * counted
            wq = w * q * q
            dz = wq * (q + 2.0 * rest * soft)
            g_ref[pl.ds(at, CLASSES), r * 128 : r * 128 + 128] = jnp.where(hit, -dz, dz).astype(bf16)
            sums.append(carry[r] + jnp.sum(wq * soft, axis=0, keepdims=True))
        return tuple(sums)

    zero = jnp.zeros((1, 128), f32)
    focal = lax.fori_loop(0, ANCHORS, one_anchor, (zero, zero))

    aw, ah = anchor_sizes((16, 128))
    cx = (lax.broadcasted_iota(jnp.int32, (16, 128), 1).astype(f32) + 0.5) * STRIDE
    for r in range(2):
        cy = (jnp.full((16, 128), first[0] + r, jnp.int32).astype(f32) + 0.5) * STRIDE
        which = idx_ref[r * 16 : r * 16 + 16, :]
        corner = [
            jnp.take_along_axis(jnp.broadcast_to(box_ref[k : k + 1, :], (16, 128)), which, axis=1) for k in range(4)
        ]
        positive = lab_ref[r * 16 : r * 16 + 16, :] >= 0
        o = [b_ref[pl.ds(r * 64 + k, 16, stride=4), :] for k in range(4)]
        value, pull = jax.vjp(
            lambda o0, o1, o2, o3: giou_terms(o0, o1, o2, o3, aw, ah, cx, cy, *corner), *o
        )
        grads = pull(jnp.ones((16, 128), f32))
        for k in range(4):
            gb_ref[pl.ds(r * 64 + k, 16, stride=4), :] = jnp.where(positive, grads[k], 0.0)
        giou = jnp.sum(jnp.where(positive, value, 0.0), axis=0, keepdims=True)
        count = jnp.sum(positive.astype(f32), axis=0, keepdims=True)
        rows = []
        for v in (focal[r], giou):
            hi = v.astype(bf16).astype(f32)
            rows += [hi, v - hi]
        rows.append(count)
        for n, v in enumerate(rows):
            gb_ref[r * 64 + 36 + n : r * 64 + 37 + n, :] = v
        g_ref[720:768, r * 128 : r * 128 + 128] = gb_ref[r * 64 : r * 64 + 48, :].astype(bf16)
    g_out[...] = g_ref[...]
    keep[...] = g_ref[pl.ds(pl.multiple_of(ci[0] * HALF, 16), HALF), :]
    send[...] = g_ref[pl.ds(pl.multiple_of((1 - ci[0]) * HALF, 16), HALF), :]


def tower_kernel(ci, g, w_ref, unused, mid, outer, inner, token):
    token[...] = jnp.zeros((8, 128), f32)
    gt = g[...].astype(f32).T
    gj = []
    for j in range(3):
        gj.append(
            jnp.concatenate([shifted(gt[r * 128 : r * 128 + 128], 2 - j) for r in range(2)], axis=0).astype(bf16)
        )
    t = []
    for i in range(3):
        acc = jnp.zeros((256, 256), f32)
        for j in range(3):
            at = (3 * i + j) * 256
            acc = acc + dot(gj[j], w_ref[:, at : at + 256], ((1,), (0,)))
        t.append(acc)
    low = jnp.full((128, 256), ci[0], jnp.int32) == 0
    up = t[0][0:128]
    down = t[2][128:256]
    outer[0] = jnp.where(low, up, down).astype(bf16)
    inner[0] = jnp.where(low, down, up).astype(bf16)
    mid[0] = t[1][0:128] + t[0][128:256]
    mid[1] = t[1][128:256] + t[2][0:128]


def tower_end_kernel(ci, mid, outer, inner, t_ref, token):
    token[...] = jnp.zeros((8, 128), f32)
    c = ci[0]
    t_ref[0, c] = (mid[c] + outer[0].astype(f32)).astype(bf16)
    t_ref[0, 1 - c] = (mid[1 - c] + inner[0].astype(f32)).astype(bf16)


def weight_kernel(yi, xi, ci, keep, got, outer, own, inner, other_edge, *refs):
    outs = refs[0:4]
    token, t_ref, s_ref, g_ref, m_ref = refs[4:]
    token[...] = jnp.zeros((8, 128), f32)
    c = ci[0]
    t_ref[5 * c] = outer[1 - c]
    t_ref[5 - 5 * c] = other_edge[0]
    for r in range(2):
        t_ref[1 + 2 * c + r] = own[r]
        t_ref[3 - 2 * c + r] = inner[r]
    g_ref[c] = keep[...]
    g_ref[1 - c] = got[...]

    def shift(row, carry):
        x = t_ref[row].astype(f32)
        at = pl.multiple_of(row * 128, 128)
        for j in range(3):
            s_ref[j, pl.ds(at, 128), :] = shifted(x, j).astype(bf16)
        return carry

    lax.fori_loop(0, 6, shift, 0)
    lhs = jnp.concatenate([g_ref[0], g_ref[1]], axis=1)
    for tap in range(9):
        i, j = divmod(tap, 3)
        acc = dot(lhs, s_ref[j, i * 128 : i * 128 + 512, :], ((1,), (0,)))
        for m in range(16):
            for rb in range(3):
                row = m * BLOCK + rb * 8
                both = jnp.concatenate([acc[row : row + 8, 0:128], acc[row : row + 8, 128:256]], axis=0)
                v = (rb * 18 + 2 * tap) * 8
                m_ref[m, v : v + 16, :] = both.astype(bf16)
    bias = dot(jnp.ones((8, 512), bf16), lhs, ((1,), (1,)))
    for m in range(16):
        tile, off = divmod(m * BLOCK, 128)
        e = bias[:, tile * 128 : tile * 128 + 128]
        e = e if off == 0 else pltpu.roll(e, 128 - off, 1)
        if off + BLOCK > 128:
            past = pltpu.roll(bias[:, tile * 128 + 128 : tile * 128 + 256], 128 - off, 1)
            lane = lax.broadcasted_iota(jnp.int32, (8, 128), 1)
            e = jnp.where(lane < 128 - off, e, past)
        hi = e.astype(bf16).astype(f32)
        m_ref[m, 432:448, :] = jnp.concatenate([hi, e - hi], axis=0).astype(bf16)
    for k in range(4):
        for q in range(4):
            outs[k][q] = m_ref[jnp.where(c == 0, ((yi[0] + k) & 3) * 4 + q, q * 4 + ((xi[0] + k) & 3))]


def row_sum_kernel(yi, xi, ci, *refs):
    parts = refs[0:4]
    outs = refs[5:9]
    here = jnp.where(ci[0] == 0, xi[0], yi[0])
    for k in range(4):
        q = (here + k) & 3
        acc = parts[0][q].astype(f32)
        for n in range(1, 4):
            acc = acc + parts[n][q].astype(f32)
        e = acc[432:440] + acc[440:448]
        hi = e.astype(bf16).astype(f32)
        outs[k][0:432, :] = acc[0:432].astype(bf16)
        outs[k][432:448, :] = jnp.concatenate([hi, e - hi], axis=0).astype(bf16)


def split(acc):
    e = acc[0:8] + acc[8:16]
    hi = e.astype(bf16).astype(f32)
    return jnp.concatenate([hi, e - hi], axis=0)


def block_sum_kernel(ji, a, b, c, d, *refs):
    outs, s_ref = refs[0:4], refs[4]
    acc = (a[...].astype(f32) + b[...].astype(f32)) + (c[...].astype(f32) + d[...].astype(f32))
    s_ref[0:432, :] = acc[0:432].astype(bf16)
    s_ref[432:448, :] = split(acc[432:448]).astype(bf16)
    for k in range(4):
        outs[k][...] = s_ref[pl.ds(pl.multiple_of(((ji[0] + k) & 3) * QUARTER, 16), QUARTER), :]


def quarter_sum_kernel(ji, *refs):
    acc = refs[0][...].astype(f32)
    for ref in refs[1:-1]:
        acc = acc + ref[...].astype(f32)
    tail = acc[96:112]
    tail = jnp.where(jnp.full((16, 128), ji[0], jnp.int32) == 3, split(tail), tail)
    refs[-1][0:96, :] = acc[0:96].astype(bf16)
    refs[-1][96:112, :] = tail.astype(bf16)


def gather_kernel(ji, *refs):
    for k in range(4):
        refs[4][pl.ds(pl.multiple_of(((ji[0] - k) & 3) * QUARTER, 16), QUARTER), :] = refs[k][...]


def join_kernel(a, b, c, d, o_ref):
    for k, ref in enumerate((a, b, c, d)):
        o_ref[k] = ref[...]


LAST = 5


def block_of(yi, xi, ci, n, k):
    c = ci[0] if n < 4 else 1 - ci[0]
    far = n % 4
    y = (yi[0] - jnp.where(c == 0, far, k)) & 3
    x = (xi[0] - jnp.where(c == 0, k, far)) & 3
    return c * 16 + y * 4 + x


def squares(yi, xi, ci, n, src):
    srow = lax.broadcasted_iota(jnp.int32, (8, 128), 0)
    lane = lax.broadcasted_iota(jnp.int32, (8, 128), 1)

    def one(k, total):
        base = block_of(yi, xi, ci, n, k) * BLOCK
        for rb in range(3):
            acc = jnp.zeros((16, 128), f32)
            for t in range(9):
                v = src[k, (rb * 9 + t) * 16 : (rb * 9 + t) * 16 + 16, :].astype(f32)
                acc = acc + v * v
            ok = base + rb * 8 + srow < VALID
            total = total + jnp.where(ok, acc[0:8] + acc[8:16], 0.0)
        e = src[k, 432:448, :].astype(f32)
        e = e[0:8] + e[8:16]
        ok = (base + lane < VALID) & (lane < BLOCK) & (srow == 0)
        return total + jnp.where(ok, e * e, 0.0)

    return one


def squares_kernel(yi, xi, ci, *refs):
    total = jnp.zeros((8, 128), f32)
    for n, src in zip([n for n in range(8) if n != LAST], refs[:7]):
        total = lax.fori_loop(0, 4, squares(yi, xi, ci, n, src), total)
    refs[7][...] = total


def final_kernel(yi, xi, ci, *refs):
    sources = refs[0:8]
    partial, cw_out, bw_out, cb_out, bb_out, loss, w_ref, e_ref, row_ref, sem = refs[8:]
    srow = lax.broadcasted_iota(jnp.int32, (8, 128), 0)
    lane = lax.broadcasted_iota(jnp.int32, (8, 128), 1)
    total = lax.fori_loop(0, 4, squares(yi, xi, ci, LAST, sources[LAST]), partial[...])
    mean = jnp.sum(total) * (1.0 / (VALID * 2305))
    scale = lax.rsqrt(jnp.full((8, 128), mean + NORM_EPS, f32))

    def chunk(block):
        rows = pl.ds(pl.multiple_of(block * BLOCK, 8), BLOCK)
        return pltpu.make_async_copy(w_ref.at[rows], cw_out.at[rows], sem)

    def write(n):
        src = sources[n]

        def one(k, carry):
            block = block_of(yi, xi, ci, n, k)
            e = src[k, 432:448, :].astype(f32)
            e_ref[block] = e[0:8] + e[8:16]
            for rb in range(3):
                row = pl.multiple_of(block * BLOCK + rb * 8, 8)
                for t in range(9):
                    v = src[k, (rb * 9 + t) * 16 : (rb * 9 + t) * 16 + 16, :].astype(f32)
                    w_ref[pl.ds(row, 8), t * 256 : t * 256 + 128] = v[0:8] * scale
                    w_ref[pl.ds(row, 8), t * 256 + 128 : t * 256 + 256] = v[8:16] * scale

            @pl.when(block < 30)
            def _():
                chunk(block).start()

            return carry

        return one

    for n in range(8):
        lax.fori_loop(0, 4, write(n), 0)
    bw_out[...] = w_ref[720:756, :]
    row_ref[...] = jnp.zeros((8, 896), f32)
    for block in range(32):
        tile, off = divmod(block * BLOCK, 128)
        e = e_ref[block] * scale
        e = e if off == 0 else pltpu.roll(e, off, 1)
        here = (lane >= off) & (lane < off + BLOCK)
        row_ref[:, tile * 128 : tile * 128 + 128] = jnp.where(here, e, row_ref[:, tile * 128 : tile * 128 + 128])
        if off + BLOCK > 128:
            past = lane < off + BLOCK - 128
            row_ref[:, tile * 128 + 128 : tile * 128 + 256] = jnp.where(past, e, 0.0)
    cb_out[...] = row_ref[0, 0:720]
    bb_out[...] = pltpu.roll(row_ref[:, 640:768], 128 - 80, 1)[0, 0:36]
    e = jnp.where(srow == 0, e_ref[31], 0.0)
    sums = jnp.sum(jnp.where((lane >= 12) & (lane < 16), e, 0.0))
    count = jnp.sum(jnp.where(lane == 16, e, 0.0))
    loss[...] = jnp.full((1, 128), sums, f32) / jnp.full((1, 128), count, f32)

    def drain(k, carry):
        chunk(k).wait()
        return carry

    lax.fori_loop(0, 30, drain, 0)


VMEM = pl.BlockSpec(memory_space=pltpu.VMEM)
SMEM = pl.BlockSpec(memory_space=pltpu.SMEM)
ANY = pl.BlockSpec(memory_space=pl.ANY)


def near_memory(arrays):
    return [pltpu.with_memory_space_constraint(v, pltpu.VMEM) for v in arrays]


def far_memory(arrays):
    return [pltpu.with_memory_space_constraint(v, pltpu.HBM) for v in arrays]


def shape(*dims, dtype=f32):
    return jax.ShapeDtypeStruct(dims, dtype)


def stage(cw, bw):
    return pl.pallas_call(
        stage_kernel,
        out_shape=pltpu.VMEM((ROWS_ALL, 2304), bf16),
        in_specs=[ANY, VMEM],
        out_specs=VMEM,
        scratch_shapes=[pltpu.SemaphoreType.DMA],
        compiler_params=pltpu.CompilerParams(vmem_limit_bytes=LIMIT),
        name="stage",
    )(*far_memory([cw, bw]))


def head(first, ci, outer, own, inner, w, cb, bb, lab, idx, box):
    return pl.pallas_call(
        head_kernel,
        out_shape=[
            pltpu.HBM((ROWS_ALL, 256), bf16),
            pltpu.HBM((HALF, 256), bf16),
            pltpu.HBM((HALF, 256), bf16),
            pltpu.VMEM((1, 128, 256), bf16),
        ],
        in_specs=[SMEM] * 2 + [VMEM] * 9,
        out_specs=[VMEM] * 4,
        scratch_shapes=[
            pltpu.VMEM((256, 2304), bf16),
            pltpu.VMEM((720, 256), f32),
            pltpu.VMEM((128, 128), f32),
            pltpu.VMEM((128, 128), f32),
            pltpu.VMEM((ROWS_ALL, 256), bf16),
            pltpu.VMEM((16, 768), f32),
            pltpu.VMEM((8, 128), f32),
            pltpu.VMEM((32, 128), jnp.int32),
            pltpu.VMEM((32, 128), jnp.int32),
            pltpu.VMEM((4, 128, 256), bf16),
        ],
        compiler_params=pltpu.CompilerParams(vmem_limit_bytes=LIMIT),
        name="head",
    )(first, ci, *far_memory([outer, own, inner]), *near_memory([w]), *far_memory([cb, bb, lab, idx, box]))


def tower_terms(ci, g, w, after):
    return pl.pallas_call(
        tower_kernel,
        out_shape=(
            pltpu.HBM((2, 128, 256), f32),
            pltpu.VMEM((1, 128, 256), bf16),
            pltpu.VMEM((1, 128, 256), bf16),
            shape(8, 128),
        ),
        in_specs=[SMEM, VMEM, VMEM, ANY],
        out_specs=(VMEM, VMEM, VMEM, VMEM),
        compiler_params=pltpu.CompilerParams(vmem_limit_bytes=LIMIT),
        name="tower_terms",
        cost_estimate=pl.CostEstimate(flops=2 * 756 * 2304 * 256, transcendentals=0, bytes_accessed=4500000),
    )(ci, *far_memory([g]), *near_memory([w]), after)


def tower_end(ci, mid, outer, inner):
    return pl.pallas_call(
        tower_end_kernel,
        out_shape=(shape(1, 2, 128, 256, dtype=bf16), shape(8, 128)),
        in_specs=[SMEM] + [VMEM] * 3,
        out_specs=(VMEM, VMEM),
        compiler_params=pltpu.CompilerParams(vmem_limit_bytes=LIMIT),
        name="tower_end",
    )(ci, *far_memory([mid]), outer, inner)


def weight_terms(yi, xi, ci, keep, got, outer, own, inner, other_edge):
    return pl.pallas_call(
        weight_kernel,
        out_shape=[pltpu.VMEM((4, PIECE, 128), bf16)] * 4 + [shape(8, 128)],
        in_specs=[SMEM] * 3 + [VMEM] * 6,
        out_specs=[VMEM] * 5,
        scratch_shapes=[
            pltpu.VMEM((6, 128, 256), bf16),
            pltpu.VMEM((3, 768, 256), bf16),
            pltpu.VMEM((2, HALF, 256), bf16),
            pltpu.VMEM((16, PIECE, 128), bf16),
        ],
        compiler_params=pltpu.CompilerParams(vmem_limit_bytes=LIMIT),
        name="weight_terms",
    )(yi, xi, ci, *far_memory([keep, got, outer, own, inner]), other_edge)


def row_sum(yi, xi, ci, parts, after):
    return pl.pallas_call(
        row_sum_kernel,
        out_shape=[pltpu.VMEM((PIECE, 128), bf16)] * 4,
        in_specs=[SMEM] * 3 + [VMEM] * 4 + [ANY],
        out_specs=[VMEM] * 4,
        compiler_params=pltpu.CompilerParams(vmem_limit_bytes=LIMIT),
        name="row_sum",
    )(yi, xi, ci, *near_memory(parts), after)


def block_sum(ji, parts):
    return pl.pallas_call(
        block_sum_kernel,
        out_shape=[pltpu.VMEM((QUARTER, 128), bf16)] * 4,
        in_specs=[SMEM] + [VMEM] * 4,
        out_specs=[VMEM] * 4,
        scratch_shapes=[pltpu.VMEM((PIECE, 128), bf16)],
        compiler_params=pltpu.CompilerParams(vmem_limit_bytes=LIMIT),
        name="block_sum",
    )(ji, *near_memory(parts))


def quarter_sum(ji, parts, name):
    return pl.pallas_call(
        quarter_sum_kernel,
        out_shape=pltpu.VMEM((QUARTER, 128), bf16),
        in_specs=[SMEM] + [VMEM] * len(parts),
        out_specs=VMEM,
        compiler_params=pltpu.CompilerParams(vmem_limit_bytes=LIMIT),
        name=name,
    )(ji, *near_memory(parts))


def gather(ji, parts):
    return pl.pallas_call(
        gather_kernel,
        out_shape=pltpu.VMEM((PIECE, 128), bf16),
        in_specs=[SMEM] + [VMEM] * 4,
        out_specs=VMEM,
        compiler_params=pltpu.CompilerParams(vmem_limit_bytes=LIMIT),
        name="gather",
    )(ji, *near_memory(parts))


def join(parts):
    return pl.pallas_call(
        join_kernel,
        out_shape=pltpu.VMEM((4, PIECE, 128), bf16),
        in_specs=[VMEM] * 4,
        out_specs=VMEM,
        compiler_params=pltpu.CompilerParams(vmem_limit_bytes=LIMIT),
        name="join",
    )(*near_memory(parts))


def squares_of(yi, xi, ci, pieces):
    return pl.pallas_call(
        squares_kernel,
        out_shape=pltpu.VMEM((8, 128), f32),
        in_specs=[SMEM] * 3 + [VMEM] * 7,
        out_specs=VMEM,
        compiler_params=pltpu.CompilerParams(vmem_limit_bytes=LIMIT),
        name="squares",
    )(yi, xi, ci, *near_memory(pieces))


def finish(yi, xi, ci, pieces, partial):
    return pl.pallas_call(
        final_kernel,
        out_shape=(shape(720, 2304), shape(36, 2304), shape(720), shape(36), shape(1, 128)),
        in_specs=[SMEM] * 3 + [VMEM] * 9,
        out_specs=(ANY, VMEM, VMEM, VMEM, VMEM),
        scratch_shapes=[
            pltpu.VMEM((ROWS_ALL, 2304), f32),
            pltpu.VMEM((32, 8, 128), f32),
            pltpu.VMEM((8, 896), f32),
            pltpu.SemaphoreType.DMA,
        ],
        compiler_params=pltpu.CompilerParams(vmem_limit_bytes=LIMIT),
        name="finish",
    )(yi, xi, ci, *near_memory([*pieces, partial]))


def swap(value):
    return lax.ppermute(value, "core", [(0, 1), (1, 0)])


def across(value):
    pairs = [(t, t + 1) for t in range(1, 31, 2)]
    return lax.ppermute(value, TILE_AXES, pairs + [(b, a) for a, b in pairs])


def along_z(value, target):
    place = lambda z: (z % 4) * 2 + z // 4
    return lax.ppermute(value, ("zlo", "zhi"), [(place(z), place(target(z))) for z in range(8)])


def along(value, k, first_axis):
    pairs = []
    for y in range(4):
        for c in range(2):
            for x in range(4):
                dx = k if (first_axis == "x") == (c == 0) else 0
                dy = k - dx
                pairs.append(((y * 2 + c) * 4 + x, (((y + dy) % 4) * 2 + c) * 4 + (x + dx) % 4))
    return lax.ppermute(value, ("y", "core", "x"), pairs)


def per_device(tower, cls_weight, cls_bias, box_weight, box_bias, labels, target_index, boxes):
    own = tower[0]
    outer = across(own)
    inner = swap(own)
    ci = lax.axis_index("core").reshape(1)
    yi = lax.axis_index("y").reshape(1)
    xi = lax.axis_index("x").reshape(1)
    ji = ((lax.axis_index("zhi") * 4 + lax.axis_index("zlo")) // 2).reshape(1)
    first = (lax.axis_index(TILE_AXES) * 2).reshape(1)

    w = stage(cls_weight, box_weight)
    g, keep, send, edge = head(
        first, ci, outer, own, inner, w, cls_bias, box_bias, labels[0], target_index[0], boxes[0]
    )
    *parts, token = weight_terms(yi, xi, ci, keep, swap(send), outer, own, inner, swap(edge))

    mid, to_outer, to_inner, _ = tower_terms(ci, g, w, token)
    tower_grad, end_token = tower_end(ci, mid, across(to_outer), swap(to_inner))

    parts = [parts[0]] + [along(parts[k], k, "y") for k in (1, 2, 3)]
    parts = row_sum(yi, xi, ci, parts, end_token)
    parts = [parts[0]] + [along(parts[k], k, "x") for k in (1, 2, 3)]
    parts = block_sum(ji, parts)
    parts = [parts[0]] + [along_z(parts[k], lambda z, k=k: (z + 2 * k) % 8) for k in (1, 2, 3)]
    quarter = quarter_sum(ji, parts, "quarter_sum")
    quarter = quarter_sum(ji, [quarter, along_z(quarter, lambda z: z ^ 1)], "pair_sum")
    block = gather(ji, [quarter] + [along_z(quarter, lambda z, k=k: (z + 2 * k) % 8) for k in (1, 2, 3)])
    row = join([block] + [along(block, k, "x") for k in (1, 2, 3)])
    mine = [row] + [along(row, k, "y") for k in (1, 2, 3)]
    pieces = mine + [swap(v) for v in mine]
    partial = squares_of(yi, xi, ci, pieces[:LAST] + pieces[LAST + 1 :])
    cw_grad, bw_grad, cb_grad, bb_grad, loss = finish(yi, xi, ci, pieces, partial)
    return loss[0, 0], cw_grad, cb_grad, bw_grad, bb_grad, tower_grad


def solution(mesh):
    fine = Mesh(mesh.devices.reshape(4, 4, 2, 4, 2), ("zlo", "y", "core", "x", "zhi"))
    placed = (
        P(IMG_AXES, TILE_AXES, None, None),
        P(),
        P(),
        P(),
        P(),
        P(IMG_AXES, None, TILE_AXES, None),
        P(IMG_AXES, None, TILE_AXES, None),
        P(IMG_AXES, None, None),
    )
    return jax.shard_map(
        per_device,
        mesh=fine,
        in_specs=placed,
        out_specs=(P(), P(), P(), P(), P(), P(IMG_AXES, TILE_AXES, None, None)),
        check_vma=False,
    )
```

```python
import jax
import jax.numpy as jnp
from jax import lax
from jax.experimental import pallas as pl
from jax.experimental.pallas import tpu as pltpu
from jax.sharding import Mesh, PartitionSpec as P

CLASSES = 80
ANCHORS = 9
STRIDE = 8
FOCAL_ALPHA = 0.25
NORM_EPS = 1e-06

ROWS_ALL = 768
VALID = 756
HALF = 384
GROUP_ROWS = 96
BLOCK = 24
TILES = 56
PIECE = 448

LIMIT = 24 << 20

TILE_AXES = ("zlo", "y", "core")
IMG_AXES = ("x", "zhi")

f32 = jnp.float32
bf16 = jnp.bfloat16


def dot(a, b, dims):
    return lax.dot_general(a, b, (dims, ((), ())), preferred_element_type=f32)


def shifted(x, j):
    if j == 1:
        return x
    ids = lax.broadcasted_iota(jnp.int32, x.shape, 0)
    if j == 0:
        return jnp.where(ids == 0, 0.0, pltpu.roll(x, 1, 0))
    return jnp.where(ids == x.shape[0] - 1, 0.0, pltpu.roll(x, x.shape[0] - 1, 0))


def fill_patches(rows, p_ref, base):
    for e, row in enumerate(rows):
        x = row.astype(f32)
        for j in range(3):
            v = shifted(x, j).astype(bf16)
            for i in range(3):
                r = e - i
                if 0 <= r < 2:
                    p_ref[base + r * 128 : base + r * 128 + 128, (3 * i + j) * 256 : (3 * i + j) * 256 + 256] = v


def anchor_sizes(shape):
    ids = lax.broadcasted_iota(jnp.int32, shape, 0)
    w = jnp.ones(shape, f32)
    h = jnp.ones(shape, f32)
    for a in range(ANCHORS):
        base = 4.0 * STRIDE * 2.0 ** ((a // 3) / 3.0)
        ratio = a % 3 - 1
        w = jnp.where(ids == a, base * 2.0 ** (-ratio / 2.0), w)
        h = jnp.where(ids == a, base * 2.0 ** (ratio / 2.0), h)
    return w, h


def giou_terms(o0, o1, o2, o3, aw, ah, cx, cy, tl, tt, tr, tb):
    mx = cx + o0 * aw
    my = cy + o1 * ah
    pw = aw * jnp.exp(o2)
    ph = ah * jnp.exp(o3)
    left = mx - 0.5 * pw
    right = mx + 0.5 * pw
    top = my - 0.5 * ph
    bottom = my + 0.5 * ph
    iw = jnp.maximum(jnp.minimum(right, tr) - jnp.maximum(left, tl), 0.0)
    ih = jnp.maximum(jnp.minimum(bottom, tb) - jnp.maximum(top, tt), 0.0)
    inter = iw * ih
    union = pw * ph + (tr - tl) * (tb - tt) - inter
    ow = jnp.maximum(right, tr) - jnp.minimum(left, tl)
    oh = jnp.maximum(bottom, tb) - jnp.minimum(top, tt)
    outer = ow * oh
    return 1.0 - (inter / union - (outer - union) / outer)


def stage_kernel(cw, bw, w_ref, sem):
    copy = pltpu.make_async_copy(cw, w_ref.at[pl.ds(0, 720)], sem)
    copy.start()
    w_ref[752:768, :] = jnp.zeros((16, 2304), bf16)
    w_ref[720:756, :] = bw[...]
    copy.wait()


def head_kernel(first, ci, outer, own, inner, w, cb, bb, lab, idx, box, *refs):
    g_out, keep, send, edge = refs[0:4]
    p_ref, o_ref, b_ref, gb_ref, g_ref, row_ref, box_ref, lab_ref, idx_ref, ext_ref = refs[4:]
    c = ci[0]
    edge[0] = outer[1 - c]
    ext_ref[3 * c] = outer[1 - c]
    ext_ref[3 - 3 * c] = inner[c]
    fill_patches([ext_ref[0], own[0], own[1], ext_ref[3]], p_ref, 0)
    row_ref[0, 0:720] = cb[...]
    row_ref[8, 0:36] = bb[...]
    column = row_ref[0:8, :].T[:, 0:1]
    box_column = row_ref[8:16, 0:128].T[:, 0:1]
    box_ref[0:4, 0:100] = box[...]
    lab_ref[...] = jnp.full((32, 128), -2, jnp.int32)
    idx_ref[...] = jnp.zeros((32, 128), jnp.int32)
    for r in range(2):
        for a in range(ANCHORS):
            lab_ref[r * 16 + a : r * 16 + a + 1, :] = lab[a, r : r + 1, :]
            idx_ref[r * 16 + a : r * 16 + a + 1, :] = idx[a, r : r + 1, :]
    p = p_ref[...]
    out = dot(w[...], p, ((1,), (1,)))
    o_ref[...] = out[0:720] + column[0:720]
    small_out = out[720:756] + box_column[0:36]
    for r in range(2):
        b_ref[r * 64 + 32 : r * 64 + 64, :] = jnp.zeros((32, 128), f32)
        b_ref[r * 64 : r * 64 + 36, :] = small_out[:, r * 128 : r * 128 + 128]
    cls = lax.broadcasted_iota(jnp.int32, (CLASSES, 128), 0)

    def one_anchor(a, carry):
        sums = []
        at = pl.multiple_of(a * CLASSES, 16)
        for r in range(2):
            label = lab_ref[pl.ds(r * 16 + a, 1), :]
            x = o_ref[pl.ds(at, CLASSES), r * 128 : r * 128 + 128]
            hit = label == cls
            z = jnp.where(hit, -x, x)
            e = jnp.exp(-jnp.abs(z))
            soft = jnp.maximum(z, 0.0) + jnp.log1p(e)
            big = 1.0 / (1.0 + e)
            small = e * big
            up = z >= 0.0
            q = jnp.where(up, big, small)
            rest = jnp.where(up, small, big)
            counted = (label >= -1).astype(f32)
            w = jnp.where(hit, FOCAL_ALPHA, 1.0 - FOCAL_ALPHA) * counted
            wq = w * q * q
            dz = wq * (q + 2.0 * rest * soft)
            g_ref[pl.ds(at, CLASSES), r * 128 : r * 128 + 128] = jnp.where(hit, -dz, dz).astype(bf16)
            sums.append(carry[r] + jnp.sum(wq * soft, axis=0, keepdims=True))
        return tuple(sums)

    zero = jnp.zeros((1, 128), f32)
    focal = lax.fori_loop(0, ANCHORS, one_anchor, (zero, zero))

    aw, ah = anchor_sizes((16, 128))
    cx = (lax.broadcasted_iota(jnp.int32, (16, 128), 1).astype(f32) + 0.5) * STRIDE
    for r in range(2):
        cy = (jnp.full((16, 128), first[0] + r, jnp.int32).astype(f32) + 0.5) * STRIDE
        which = idx_ref[r * 16 : r * 16 + 16, :]
        corner = [
            jnp.take_along_axis(jnp.broadcast_to(box_ref[k : k + 1, :], (16, 128)), which, axis=1) for k in range(4)
        ]
        positive = lab_ref[r * 16 : r * 16 + 16, :] >= 0
        o = [b_ref[pl.ds(r * 64 + k, 16, stride=4), :] for k in range(4)]
        value, pull = jax.vjp(
            lambda o0, o1, o2, o3: giou_terms(o0, o1, o2, o3, aw, ah, cx, cy, *corner), *o
        )
        grads = pull(jnp.ones((16, 128), f32))
        for k in range(4):
            gb_ref[pl.ds(r * 64 + k, 16, stride=4), :] = jnp.where(positive, grads[k], 0.0)
        giou = jnp.sum(jnp.where(positive, value, 0.0), axis=0, keepdims=True)
        count = jnp.sum(positive.astype(f32), axis=0, keepdims=True)
        rows = []
        for v in (focal[r], giou):
            hi = v.astype(bf16).astype(f32)
            rows += [hi, v - hi]
        rows.append(count)
        for n, v in enumerate(rows):
            gb_ref[r * 64 + 36 + n : r * 64 + 37 + n, :] = v
        g_ref[720:768, r * 128 : r * 128 + 128] = gb_ref[r * 64 : r * 64 + 48, :].astype(bf16)
    g_out[...] = g_ref[...]
    keep[...] = g_ref[pl.ds(pl.multiple_of(ci[0] * HALF, 16), HALF), :]
    send[...] = g_ref[pl.ds(pl.multiple_of((1 - ci[0]) * HALF, 16), HALF), :]


def tower_kernel(ci, g, w_ref, unused, mid, outer, inner, token):
    token[...] = jnp.zeros((8, 128), f32)
    gt = g[...].astype(f32).T
    gj = []
    for j in range(3):
        gj.append(
            jnp.concatenate([shifted(gt[r * 128 : r * 128 + 128], 2 - j) for r in range(2)], axis=0).astype(bf16)
        )
    t = []
    for i in range(3):
        acc = jnp.zeros((256, 256), f32)
        for j in range(3):
            at = (3 * i + j) * 256
            acc = acc + dot(gj[j], w_ref[:, at : at + 256], ((1,), (0,)))
        t.append(acc)
    low = jnp.full((128, 256), ci[0], jnp.int32) == 0
    up = t[0][0:128]
    down = t[2][128:256]
    outer[0] = jnp.where(low, up, down).astype(bf16)
    inner[0] = jnp.where(low, down, up).astype(bf16)
    mid[0] = t[1][0:128] + t[0][128:256]
    mid[1] = t[1][128:256] + t[2][0:128]


def tower_end_kernel(ci, mid, outer, inner, t_ref, token):
    token[...] = jnp.zeros((8, 128), f32)
    c = ci[0]
    t_ref[0, c] = (mid[c] + outer[0].astype(f32)).astype(bf16)
    t_ref[0, 1 - c] = (mid[1 - c] + inner[0].astype(f32)).astype(bf16)


def weight_kernel(yi, xi, ci, keep, got, outer, own, inner, other_edge, *refs):
    outs = refs[0:4]
    token, t_ref, s_ref, g_ref, m_ref = refs[4:]
    token[...] = jnp.zeros((8, 128), f32)
    c = ci[0]
    t_ref[5 * c] = outer[1 - c]
    t_ref[5 - 5 * c] = other_edge[0]
    for r in range(2):
        t_ref[1 + 2 * c + r] = own[r]
        t_ref[3 - 2 * c + r] = inner[r]
    g_ref[c] = keep[...]
    g_ref[1 - c] = got[...]

    def shift(row, carry):
        x = t_ref[row].astype(f32)
        at = pl.multiple_of(row * 128, 128)
        for j in range(3):
            s_ref[j, pl.ds(at, 128), :] = shifted(x, j).astype(bf16)
        return carry

    lax.fori_loop(0, 6, shift, 0)
    lhs = jnp.concatenate([g_ref[0], g_ref[1]], axis=1)
    for tap in range(9):
        i, j = divmod(tap, 3)
        acc = dot(lhs, s_ref[j, i * 128 : i * 128 + 512, :], ((1,), (0,)))
        for m in range(16):
            for rb in range(3):
                row = m * BLOCK + rb * 8
                both = jnp.concatenate([acc[row : row + 8, 0:128], acc[row : row + 8, 128:256]], axis=0)
                v = (rb * 18 + 2 * tap) * 8
                m_ref[m, v : v + 16, :] = both.astype(bf16)
    bias = dot(jnp.ones((8, 512), bf16), lhs, ((1,), (1,)))
    for m in range(16):
        tile, off = divmod(m * BLOCK, 128)
        e = bias[:, tile * 128 : tile * 128 + 128]
        e = e if off == 0 else pltpu.roll(e, 128 - off, 1)
        if off + BLOCK > 128:
            past = pltpu.roll(bias[:, tile * 128 + 128 : tile * 128 + 256], 128 - off, 1)
            lane = lax.broadcasted_iota(jnp.int32, (8, 128), 1)
            e = jnp.where(lane < 128 - off, e, past)
        hi = e.astype(bf16).astype(f32)
        m_ref[m, 432:448, :] = jnp.concatenate([hi, e - hi], axis=0).astype(bf16)
    for k in range(4):
        for q in range(4):
            outs[k][q] = m_ref[jnp.where(c == 0, ((yi[0] + k) & 3) * 4 + q, q * 4 + ((xi[0] + k) & 3))]


def row_sum_kernel(yi, xi, ci, *refs):
    parts = refs[0:4]
    outs = refs[5:9]
    here = jnp.where(ci[0] == 0, xi[0], yi[0])
    for k in range(4):
        q = (here + k) & 3
        acc = parts[0][q].astype(f32)
        for n in range(1, 4):
            acc = acc + parts[n][q].astype(f32)
        e = acc[432:440] + acc[440:448]
        hi = e.astype(bf16).astype(f32)
        outs[k][0:432, :] = acc[0:432].astype(bf16)
        outs[k][432:448, :] = jnp.concatenate([hi, e - hi], axis=0).astype(bf16)


def block_sum_kernel(zi, a, b, c, d, s_ref):
    acc = (a[...].astype(f32) + b[...].astype(f32)) + (c[...].astype(f32) + d[...].astype(f32))
    e = acc[432:440] + acc[440:448]
    hi = e.astype(bf16).astype(f32)
    s_ref[0:432, :] = acc[0:432].astype(bf16)
    s_ref[432:448, :] = jnp.concatenate([hi, e - hi], axis=0).astype(bf16)


def piece_sum_kernel(zi, m_ref, c_ref):
    acc = m_ref[0].astype(f32)
    for m in range(1, 8):
        acc = acc + m_ref[m].astype(f32)
    last = jnp.full((8, 128), zi[0], jnp.int32) == 7
    e = acc[40:48] + acc[48:56]
    hi = e.astype(bf16).astype(f32)
    out = jnp.concatenate(
        [acc[0:40], jnp.where(last, hi, acc[40:48]), jnp.where(last, e - hi, acc[48:56])], axis=0
    ).astype(bf16)
    for z in range(8):
        c_ref[z] = out


def join_kernel(a, b, c, d, o_ref):
    for k, ref in enumerate((a, b, c, d)):
        o_ref[k] = ref[...]


LAST = 5


def block_of(yi, xi, ci, n, k):
    c = ci[0] if n < 4 else 1 - ci[0]
    far = n % 4
    y = (yi[0] - jnp.where(c == 0, far, k)) & 3
    x = (xi[0] - jnp.where(c == 0, k, far)) & 3
    return c * 16 + y * 4 + x


def squares(yi, xi, ci, n, src):
    srow = lax.broadcasted_iota(jnp.int32, (8, 128), 0)
    lane = lax.broadcasted_iota(jnp.int32, (8, 128), 1)

    def one(k, total):
        base = block_of(yi, xi, ci, n, k) * BLOCK
        for rb in range(3):
            acc = jnp.zeros((16, 128), f32)
            for t in range(9):
                v = src[k, (rb * 9 + t) * 16 : (rb * 9 + t) * 16 + 16, :].astype(f32)
                acc = acc + v * v
            ok = base + rb * 8 + srow < VALID
            total = total + jnp.where(ok, acc[0:8] + acc[8:16], 0.0)
        e = src[k, 432:448, :].astype(f32)
        e = e[0:8] + e[8:16]
        ok = (base + lane < VALID) & (lane < BLOCK) & (srow == 0)
        return total + jnp.where(ok, e * e, 0.0)

    return one


def squares_kernel(yi, xi, ci, *refs):
    total = jnp.zeros((8, 128), f32)
    for n, src in zip([n for n in range(8) if n != LAST], refs[:7]):
        total = lax.fori_loop(0, 4, squares(yi, xi, ci, n, src), total)
    refs[7][...] = total


def final_kernel(yi, xi, ci, *refs):
    sources = refs[0:8]
    partial, cw_out, bw_out, cb_out, bb_out, loss, w_ref, e_ref, row_ref, sem = refs[8:]
    srow = lax.broadcasted_iota(jnp.int32, (8, 128), 0)
    lane = lax.broadcasted_iota(jnp.int32, (8, 128), 1)
    total = lax.fori_loop(0, 4, squares(yi, xi, ci, LAST, sources[LAST]), partial[...])
    mean = jnp.sum(total) * (1.0 / (VALID * 2305))
    scale = lax.rsqrt(jnp.full((8, 128), mean + NORM_EPS, f32))

    def chunk(block):
        rows = pl.ds(pl.multiple_of(block * BLOCK, 8), BLOCK)
        return pltpu.make_async_copy(w_ref.at[rows], cw_out.at[rows], sem)

    def write(n):
        src = sources[n]

        def one(k, carry):
            block = block_of(yi, xi, ci, n, k)
            e = src[k, 432:448, :].astype(f32)
            e_ref[block] = e[0:8] + e[8:16]
            for rb in range(3):
                row = pl.multiple_of(block * BLOCK + rb * 8, 8)
                for t in range(9):
                    v = src[k, (rb * 9 + t) * 16 : (rb * 9 + t) * 16 + 16, :].astype(f32)
                    w_ref[pl.ds(row, 8), t * 256 : t * 256 + 128] = v[0:8] * scale
                    w_ref[pl.ds(row, 8), t * 256 + 128 : t * 256 + 256] = v[8:16] * scale

            @pl.when(block < 30)
            def _():
                chunk(block).start()

            return carry

        return one

    for n in range(8):
        lax.fori_loop(0, 4, write(n), 0)
    bw_out[...] = w_ref[720:756, :]
    row_ref[...] = jnp.zeros((8, 896), f32)
    for block in range(32):
        tile, off = divmod(block * BLOCK, 128)
        e = e_ref[block] * scale
        e = e if off == 0 else pltpu.roll(e, off, 1)
        here = (lane >= off) & (lane < off + BLOCK)
        row_ref[:, tile * 128 : tile * 128 + 128] = jnp.where(here, e, row_ref[:, tile * 128 : tile * 128 + 128])
        if off + BLOCK > 128:
            past = lane < off + BLOCK - 128
            row_ref[:, tile * 128 + 128 : tile * 128 + 256] = jnp.where(past, e, 0.0)
    cb_out[...] = row_ref[0, 0:720]
    bb_out[...] = pltpu.roll(row_ref[:, 640:768], 128 - 80, 1)[0, 0:36]
    e = jnp.where(srow == 0, e_ref[31], 0.0)
    sums = jnp.sum(jnp.where((lane >= 12) & (lane < 16), e, 0.0))
    count = jnp.sum(jnp.where(lane == 16, e, 0.0))
    loss[...] = jnp.full((1, 128), sums, f32) / jnp.full((1, 128), count, f32)

    def drain(k, carry):
        chunk(k).wait()
        return carry

    lax.fori_loop(0, 30, drain, 0)


VMEM = pl.BlockSpec(memory_space=pltpu.VMEM)
SMEM = pl.BlockSpec(memory_space=pltpu.SMEM)
ANY = pl.BlockSpec(memory_space=pl.ANY)


def near_memory(arrays):
    return [pltpu.with_memory_space_constraint(v, pltpu.VMEM) for v in arrays]


def far_memory(arrays):
    return [pltpu.with_memory_space_constraint(v, pltpu.HBM) for v in arrays]


def shape(*dims, dtype=f32):
    return jax.ShapeDtypeStruct(dims, dtype)


def stage(cw, bw):
    return pl.pallas_call(
        stage_kernel,
        out_shape=pltpu.VMEM((ROWS_ALL, 2304), bf16),
        in_specs=[ANY, VMEM],
        out_specs=VMEM,
        scratch_shapes=[pltpu.SemaphoreType.DMA],
        compiler_params=pltpu.CompilerParams(vmem_limit_bytes=LIMIT),
        name="stage",
    )(*far_memory([cw, bw]))


def head(first, ci, outer, own, inner, w, cb, bb, lab, idx, box):
    return pl.pallas_call(
        head_kernel,
        out_shape=[
            pltpu.HBM((ROWS_ALL, 256), bf16),
            pltpu.HBM((HALF, 256), bf16),
            pltpu.HBM((HALF, 256), bf16),
            pltpu.VMEM((1, 128, 256), bf16),
        ],
        in_specs=[SMEM] * 2 + [VMEM] * 9,
        out_specs=[VMEM] * 4,
        scratch_shapes=[
            pltpu.VMEM((256, 2304), bf16),
            pltpu.VMEM((720, 256), f32),
            pltpu.VMEM((128, 128), f32),
            pltpu.VMEM((128, 128), f32),
            pltpu.VMEM((ROWS_ALL, 256), bf16),
            pltpu.VMEM((16, 768), f32),
            pltpu.VMEM((8, 128), f32),
            pltpu.VMEM((32, 128), jnp.int32),
            pltpu.VMEM((32, 128), jnp.int32),
            pltpu.VMEM((4, 128, 256), bf16),
        ],
        compiler_params=pltpu.CompilerParams(vmem_limit_bytes=LIMIT),
        name="head",
    )(first, ci, *far_memory([outer, own, inner]), *near_memory([w]), *far_memory([cb, bb, lab, idx, box]))


def tower_terms(ci, g, w, after):
    return pl.pallas_call(
        tower_kernel,
        out_shape=(
            pltpu.HBM((2, 128, 256), f32),
            pltpu.VMEM((1, 128, 256), bf16),
            pltpu.VMEM((1, 128, 256), bf16),
            shape(8, 128),
        ),
        in_specs=[SMEM, VMEM, VMEM, ANY],
        out_specs=(VMEM, VMEM, VMEM, VMEM),
        compiler_params=pltpu.CompilerParams(vmem_limit_bytes=LIMIT),
        name="tower_terms",
        cost_estimate=pl.CostEstimate(flops=2 * 756 * 2304 * 256, transcendentals=0, bytes_accessed=4500000),
    )(ci, *far_memory([g]), *near_memory([w]), after)


def tower_end(ci, mid, outer, inner):
    return pl.pallas_call(
        tower_end_kernel,
        out_shape=(shape(1, 2, 128, 256, dtype=bf16), shape(8, 128)),
        in_specs=[SMEM] + [VMEM] * 3,
        out_specs=(VMEM, VMEM),
        compiler_params=pltpu.CompilerParams(vmem_limit_bytes=LIMIT),
        name="tower_end",
    )(ci, *far_memory([mid]), outer, inner)


def weight_terms(yi, xi, ci, keep, got, outer, own, inner, other_edge):
    return pl.pallas_call(
        weight_kernel,
        out_shape=[pltpu.VMEM((4, PIECE, 128), bf16)] * 4 + [shape(8, 128)],
        in_specs=[SMEM] * 3 + [VMEM] * 6,
        out_specs=[VMEM] * 5,
        scratch_shapes=[
            pltpu.VMEM((6, 128, 256), bf16),
            pltpu.VMEM((3, 768, 256), bf16),
            pltpu.VMEM((2, HALF, 256), bf16),
            pltpu.VMEM((16, PIECE, 128), bf16),
        ],
        compiler_params=pltpu.CompilerParams(vmem_limit_bytes=LIMIT),
        name="weight_terms",
    )(yi, xi, ci, *far_memory([keep, got, outer, own, inner]), other_edge)


def row_sum(yi, xi, ci, parts, after):
    return pl.pallas_call(
        row_sum_kernel,
        out_shape=[pltpu.VMEM((PIECE, 128), bf16)] * 4,
        in_specs=[SMEM] * 3 + [VMEM] * 4 + [ANY],
        out_specs=[VMEM] * 4,
        compiler_params=pltpu.CompilerParams(vmem_limit_bytes=LIMIT),
        name="row_sum",
    )(yi, xi, ci, *near_memory(parts), after)


def block_sum(zi, parts):
    return pl.pallas_call(
        block_sum_kernel,
        out_shape=pltpu.VMEM((PIECE, 128), bf16),
        in_specs=[SMEM] + [VMEM] * 4,
        out_specs=VMEM,
        compiler_params=pltpu.CompilerParams(vmem_limit_bytes=LIMIT),
        name="block_sum",
    )(zi, *near_memory(parts))


def piece_sum(zi, m):
    return pl.pallas_call(
        piece_sum_kernel,
        out_shape=pltpu.VMEM((8, 56, 128), bf16),
        in_specs=[SMEM, VMEM],
        out_specs=VMEM,
        compiler_params=pltpu.CompilerParams(vmem_limit_bytes=LIMIT),
        name="piece_sum",
    )(zi, *near_memory([m]))


def join(parts):
    return pl.pallas_call(
        join_kernel,
        out_shape=pltpu.VMEM((4, PIECE, 128), bf16),
        in_specs=[VMEM] * 4,
        out_specs=VMEM,
        compiler_params=pltpu.CompilerParams(vmem_limit_bytes=LIMIT),
        name="join",
    )(*near_memory(parts))


def squares_of(yi, xi, ci, pieces):
    return pl.pallas_call(
        squares_kernel,
        out_shape=pltpu.VMEM((8, 128), f32),
        in_specs=[SMEM] * 3 + [VMEM] * 7,
        out_specs=VMEM,
        compiler_params=pltpu.CompilerParams(vmem_limit_bytes=LIMIT),
        name="squares",
    )(yi, xi, ci, *near_memory(pieces))


def finish(yi, xi, ci, pieces, partial):
    return pl.pallas_call(
        final_kernel,
        out_shape=(shape(720, 2304), shape(36, 2304), shape(720), shape(36), shape(1, 128)),
        in_specs=[SMEM] * 3 + [VMEM] * 9,
        out_specs=(ANY, VMEM, VMEM, VMEM, VMEM),
        scratch_shapes=[
            pltpu.VMEM((ROWS_ALL, 2304), f32),
            pltpu.VMEM((32, 8, 128), f32),
            pltpu.VMEM((8, 896), f32),
            pltpu.SemaphoreType.DMA,
        ],
        compiler_params=pltpu.CompilerParams(vmem_limit_bytes=LIMIT),
        name="finish",
    )(yi, xi, ci, *near_memory([*pieces, partial]))


def swap(value):
    return lax.ppermute(value, "core", [(0, 1), (1, 0)])


def across(value):
    pairs = [(t, t + 1) for t in range(1, 31, 2)]
    return lax.ppermute(value, TILE_AXES, pairs + [(b, a) for a, b in pairs])


def along(value, k, first_axis):
    pairs = []
    for y in range(4):
        for c in range(2):
            for x in range(4):
                dx = k if (first_axis == "x") == (c == 0) else 0
                dy = k - dx
                pairs.append(((y * 2 + c) * 4 + x, (((y + dy) % 4) * 2 + c) * 4 + (x + dx) % 4))
    return lax.ppermute(value, ("y", "core", "x"), pairs)


def per_device(tower, cls_weight, cls_bias, box_weight, box_bias, labels, target_index, boxes):
    own = tower[0]
    outer = across(own)
    inner = swap(own)
    ci = lax.axis_index("core").reshape(1)
    yi = lax.axis_index("y").reshape(1)
    xi = lax.axis_index("x").reshape(1)
    zi = (lax.axis_index("zlo") * 2 + lax.axis_index("zhi")).reshape(1)
    first = (lax.axis_index(TILE_AXES) * 2).reshape(1)

    w = stage(cls_weight, box_weight)
    g, keep, send, edge = head(
        first, ci, outer, own, inner, w, cls_bias, box_bias, labels[0], target_index[0], boxes[0]
    )
    *parts, token = weight_terms(yi, xi, ci, keep, swap(send), outer, own, inner, swap(edge))

    mid, to_outer, to_inner, _ = tower_terms(ci, g, w, token)
    tower_grad, end_token = tower_end(ci, mid, across(to_outer), swap(to_inner))

    parts = [parts[0]] + [along(parts[k], k, "y") for k in (1, 2, 3)]
    parts = row_sum(yi, xi, ci, parts, end_token)
    parts = [parts[0]] + [along(parts[k], k, "x") for k in (1, 2, 3)]
    terms = lax.all_to_all(block_sum(zi, parts).reshape(8, 56, 128), ("zlo", "zhi"), 0, 0, tiled=True)
    copies = lax.all_to_all(piece_sum(zi, terms), ("zlo", "zhi"), 0, 0, tiled=True)
    block = copies.reshape(PIECE, 128)
    row = join([block] + [along(block, k, "x") for k in (1, 2, 3)])
    mine = [row] + [along(row, k, "y") for k in (1, 2, 3)]
    pieces = mine + [swap(v) for v in mine]
    partial = squares_of(yi, xi, ci, pieces[:LAST] + pieces[LAST + 1 :])
    cw_grad, bw_grad, cb_grad, bb_grad, loss = finish(yi, xi, ci, pieces, partial)
    return loss[0, 0], cw_grad, cb_grad, bw_grad, bb_grad, tower_grad


def solution(mesh):
    fine = Mesh(mesh.devices.reshape(4, 4, 2, 4, 2), ("zlo", "y", "core", "x", "zhi"))
    placed = (
        P(IMG_AXES, TILE_AXES, None, None),
        P(),
        P(),
        P(),
        P(),
        P(IMG_AXES, None, TILE_AXES, None),
        P(IMG_AXES, None, TILE_AXES, None),
        P(IMG_AXES, None, None),
    )
    return jax.shard_map(
        per_device,
        mesh=fine,
        in_specs=placed,
        out_specs=(P(), P(), P(), P(), P(), P(IMG_AXES, TILE_AXES, None, None)),
        check_vma=False,
    )
```

```python
import jax
import jax.numpy as jnp
from jax import lax
from jax.experimental import pallas as pl
from jax.experimental.pallas import tpu as pltpu
from jax.sharding import Mesh, PartitionSpec as P

CLASSES = 80
ANCHORS = 9
STRIDE = 8
FOCAL_ALPHA = 0.25
NORM_EPS = 1e-06

ROWS_ALL = 768
VALID = 756
HALF = 384
GROUP_ROWS = 96
BLOCK = 24
TILES = 56
PIECE = 448

LIMIT = 24 << 20

TILE_AXES = ("zlo", "y", "core")
IMG_AXES = ("x", "zhi")

f32 = jnp.float32
bf16 = jnp.bfloat16


def dot(a, b, dims):
    return lax.dot_general(a, b, (dims, ((), ())), preferred_element_type=f32)


def shifted(x, j):
    if j == 1:
        return x
    ids = lax.broadcasted_iota(jnp.int32, x.shape, 0)
    if j == 0:
        return jnp.where(ids == 0, 0.0, pltpu.roll(x, 1, 0))
    return jnp.where(ids == x.shape[0] - 1, 0.0, pltpu.roll(x, x.shape[0] - 1, 0))


def fill_patches(rows, p_ref):
    for e, row in enumerate(rows):
        if row is None:
            continue
        x = row.astype(f32)
        for j in range(3):
            v = shifted(x, j).astype(bf16)
            for i in range(3):
                r = e - i
                if 0 <= r < 2:
                    p_ref[r * 128 : r * 128 + 128, (3 * i + j) * 256 : (3 * i + j) * 256 + 256] = v


def anchor_sizes(shape):
    ids = lax.broadcasted_iota(jnp.int32, shape, 0)
    w = jnp.ones(shape, f32)
    h = jnp.ones(shape, f32)
    for a in range(ANCHORS):
        base = 4.0 * STRIDE * 2.0 ** ((a // 3) / 3.0)
        ratio = a % 3 - 1
        w = jnp.where(ids == a, base * 2.0 ** (-ratio / 2.0), w)
        h = jnp.where(ids == a, base * 2.0 ** (ratio / 2.0), h)
    return w, h


def giou_terms(o0, o1, o2, o3, aw, ah, cx, cy, tl, tt, tr, tb):
    mx = cx + o0 * aw
    my = cy + o1 * ah
    pw = aw * jnp.exp(o2)
    ph = ah * jnp.exp(o3)
    left = mx - 0.5 * pw
    right = mx + 0.5 * pw
    top = my - 0.5 * ph
    bottom = my + 0.5 * ph
    iw = jnp.maximum(jnp.minimum(right, tr) - jnp.maximum(left, tl), 0.0)
    ih = jnp.maximum(jnp.minimum(bottom, tb) - jnp.maximum(top, tt), 0.0)
    inter = iw * ih
    union = pw * ph + (tr - tl) * (tb - tt) - inter
    ow = jnp.maximum(right, tr) - jnp.minimum(left, tl)
    oh = jnp.maximum(bottom, tb) - jnp.minimum(top, tt)
    outer = ow * oh
    return 1.0 - (inter / union - (outer - union) / outer)


def stage_kernel(cw, bw, own, cb, bb, lab, idx, box, w_ref, part_ref, lab_ref, idx_ref, box_ref, row_ref, p_ref, sem):
    copy = pltpu.make_async_copy(cw, w_ref.at[pl.ds(0, 720)], sem)
    copy.start()
    w_ref[752:768, :] = jnp.zeros((16, 2304), bf16)
    w_ref[720:756, :] = bw[...]
    fill_patches([None, own[0], own[1], None], p_ref)
    p_ref[0:128, 0:768] = jnp.zeros((128, 768), bf16)
    p_ref[128:256, 1536:2304] = jnp.zeros((128, 768), bf16)
    row_ref[...] = jnp.zeros((16, 768), f32)
    row_ref[0, 0:720] = cb[...]
    row_ref[8, 0:36] = bb[...]
    bias = jnp.concatenate([row_ref[0:8, :].T[0:720, 0:1], row_ref[8:16, 0:128].T[0:48, 0:1]], axis=0)
    box_ref[...] = jnp.zeros((8, 128), f32)
    box_ref[0:4, 0:100] = box[...]
    lab_ref[...] = jnp.full((32, 128), -2, jnp.int32)
    idx_ref[...] = jnp.zeros((32, 128), jnp.int32)
    for r in range(2):
        for a in range(ANCHORS):
            lab_ref[r * 16 + a : r * 16 + a + 1, :] = lab[a, r : r + 1, :]
            idx_ref[r * 16 + a : r * 16 + a + 1, :] = idx[a, r : r + 1, :]
    copy.wait()
    part_ref[...] = dot(w_ref[...], p_ref[...], ((1,), (1,))) + bias


def head_kernel(first, ci, outer, inner, w, part, lab_ref, idx_ref, box_ref, *refs):
    g_out, keep, send, edge = refs[0:4]
    p_ref, o_ref, b_ref, gb_ref, g_ref, ext_ref = refs[4:]
    c = ci[0]
    edge[0] = outer[1 - c]
    ext_ref[3 * c] = outer[1 - c]
    ext_ref[3 - 3 * c] = inner[c]
    for n in range(2):
        x = ext_ref[3 * n].astype(f32)
        for j in range(3):
            p_ref[n, :, j * 256 : j * 256 + 256] = shifted(x, j).astype(bf16)
    small_out = []
    for n in range(2):
        out = dot(w[:, 1536 * n : 1536 * n + 768], p_ref[n], ((1,), (1,))) + part[:, n * 128 : n * 128 + 128]
        o_ref[:, n * 128 : n * 128 + 128] = out[0:720]
        small_out.append(out[720:756])
    for r in range(2):
        b_ref[r * 64 + 32 : r * 64 + 64, :] = jnp.zeros((32, 128), f32)
        b_ref[r * 64 : r * 64 + 36, :] = small_out[r]
    cls = lax.broadcasted_iota(jnp.int32, (CLASSES, 128), 0)

    def one_anchor(a, carry):
        sums = []
        at = pl.multiple_of(a * CLASSES, 16)
        for r in range(2):
            label = lab_ref[pl.ds(r * 16 + a, 1), :]
            x = o_ref[pl.ds(at, CLASSES), r * 128 : r * 128 + 128]
            hit = label == cls
            z = jnp.where(hit, -x, x)
            e = jnp.exp(-jnp.abs(z))
            soft = jnp.maximum(z, 0.0) + jnp.log1p(e)
            big = 1.0 / (1.0 + e)
            small = e * big
            up = z >= 0.0
            q = jnp.where(up, big, small)
            rest = jnp.where(up, small, big)
            counted = (label >= -1).astype(f32)
            w = jnp.where(hit, FOCAL_ALPHA, 1.0 - FOCAL_ALPHA) * counted
            wq = w * q * q
            dz = wq * (q + 2.0 * rest * soft)
            g_ref[pl.ds(at, CLASSES), r * 128 : r * 128 + 128] = jnp.where(hit, -dz, dz).astype(bf16)
            sums.append(carry[r] + jnp.sum(wq * soft, axis=0, keepdims=True))
        return tuple(sums)

    zero = jnp.zeros((1, 128), f32)
    focal = lax.fori_loop(0, ANCHORS, one_anchor, (zero, zero))

    aw, ah = anchor_sizes((16, 128))
    cx = (lax.broadcasted_iota(jnp.int32, (16, 128), 1).astype(f32) + 0.5) * STRIDE
    for r in range(2):
        cy = (jnp.full((16, 128), first[0] + r, jnp.int32).astype(f32) + 0.5) * STRIDE
        which = idx_ref[r * 16 : r * 16 + 16, :]
        corner = [
            jnp.take_along_axis(jnp.broadcast_to(box_ref[k : k + 1, :], (16, 128)), which, axis=1) for k in range(4)
        ]
        positive = lab_ref[r * 16 : r * 16 + 16, :] >= 0
        o = [b_ref[pl.ds(r * 64 + k, 16, stride=4), :] for k in range(4)]
        value, pull = jax.vjp(
            lambda o0, o1, o2, o3: giou_terms(o0, o1, o2, o3, aw, ah, cx, cy, *corner), *o
        )
        grads = pull(jnp.ones((16, 128), f32))
        for k in range(4):
            gb_ref[pl.ds(r * 64 + k, 16, stride=4), :] = jnp.where(positive, grads[k], 0.0)
        giou = jnp.sum(jnp.where(positive, value, 0.0), axis=0, keepdims=True)
        count = jnp.sum(positive.astype(f32), axis=0, keepdims=True)
        rows = []
        for v in (focal[r], giou):
            hi = v.astype(bf16).astype(f32)
            rows += [hi, v - hi]
        rows.append(count)
        for n, v in enumerate(rows):
            gb_ref[r * 64 + 36 + n : r * 64 + 37 + n, :] = v
        g_ref[720:768, r * 128 : r * 128 + 128] = gb_ref[r * 64 : r * 64 + 48, :].astype(bf16)
    g_out[...] = g_ref[...]
    keep[...] = g_ref[pl.ds(pl.multiple_of(ci[0] * HALF, 16), HALF), :]
    send[...] = g_ref[pl.ds(pl.multiple_of((1 - ci[0]) * HALF, 16), HALF), :]


def tower_kernel(ci, g, w_ref, unused, mid, outer, inner, token):
    token[...] = jnp.zeros((8, 128), f32)
    gt = g[...].astype(f32).T
    gj = []
    for j in range(3):
        gj.append(
            jnp.concatenate([shifted(gt[r * 128 : r * 128 + 128], 2 - j) for r in range(2)], axis=0).astype(bf16)
        )
    t = []
    for i in range(3):
        acc = jnp.zeros((256, 256), f32)
        for j in range(3):
            at = (3 * i + j) * 256
            acc = acc + dot(gj[j], w_ref[:, at : at + 256], ((1,), (0,)))
        t.append(acc)
    low = jnp.full((128, 256), ci[0], jnp.int32) == 0
    up = t[0][0:128]
    down = t[2][128:256]
    outer[0] = jnp.where(low, up, down).astype(bf16)
    inner[0] = jnp.where(low, down, up).astype(bf16)
    mid[0] = t[1][0:128] + t[0][128:256]
    mid[1] = t[1][128:256] + t[2][0:128]


def tower_end_kernel(ci, mid, outer, inner, t_ref, token):
    token[...] = jnp.zeros((8, 128), f32)
    c = ci[0]
    t_ref[0, c] = (mid[c] + outer[0].astype(f32)).astype(bf16)
    t_ref[0, 1 - c] = (mid[1 - c] + inner[0].astype(f32)).astype(bf16)


def weight_kernel(yi, xi, ci, keep, got, outer, own, inner, other_edge, *refs):
    outs = refs[0:4]
    token, t_ref, s_ref, g_ref, m_ref = refs[4:]
    token[...] = jnp.zeros((8, 128), f32)
    c = ci[0]
    t_ref[5 * c] = outer[1 - c]
    t_ref[5 - 5 * c] = other_edge[0]
    for r in range(2):
        t_ref[1 + 2 * c + r] = own[r]
        t_ref[3 - 2 * c + r] = inner[r]
    g_ref[c] = keep[...]
    g_ref[1 - c] = got[...]

    def shift(row, carry):
        x = t_ref[row].astype(f32)
        at = pl.multiple_of(row * 128, 128)
        for j in range(3):
            s_ref[j, pl.ds(at, 128), :] = shifted(x, j).astype(bf16)
        return carry

    lax.fori_loop(0, 6, shift, 0)
    lhs = jnp.concatenate([g_ref[0], g_ref[1]], axis=1)
    for tap in range(9):
        i, j = divmod(tap, 3)
        acc = dot(lhs, s_ref[j, i * 128 : i * 128 + 512, :], ((1,), (0,)))
        for m in range(16):
            for rb in range(3):
                row = m * BLOCK + rb * 8
                both = jnp.concatenate([acc[row : row + 8, 0:128], acc[row : row + 8, 128:256]], axis=0)
                v = (rb * 18 + 2 * tap) * 8
                m_ref[m, v : v + 16, :] = both.astype(bf16)
    bias = dot(jnp.ones((8, 512), bf16), lhs, ((1,), (1,)))
    for m in range(16):
        tile, off = divmod(m * BLOCK, 128)
        e = bias[:, tile * 128 : tile * 128 + 128]
        e = e if off == 0 else pltpu.roll(e, 128 - off, 1)
        if off + BLOCK > 128:
            past = pltpu.roll(bias[:, tile * 128 + 128 : tile * 128 + 256], 128 - off, 1)
            lane = lax.broadcasted_iota(jnp.int32, (8, 128), 1)
            e = jnp.where(lane < 128 - off, e, past)
        hi = e.astype(bf16).astype(f32)
        m_ref[m, 432:448, :] = jnp.concatenate([hi, e - hi], axis=0).astype(bf16)
    for k in range(4):
        for q in range(4):
            outs[k][q] = m_ref[jnp.where(c == 0, ((yi[0] + k) & 3) * 4 + q, q * 4 + ((xi[0] + k) & 3))]


def row_sum_kernel(yi, xi, ci, *refs):
    parts = refs[0:4]
    outs = refs[5:9]
    here = jnp.where(ci[0] == 0, xi[0], yi[0])
    for k in range(4):
        q = (here + k) & 3
        acc = parts[0][q].astype(f32)
        for n in range(1, 4):
            acc = acc + parts[n][q].astype(f32)
        e = acc[432:440] + acc[440:448]
        hi = e.astype(bf16).astype(f32)
        outs[k][0:432, :] = acc[0:432].astype(bf16)
        outs[k][432:448, :] = jnp.concatenate([hi, e - hi], axis=0).astype(bf16)


def block_sum_kernel(zi, a, b, c, d, s_ref):
    acc = (a[...].astype(f32) + b[...].astype(f32)) + (c[...].astype(f32) + d[...].astype(f32))
    e = acc[432:440] + acc[440:448]
    hi = e.astype(bf16).astype(f32)
    s_ref[0:432, :] = acc[0:432].astype(bf16)
    s_ref[432:448, :] = jnp.concatenate([hi, e - hi], axis=0).astype(bf16)


def piece_sum_kernel(zi, m_ref, c_ref):
    acc = m_ref[0].astype(f32)
    for m in range(1, 8):
        acc = acc + m_ref[m].astype(f32)
    last = jnp.full((8, 128), zi[0], jnp.int32) == 7
    e = acc[40:48] + acc[48:56]
    hi = e.astype(bf16).astype(f32)
    out = jnp.concatenate(
        [acc[0:40], jnp.where(last, hi, acc[40:48]), jnp.where(last, e - hi, acc[48:56])], axis=0
    ).astype(bf16)
    for z in range(8):
        c_ref[z] = out


def join_kernel(a, b, c, d, o_ref):
    for k, ref in enumerate((a, b, c, d)):
        o_ref[k] = ref[...]


LAST = 5


def block_of(yi, xi, ci, n, k):
    c = ci[0] if n < 4 else 1 - ci[0]
    far = n % 4
    y = (yi[0] - jnp.where(c == 0, far, k)) & 3
    x = (xi[0] - jnp.where(c == 0, k, far)) & 3
    return c * 16 + y * 4 + x


def squares(yi, xi, ci, n, src):
    srow = lax.broadcasted_iota(jnp.int32, (8, 128), 0)
    lane = lax.broadcasted_iota(jnp.int32, (8, 128), 1)

    def one(k, total):
        base = block_of(yi, xi, ci, n, k) * BLOCK
        for rb in range(3):
            acc = jnp.zeros((16, 128), f32)
            for t in range(9):
                v = src[k, (rb * 9 + t) * 16 : (rb * 9 + t) * 16 + 16, :].astype(f32)
                acc = acc + v * v
            ok = base + rb * 8 + srow < VALID
            total = total + jnp.where(ok, acc[0:8] + acc[8:16], 0.0)
        e = src[k, 432:448, :].astype(f32)
        e = e[0:8] + e[8:16]
        ok = (base + lane < VALID) & (lane < BLOCK) & (srow == 0)
        return total + jnp.where(ok, e * e, 0.0)

    return one


def squares_kernel(yi, xi, ci, *refs):
    total = jnp.zeros((8, 128), f32)
    for n, src in zip([n for n in range(8) if n != LAST], refs[:7]):
        total = lax.fori_loop(0, 4, squares(yi, xi, ci, n, src), total)
    refs[7][...] = total


def final_kernel(yi, xi, ci, *refs):
    sources = refs[0:8]
    partial, cw_out, bw_out, cb_out, bb_out, loss, w_ref, e_ref, row_ref, sem = refs[8:]
    srow = lax.broadcasted_iota(jnp.int32, (8, 128), 0)
    lane = lax.broadcasted_iota(jnp.int32, (8, 128), 1)
    total = lax.fori_loop(0, 4, squares(yi, xi, ci, LAST, sources[LAST]), partial[...])
    mean = jnp.sum(total) * (1.0 / (VALID * 2305))
    scale = lax.rsqrt(jnp.full((8, 128), mean + NORM_EPS, f32))

    def chunk(block):
        rows = pl.ds(pl.multiple_of(block * BLOCK, 8), BLOCK)
        return pltpu.make_async_copy(w_ref.at[rows], cw_out.at[rows], sem)

    def write(n):
        src = sources[n]

        def one(k, carry):
            block = block_of(yi, xi, ci, n, k)
            e = src[k, 432:448, :].astype(f32)
            e_ref[block] = e[0:8] + e[8:16]
            for rb in range(3):
                row = pl.multiple_of(block * BLOCK + rb * 8, 8)
                for t in range(9):
                    v = src[k, (rb * 9 + t) * 16 : (rb * 9 + t) * 16 + 16, :].astype(f32)
                    w_ref[pl.ds(row, 8), t * 256 : t * 256 + 128] = v[0:8] * scale
                    w_ref[pl.ds(row, 8), t * 256 + 128 : t * 256 + 256] = v[8:16] * scale

            @pl.when(block < 30)
            def _():
                chunk(block).start()

            return carry

        return one

    for n in range(8):
        lax.fori_loop(0, 4, write(n), 0)
    bw_out[...] = w_ref[720:756, :]
    row_ref[...] = jnp.zeros((8, 896), f32)
    for block in range(32):
        tile, off = divmod(block * BLOCK, 128)
        e = e_ref[block] * scale
        e = e if off == 0 else pltpu.roll(e, off, 1)
        here = (lane >= off) & (lane < off + BLOCK)
        row_ref[:, tile * 128 : tile * 128 + 128] = jnp.where(here, e, row_ref[:, tile * 128 : tile * 128 + 128])
        if off + BLOCK > 128:
            past = lane < off + BLOCK - 128
            row_ref[:, tile * 128 + 128 : tile * 128 + 256] = jnp.where(past, e, 0.0)
    cb_out[...] = row_ref[0, 0:720]
    bb_out[...] = pltpu.roll(row_ref[:, 640:768], 128 - 80, 1)[0, 0:36]
    e = jnp.where(srow == 0, e_ref[31], 0.0)
    sums = jnp.sum(jnp.where((lane >= 12) & (lane < 16), e, 0.0))
    count = jnp.sum(jnp.where(lane == 16, e, 0.0))
    loss[...] = jnp.full((1, 128), sums, f32) / jnp.full((1, 128), count, f32)

    def drain(k, carry):
        chunk(k).wait()
        return carry

    lax.fori_loop(0, 30, drain, 0)


VMEM = pl.BlockSpec(memory_space=pltpu.VMEM)
SMEM = pl.BlockSpec(memory_space=pltpu.SMEM)
ANY = pl.BlockSpec(memory_space=pl.ANY)


def near_memory(arrays):
    return [pltpu.with_memory_space_constraint(v, pltpu.VMEM) for v in arrays]


def far_memory(arrays):
    return [pltpu.with_memory_space_constraint(v, pltpu.HBM) for v in arrays]


def shape(*dims, dtype=f32):
    return jax.ShapeDtypeStruct(dims, dtype)


def stage(cw, bw, own, cb, bb, lab, idx, box):
    return pl.pallas_call(
        stage_kernel,
        out_shape=[
            pltpu.VMEM((ROWS_ALL, 2304), bf16),
            pltpu.HBM((ROWS_ALL, 256), f32),
            pltpu.VMEM((32, 128), jnp.int32),
            pltpu.VMEM((32, 128), jnp.int32),
            pltpu.VMEM((8, 128), f32),
        ],
        in_specs=[ANY] + [VMEM] * 7,
        out_specs=[VMEM] * 5,
        scratch_shapes=[
            pltpu.VMEM((16, 768), f32),
            pltpu.VMEM((256, 2304), bf16),
            pltpu.SemaphoreType.DMA,
        ],
        compiler_params=pltpu.CompilerParams(vmem_limit_bytes=LIMIT),
        name="stage",
    )(*far_memory([cw, bw, own, cb, bb, lab, idx, box]))


def head(first, ci, outer, inner, w, part, *small):
    return pl.pallas_call(
        head_kernel,
        out_shape=[
            pltpu.HBM((ROWS_ALL, 256), bf16),
            pltpu.HBM((HALF, 256), bf16),
            pltpu.HBM((HALF, 256), bf16),
            pltpu.VMEM((1, 128, 256), bf16),
        ],
        in_specs=[SMEM] * 2 + [VMEM] * 7,
        out_specs=[VMEM] * 4,
        scratch_shapes=[
            pltpu.VMEM((2, 128, 768), bf16),
            pltpu.VMEM((720, 256), f32),
            pltpu.VMEM((128, 128), f32),
            pltpu.VMEM((128, 128), f32),
            pltpu.VMEM((ROWS_ALL, 256), bf16),
            pltpu.VMEM((4, 128, 256), bf16),
        ],
        compiler_params=pltpu.CompilerParams(vmem_limit_bytes=LIMIT),
        name="head",
    )(first, ci, *far_memory([outer, inner]), *near_memory([w]), *far_memory([part]), *near_memory(small))


def tower_terms(ci, g, w, after):
    return pl.pallas_call(
        tower_kernel,
        out_shape=(
            pltpu.HBM((2, 128, 256), f32),
            pltpu.VMEM((1, 128, 256), bf16),
            pltpu.VMEM((1, 128, 256), bf16),
            shape(8, 128),
        ),
        in_specs=[SMEM, VMEM, VMEM, ANY],
        out_specs=(VMEM, VMEM, VMEM, VMEM),
        compiler_params=pltpu.CompilerParams(vmem_limit_bytes=LIMIT),
        name="tower_terms",
        cost_estimate=pl.CostEstimate(flops=2 * 756 * 2304 * 256, transcendentals=0, bytes_accessed=4500000),
    )(ci, *far_memory([g]), *near_memory([w]), after)


def tower_end(ci, mid, outer, inner):
    return pl.pallas_call(
        tower_end_kernel,
        out_shape=(shape(1, 2, 128, 256, dtype=bf16), shape(8, 128)),
        in_specs=[SMEM] + [VMEM] * 3,
        out_specs=(VMEM, VMEM),
        compiler_params=pltpu.CompilerParams(vmem_limit_bytes=LIMIT),
        name="tower_end",
    )(ci, *far_memory([mid]), outer, inner)


def weight_terms(yi, xi, ci, keep, got, outer, own, inner, other_edge):
    return pl.pallas_call(
        weight_kernel,
        out_shape=[pltpu.VMEM((4, PIECE, 128), bf16)] * 4 + [shape(8, 128)],
        in_specs=[SMEM] * 3 + [VMEM] * 6,
        out_specs=[VMEM] * 5,
        scratch_shapes=[
            pltpu.VMEM((6, 128, 256), bf16),
            pltpu.VMEM((3, 768, 256), bf16),
            pltpu.VMEM((2, HALF, 256), bf16),
            pltpu.VMEM((16, PIECE, 128), bf16),
        ],
        compiler_params=pltpu.CompilerParams(vmem_limit_bytes=LIMIT),
        name="weight_terms",
    )(yi, xi, ci, *far_memory([keep, got, outer, own, inner]), other_edge)


def row_sum(yi, xi, ci, parts, after):
    return pl.pallas_call(
        row_sum_kernel,
        out_shape=[pltpu.VMEM((PIECE, 128), bf16)] * 4,
        in_specs=[SMEM] * 3 + [VMEM] * 4 + [ANY],
        out_specs=[VMEM] * 4,
        compiler_params=pltpu.CompilerParams(vmem_limit_bytes=LIMIT),
        name="row_sum",
    )(yi, xi, ci, *near_memory(parts), after)


def block_sum(zi, parts):
    return pl.pallas_call(
        block_sum_kernel,
        out_shape=pltpu.VMEM((PIECE, 128), bf16),
        in_specs=[SMEM] + [VMEM] * 4,
        out_specs=VMEM,
        compiler_params=pltpu.CompilerParams(vmem_limit_bytes=LIMIT),
        name="block_sum",
    )(zi, *near_memory(parts))


def piece_sum(zi, m):
    return pl.pallas_call(
        piece_sum_kernel,
        out_shape=pltpu.VMEM((8, 56, 128), bf16),
        in_specs=[SMEM, VMEM],
        out_specs=VMEM,
        compiler_params=pltpu.CompilerParams(vmem_limit_bytes=LIMIT),
        name="piece_sum",
    )(zi, *near_memory([m]))


def join(parts):
    return pl.pallas_call(
        join_kernel,
        out_shape=pltpu.VMEM((4, PIECE, 128), bf16),
        in_specs=[VMEM] * 4,
        out_specs=VMEM,
        compiler_params=pltpu.CompilerParams(vmem_limit_bytes=LIMIT),
        name="join",
    )(*near_memory(parts))


def squares_of(yi, xi, ci, pieces):
    return pl.pallas_call(
        squares_kernel,
        out_shape=pltpu.VMEM((8, 128), f32),
        in_specs=[SMEM] * 3 + [VMEM] * 7,
        out_specs=VMEM,
        compiler_params=pltpu.CompilerParams(vmem_limit_bytes=LIMIT),
        name="squares",
    )(yi, xi, ci, *near_memory(pieces))


def finish(yi, xi, ci, pieces, partial):
    return pl.pallas_call(
        final_kernel,
        out_shape=(shape(720, 2304), shape(36, 2304), shape(720), shape(36), shape(1, 128)),
        in_specs=[SMEM] * 3 + [VMEM] * 9,
        out_specs=(ANY, VMEM, VMEM, VMEM, VMEM),
        scratch_shapes=[
            pltpu.VMEM((ROWS_ALL, 2304), f32),
            pltpu.VMEM((32, 8, 128), f32),
            pltpu.VMEM((8, 896), f32),
            pltpu.SemaphoreType.DMA,
        ],
        compiler_params=pltpu.CompilerParams(vmem_limit_bytes=LIMIT),
        name="finish",
    )(yi, xi, ci, *near_memory([*pieces, partial]))


def swap(value):
    return lax.ppermute(value, "core", [(0, 1), (1, 0)])


def across(value):
    pairs = [(t, t + 1) for t in range(1, 31, 2)]
    return lax.ppermute(value, TILE_AXES, pairs + [(b, a) for a, b in pairs])


def along(value, k, first_axis):
    pairs = []
    for y in range(4):
        for c in range(2):
            for x in range(4):
                dx = k if (first_axis == "x") == (c == 0) else 0
                dy = k - dx
                pairs.append(((y * 2 + c) * 4 + x, (((y + dy) % 4) * 2 + c) * 4 + (x + dx) % 4))
    return lax.ppermute(value, ("y", "core", "x"), pairs)


def per_device(tower, cls_weight, cls_bias, box_weight, box_bias, labels, target_index, boxes):
    own = tower[0]
    outer = across(own)
    inner = swap(own)
    ci = lax.axis_index("core").reshape(1)
    yi = lax.axis_index("y").reshape(1)
    xi = lax.axis_index("x").reshape(1)
    zi = (lax.axis_index("zhi") * 4 + lax.axis_index("zlo")).reshape(1)
    first = (lax.axis_index(TILE_AXES) * 2).reshape(1)

    w, part, *small = stage(
        cls_weight, box_weight, own, cls_bias, box_bias, labels[0], target_index[0], boxes[0]
    )
    g, keep, send, edge = head(first, ci, outer, inner, w, part, *small)
    *parts, token = weight_terms(yi, xi, ci, keep, swap(send), outer, own, inner, swap(edge))

    mid, to_outer, to_inner, _ = tower_terms(ci, g, w, token)
    tower_grad, end_token = tower_end(ci, mid, across(to_outer), swap(to_inner))

    parts = [parts[0]] + [along(parts[k], k, "y") for k in (1, 2, 3)]
    parts = row_sum(yi, xi, ci, parts, end_token)
    parts = [parts[0]] + [along(parts[k], k, "x") for k in (1, 2, 3)]
    terms = lax.all_to_all(block_sum(zi, parts).reshape(8, 56, 128), ("zhi", "zlo"), 0, 0, tiled=True)
    copies = lax.all_to_all(piece_sum(zi, terms), ("zhi", "zlo"), 0, 0, tiled=True)
    block = copies.reshape(PIECE, 128)
    row = join([block] + [along(block, k, "x") for k in (1, 2, 3)])
    mine = [row] + [along(row, k, "y") for k in (1, 2, 3)]
    pieces = mine + [swap(v) for v in mine]
    partial = squares_of(yi, xi, ci, pieces[:LAST] + pieces[LAST + 1 :])
    cw_grad, bw_grad, cb_grad, bb_grad, loss = finish(yi, xi, ci, pieces, partial)
    return loss[0, 0], cw_grad, cb_grad, bw_grad, bb_grad, tower_grad


def solution(mesh):
    fine = Mesh(mesh.devices.reshape(4, 4, 2, 4, 2), ("zlo", "y", "core", "x", "zhi"))
    placed = (
        P(IMG_AXES, TILE_AXES, None, None),
        P(),
        P(),
        P(),
        P(),
        P(IMG_AXES, None, TILE_AXES, None),
        P(IMG_AXES, None, TILE_AXES, None),
        P(IMG_AXES, None, None),
    )
    return jax.shard_map(
        per_device,
        mesh=fine,
        in_specs=placed,
        out_specs=(P(), P(), P(), P(), P(), P(IMG_AXES, TILE_AXES, None, None)),
        check_vma=False,
    )
```

```python
import jax
import jax.numpy as jnp
from jax import lax
from jax.experimental import pallas as pl
from jax.experimental.pallas import tpu as pltpu
from jax.sharding import Mesh, PartitionSpec as P

CLASSES = 80
ANCHORS = 9
STRIDE = 8
FOCAL_ALPHA = 0.25
NORM_EPS = 1e-06

ROWS_ALL = 768
VALID = 756
HALF = 384
GROUP_ROWS = 96
BLOCK = 24
TILES = 56
PIECE = 448

LIMIT = 24 << 20

TILE_AXES = ("zlo", "y", "core")
IMG_AXES = ("x", "zhi")

f32 = jnp.float32
bf16 = jnp.bfloat16


def dot(a, b, dims):
    return lax.dot_general(a, b, (dims, ((), ())), preferred_element_type=f32)


def shifted(x, j):
    if j == 1:
        return x
    ids = lax.broadcasted_iota(jnp.int32, x.shape, 0)
    if j == 0:
        return jnp.where(ids == 0, 0.0, pltpu.roll(x, 1, 0))
    return jnp.where(ids == x.shape[0] - 1, 0.0, pltpu.roll(x, x.shape[0] - 1, 0))


def fill_patches(rows, p_ref, base):
    for e, row in enumerate(rows):
        x = row.astype(f32)
        for j in range(3):
            v = shifted(x, j).astype(bf16)
            for i in range(3):
                r = e - i
                if 0 <= r < 2:
                    p_ref[base + r * 128 : base + r * 128 + 128, (3 * i + j) * 256 : (3 * i + j) * 256 + 256] = v


def anchor_sizes(shape):
    ids = lax.broadcasted_iota(jnp.int32, shape, 0)
    w = jnp.ones(shape, f32)
    h = jnp.ones(shape, f32)
    for a in range(ANCHORS):
        base = 4.0 * STRIDE * 2.0 ** ((a // 3) / 3.0)
        ratio = a % 3 - 1
        w = jnp.where(ids == a, base * 2.0 ** (-ratio / 2.0), w)
        h = jnp.where(ids == a, base * 2.0 ** (ratio / 2.0), h)
    return w, h


def giou_terms(o0, o1, o2, o3, aw, ah, cx, cy, tl, tt, tr, tb):
    mx = cx + o0 * aw
    my = cy + o1 * ah
    pw = aw * jnp.exp(o2)
    ph = ah * jnp.exp(o3)
    left = mx - 0.5 * pw
    right = mx + 0.5 * pw
    top = my - 0.5 * ph
    bottom = my + 0.5 * ph
    iw = jnp.maximum(jnp.minimum(right, tr) - jnp.maximum(left, tl), 0.0)
    ih = jnp.maximum(jnp.minimum(bottom, tb) - jnp.maximum(top, tt), 0.0)
    inter = iw * ih
    union = pw * ph + (tr - tl) * (tb - tt) - inter
    ow = jnp.maximum(right, tr) - jnp.minimum(left, tl)
    oh = jnp.maximum(bottom, tb) - jnp.minimum(top, tt)
    outer = ow * oh
    return 1.0 - (inter / union - (outer - union) / outer)


def stage_kernel(cw, bw, w_ref, sem):
    copy = pltpu.make_async_copy(cw, w_ref.at[pl.ds(0, 720)], sem)
    copy.start()
    w_ref[752:768, :] = jnp.zeros((16, 2304), bf16)
    w_ref[720:756, :] = bw[...]
    copy.wait()


def head_kernel(first, ci, outer, own, inner, w, cb, bb, lab, idx, box, *refs):
    g_out, keep, send, edge = refs[0:4]
    p_ref, o_ref, b_ref, gb_ref, g_ref, row_ref, box_ref, lab_ref, idx_ref, ext_ref = refs[4:]
    c = ci[0]
    edge[0] = outer[1 - c]
    ext_ref[3 * c] = outer[1 - c]
    ext_ref[3 - 3 * c] = inner[c]
    fill_patches([ext_ref[0], own[0], own[1], ext_ref[3]], p_ref, 0)
    row_ref[0, 0:720] = cb[...]
    row_ref[8, 0:36] = bb[...]
    column = row_ref[0:8, :].T[:, 0:1]
    box_column = row_ref[8:16, 0:128].T[:, 0:1]
    box_ref[0:4, 0:100] = box[...]
    lab_ref[...] = jnp.full((32, 128), -2, jnp.int32)
    idx_ref[...] = jnp.zeros((32, 128), jnp.int32)
    for r in range(2):
        for a in range(ANCHORS):
            lab_ref[r * 16 + a : r * 16 + a + 1, :] = lab[a, r : r + 1, :]
            idx_ref[r * 16 + a : r * 16 + a + 1, :] = idx[a, r : r + 1, :]
    p = p_ref[...]
    out = dot(w[...], p, ((1,), (1,)))
    o_ref[...] = out[0:720] + column[0:720]
    small_out = out[720:756] + box_column[0:36]
    for r in range(2):
        b_ref[r * 64 + 32 : r * 64 + 64, :] = jnp.zeros((32, 128), f32)
        b_ref[r * 64 : r * 64 + 36, :] = small_out[:, r * 128 : r * 128 + 128]
    cls = lax.broadcasted_iota(jnp.int32, (CLASSES, 128), 0)

    def one_anchor(a, carry):
        sums = []
        at = pl.multiple_of(a * CLASSES, 16)
        for r in range(2):
            label = lab_ref[pl.ds(r * 16 + a, 1), :]
            x = o_ref[pl.ds(at, CLASSES), r * 128 : r * 128 + 128]
            hit = label == cls
            z = jnp.where(hit, -x, x)
            e = jnp.exp(-jnp.abs(z))
            soft = jnp.maximum(z, 0.0) + jnp.log1p(e)
            big = 1.0 / (1.0 + e)
            small = e * big
            up = z >= 0.0
            q = jnp.where(up, big, small)
            rest = jnp.where(up, small, big)
            counted = (label >= -1).astype(f32)
            w = jnp.where(hit, FOCAL_ALPHA, 1.0 - FOCAL_ALPHA) * counted
            wq = w * q * q
            dz = wq * (q + 2.0 * rest * soft)
            g_ref[pl.ds(at, CLASSES), r * 128 : r * 128 + 128] = jnp.where(hit, -dz, dz).astype(bf16)
            sums.append(carry[r] + jnp.sum(wq * soft, axis=0, keepdims=True))
        return tuple(sums)

    zero = jnp.zeros((1, 128), f32)
    focal = lax.fori_loop(0, ANCHORS, one_anchor, (zero, zero))

    aw, ah = anchor_sizes((16, 128))
    cx = (lax.broadcasted_iota(jnp.int32, (16, 128), 1).astype(f32) + 0.5) * STRIDE
    for r in range(2):
        cy = (jnp.full((16, 128), first[0] + r, jnp.int32).astype(f32) + 0.5) * STRIDE
        which = idx_ref[r * 16 : r * 16 + 16, :]
        corner = [
            jnp.take_along_axis(jnp.broadcast_to(box_ref[k : k + 1, :], (16, 128)), which, axis=1) for k in range(4)
        ]
        positive = lab_ref[r * 16 : r * 16 + 16, :] >= 0
        o = [b_ref[pl.ds(r * 64 + k, 16, stride=4), :] for k in range(4)]
        value, pull = jax.vjp(
            lambda o0, o1, o2, o3: giou_terms(o0, o1, o2, o3, aw, ah, cx, cy, *corner), *o
        )
        grads = pull(jnp.ones((16, 128), f32))
        for k in range(4):
            gb_ref[pl.ds(r * 64 + k, 16, stride=4), :] = jnp.where(positive, grads[k], 0.0)
        giou = jnp.sum(jnp.where(positive, value, 0.0), axis=0, keepdims=True)
        count = jnp.sum(positive.astype(f32), axis=0, keepdims=True)
        rows = []
        for v in (focal[r], giou):
            hi = v.astype(bf16).astype(f32)
            rows += [hi, v - hi]
        rows.append(count)
        for n, v in enumerate(rows):
            gb_ref[r * 64 + 36 + n : r * 64 + 37 + n, :] = v
        g_ref[720:768, r * 128 : r * 128 + 128] = gb_ref[r * 64 : r * 64 + 48, :].astype(bf16)
    g_out[...] = g_ref[...]
    keep[...] = g_ref[pl.ds(pl.multiple_of(ci[0] * HALF, 16), HALF), :]
    send[...] = g_ref[pl.ds(pl.multiple_of((1 - ci[0]) * HALF, 16), HALF), :]


def tower_kernel(ci, g, w_ref, unused, mid, outer, inner, token):
    token[...] = jnp.zeros((8, 128), f32)
    gt = g[...].astype(f32).T
    gj = []
    for j in range(3):
        gj.append(
            jnp.concatenate([shifted(gt[r * 128 : r * 128 + 128], 2 - j) for r in range(2)], axis=0).astype(bf16)
        )
    t = []
    for i in range(3):
        acc = jnp.zeros((256, 256), f32)
        for j in range(3):
            at = (3 * i + j) * 256
            acc = acc + dot(gj[j], w_ref[:, at : at + 256], ((1,), (0,)))
        t.append(acc)
    low = jnp.full((128, 256), ci[0], jnp.int32) == 0
    up = t[0][0:128]
    down = t[2][128:256]
    outer[0] = jnp.where(low, up, down).astype(bf16)
    inner[0] = jnp.where(low, down, up).astype(bf16)
    mid[0] = t[1][0:128] + t[0][128:256]
    mid[1] = t[1][128:256] + t[2][0:128]


def tower_end_kernel(ci, mid, outer, inner, t_ref, token):
    token[...] = jnp.zeros((8, 128), f32)
    c = ci[0]
    t_ref[0, c] = (mid[c] + outer[0].astype(f32)).astype(bf16)
    t_ref[0, 1 - c] = (mid[1 - c] + inner[0].astype(f32)).astype(bf16)


def weight_kernel(yi, xi, ci, keep, got, outer, own, inner, other_edge, *refs):
    outs = refs[0:4]
    token, t_ref, s_ref, g_ref, m_ref = refs[4:]
    token[...] = jnp.zeros((8, 128), f32)
    c = ci[0]
    t_ref[5 * c] = outer[1 - c]
    t_ref[5 - 5 * c] = other_edge[0]
    for r in range(2):
        t_ref[1 + 2 * c + r] = own[r]
        t_ref[3 - 2 * c + r] = inner[r]
    g_ref[c] = keep[...]
    g_ref[1 - c] = got[...]

    def shift(row, carry):
        x = t_ref[row].astype(f32)
        at = pl.multiple_of(row * 128, 128)
        for j in range(3):
            s_ref[j, pl.ds(at, 128), :] = shifted(x, j).astype(bf16)
        return carry

    lax.fori_loop(0, 6, shift, 0)
    lhs = jnp.concatenate([g_ref[0], g_ref[1]], axis=1)
    for tap in range(9):
        i, j = divmod(tap, 3)
        acc = dot(lhs, s_ref[j, i * 128 : i * 128 + 512, :], ((1,), (0,)))
        for m in range(16):
            for rb in range(3):
                row = m * BLOCK + rb * 8
                both = jnp.concatenate([acc[row : row + 8, 0:128], acc[row : row + 8, 128:256]], axis=0)
                v = (rb * 18 + 2 * tap) * 8
                m_ref[m, v : v + 16, :] = both.astype(bf16)
    bias = dot(jnp.ones((8, 512), bf16), lhs, ((1,), (1,)))
    for m in range(16):
        tile, off = divmod(m * BLOCK, 128)
        e = bias[:, tile * 128 : tile * 128 + 128]
        e = e if off == 0 else pltpu.roll(e, 128 - off, 1)
        if off + BLOCK > 128:
            past = pltpu.roll(bias[:, tile * 128 + 128 : tile * 128 + 256], 128 - off, 1)
            lane = lax.broadcasted_iota(jnp.int32, (8, 128), 1)
            e = jnp.where(lane < 128 - off, e, past)
        hi = e.astype(bf16).astype(f32)
        m_ref[m, 432:448, :] = jnp.concatenate([hi, e - hi], axis=0).astype(bf16)
    for k in range(4):
        for q in range(4):
            outs[k][q] = m_ref[jnp.where(c == 0, ((yi[0] + k) & 3) * 4 + q, q * 4 + ((xi[0] + k) & 3))]


def row_sum_kernel(yi, xi, ci, *refs):
    parts = refs[0:4]
    outs = refs[5:9]
    here = jnp.where(ci[0] == 0, xi[0], yi[0])
    for k in range(4):
        q = (here + k) & 3
        acc = parts[0][q].astype(f32)
        for n in range(1, 4):
            acc = acc + parts[n][q].astype(f32)
        e = acc[432:440] + acc[440:448]
        hi = e.astype(bf16).astype(f32)
        outs[k][0:432, :] = acc[0:432].astype(bf16)
        outs[k][432:448, :] = jnp.concatenate([hi, e - hi], axis=0).astype(bf16)


def block_sum_kernel(zi, a, b, c, d, s_ref):
    acc = (a[...].astype(f32) + b[...].astype(f32)) + (c[...].astype(f32) + d[...].astype(f32))
    e = acc[432:440] + acc[440:448]
    hi = e.astype(bf16).astype(f32)
    s_ref[0:432, :] = acc[0:432].astype(bf16)
    s_ref[432:448, :] = jnp.concatenate([hi, e - hi], axis=0).astype(bf16)


def piece_sum_kernel(zi, m_ref, c_ref):
    acc = m_ref[0].astype(f32)
    for m in range(1, 8):
        acc = acc + m_ref[m].astype(f32)
    last = jnp.full((8, 128), zi[0], jnp.int32) == 7
    e = acc[40:48] + acc[48:56]
    hi = e.astype(bf16).astype(f32)
    out = jnp.concatenate(
        [acc[0:40], jnp.where(last, hi, acc[40:48]), jnp.where(last, e - hi, acc[48:56])], axis=0
    ).astype(bf16)
    for z in range(8):
        c_ref[z] = out


def join_kernel(a, d, b, c, o_ref):
    for k, ref in enumerate((a, b, c, d)):
        o_ref[k] = ref[...]


LAST = 7


def block_of(yi, xi, ci, n, k):
    c = ci[0] if n < 4 else 1 - ci[0]
    far = n % 4
    y = (yi[0] - jnp.where(c == 0, far, k)) & 3
    x = (xi[0] - jnp.where(c == 0, k, far)) & 3
    return c * 16 + y * 4 + x


def squares(yi, xi, ci, n, src):
    srow = lax.broadcasted_iota(jnp.int32, (8, 128), 0)
    lane = lax.broadcasted_iota(jnp.int32, (8, 128), 1)

    def one(k, total):
        base = block_of(yi, xi, ci, n, k) * BLOCK
        for rb in range(3):
            acc = jnp.zeros((16, 128), f32)
            for t in range(9):
                v = src[k, (rb * 9 + t) * 16 : (rb * 9 + t) * 16 + 16, :].astype(f32)
                acc = acc + v * v
            ok = base + rb * 8 + srow < VALID
            total = total + jnp.where(ok, acc[0:8] + acc[8:16], 0.0)
        e = src[k, 432:448, :].astype(f32)
        e = e[0:8] + e[8:16]
        ok = (base + lane < VALID) & (lane < BLOCK) & (srow == 0)
        return total + jnp.where(ok, e * e, 0.0)

    return one


def squares_kernel(yi, xi, ci, *refs):
    total = jnp.zeros((8, 128), f32)
    for n, src in zip([n for n in range(8) if n != LAST], refs[:7]):
        total = lax.fori_loop(0, 4, squares(yi, xi, ci, n, src), total)
    refs[7][...] = total


def final_kernel(yi, xi, ci, *refs):
    sources = refs[0:8]
    partial, cw_out, bw_out, cb_out, bb_out, loss, w_ref, e_ref, row_ref, sem = refs[8:]
    srow = lax.broadcasted_iota(jnp.int32, (8, 128), 0)
    lane = lax.broadcasted_iota(jnp.int32, (8, 128), 1)
    total = lax.fori_loop(0, 4, squares(yi, xi, ci, LAST, sources[LAST]), partial[...])
    mean = jnp.sum(total) * (1.0 / (VALID * 2305))
    scale = lax.rsqrt(jnp.full((8, 128), mean + NORM_EPS, f32))

    def chunk(block):
        rows = pl.ds(pl.multiple_of(block * BLOCK, 8), BLOCK)
        return pltpu.make_async_copy(w_ref.at[rows], cw_out.at[rows], sem)

    def write(n):
        src = sources[n]

        def one(k, carry):
            block = block_of(yi, xi, ci, n, k)
            e = src[k, 432:448, :].astype(f32)
            e_ref[block] = e[0:8] + e[8:16]
            for rb in range(3):
                row = pl.multiple_of(block * BLOCK + rb * 8, 8)
                for t in range(9):
                    v = src[k, (rb * 9 + t) * 16 : (rb * 9 + t) * 16 + 16, :].astype(f32)
                    w_ref[pl.ds(row, 8), t * 256 : t * 256 + 128] = v[0:8] * scale
                    w_ref[pl.ds(row, 8), t * 256 + 128 : t * 256 + 256] = v[8:16] * scale

            @pl.when(block < 30)
            def _():
                chunk(block).start()

            return carry

        return one

    for n in range(8):
        lax.fori_loop(0, 4, write(n), 0)
    bw_out[...] = w_ref[720:756, :]
    row_ref[...] = jnp.zeros((8, 896), f32)
    for block in range(32):
        tile, off = divmod(block * BLOCK, 128)
        e = e_ref[block] * scale
        e = e if off == 0 else pltpu.roll(e, off, 1)
        here = (lane >= off) & (lane < off + BLOCK)
        row_ref[:, tile * 128 : tile * 128 + 128] = jnp.where(here, e, row_ref[:, tile * 128 : tile * 128 + 128])
        if off + BLOCK > 128:
            past = lane < off + BLOCK - 128
            row_ref[:, tile * 128 + 128 : tile * 128 + 256] = jnp.where(past, e, 0.0)
    cb_out[...] = row_ref[0, 0:720]
    bb_out[...] = pltpu.roll(row_ref[:, 640:768], 128 - 80, 1)[0, 0:36]
    e = jnp.where(srow == 0, e_ref[31], 0.0)
    sums = jnp.sum(jnp.where((lane >= 12) & (lane < 16), e, 0.0))
    count = jnp.sum(jnp.where(lane == 16, e, 0.0))
    loss[...] = jnp.full((1, 128), sums, f32) / jnp.full((1, 128), count, f32)

    def drain(k, carry):
        chunk(k).wait()
        return carry

    lax.fori_loop(0, 30, drain, 0)


VMEM = pl.BlockSpec(memory_space=pltpu.VMEM)
SMEM = pl.BlockSpec(memory_space=pltpu.SMEM)
ANY = pl.BlockSpec(memory_space=pl.ANY)


def near_memory(arrays):
    return [pltpu.with_memory_space_constraint(v, pltpu.VMEM) for v in arrays]


def far_memory(arrays):
    return [pltpu.with_memory_space_constraint(v, pltpu.HBM) for v in arrays]


def shape(*dims, dtype=f32):
    return jax.ShapeDtypeStruct(dims, dtype)


def stage(cw, bw):
    return pl.pallas_call(
        stage_kernel,
        out_shape=pltpu.VMEM((ROWS_ALL, 2304), bf16),
        in_specs=[ANY, VMEM],
        out_specs=VMEM,
        scratch_shapes=[pltpu.SemaphoreType.DMA],
        compiler_params=pltpu.CompilerParams(vmem_limit_bytes=LIMIT),
        name="stage",
    )(*far_memory([cw, bw]))


def head(first, ci, outer, own, inner, w, cb, bb, lab, idx, box):
    return pl.pallas_call(
        head_kernel,
        out_shape=[
            pltpu.HBM((ROWS_ALL, 256), bf16),
            pltpu.HBM((HALF, 256), bf16),
            pltpu.HBM((HALF, 256), bf16),
            pltpu.VMEM((1, 128, 256), bf16),
        ],
        in_specs=[SMEM] * 2 + [VMEM] * 9,
        out_specs=[VMEM] * 4,
        scratch_shapes=[
            pltpu.VMEM((256, 2304), bf16),
            pltpu.VMEM((720, 256), f32),
            pltpu.VMEM((128, 128), f32),
            pltpu.VMEM((128, 128), f32),
            pltpu.VMEM((ROWS_ALL, 256), bf16),
            pltpu.VMEM((16, 768), f32),
            pltpu.VMEM((8, 128), f32),
            pltpu.VMEM((32, 128), jnp.int32),
            pltpu.VMEM((32, 128), jnp.int32),
            pltpu.VMEM((4, 128, 256), bf16),
        ],
        compiler_params=pltpu.CompilerParams(vmem_limit_bytes=LIMIT),
        name="head",
    )(first, ci, *far_memory([outer, own, inner]), *near_memory([w]), *far_memory([cb, bb, lab, idx, box]))


def tower_terms(ci, g, w, after):
    return pl.pallas_call(
        tower_kernel,
        out_shape=(
            pltpu.HBM((2, 128, 256), f32),
            pltpu.VMEM((1, 128, 256), bf16),
            pltpu.VMEM((1, 128, 256), bf16),
            shape(8, 128),
        ),
        in_specs=[SMEM, VMEM, VMEM, ANY],
        out_specs=(VMEM, VMEM, VMEM, VMEM),
        compiler_params=pltpu.CompilerParams(vmem_limit_bytes=LIMIT),
        name="tower_terms",
        cost_estimate=pl.CostEstimate(flops=2 * 756 * 2304 * 256, transcendentals=0, bytes_accessed=4500000),
    )(ci, *far_memory([g]), *near_memory([w]), after)


def tower_end(ci, mid, outer, inner):
    return pl.pallas_call(
        tower_end_kernel,
        out_shape=(shape(1, 2, 128, 256, dtype=bf16), shape(8, 128)),
        in_specs=[SMEM] + [VMEM] * 3,
        out_specs=(VMEM, VMEM),
        compiler_params=pltpu.CompilerParams(vmem_limit_bytes=LIMIT),
        name="tower_end",
    )(ci, *far_memory([mid]), outer, inner)


def weight_terms(yi, xi, ci, keep, got, outer, own, inner, other_edge):
    return pl.pallas_call(
        weight_kernel,
        out_shape=[pltpu.VMEM((4, PIECE, 128), bf16)] * 4 + [shape(8, 128)],
        in_specs=[SMEM] * 3 + [VMEM] * 6,
        out_specs=[VMEM] * 5,
        scratch_shapes=[
            pltpu.VMEM((6, 128, 256), bf16),
            pltpu.VMEM((3, 768, 256), bf16),
            pltpu.VMEM((2, HALF, 256), bf16),
            pltpu.VMEM((16, PIECE, 128), bf16),
        ],
        compiler_params=pltpu.CompilerParams(vmem_limit_bytes=LIMIT),
        name="weight_terms",
    )(yi, xi, ci, *far_memory([keep, got, outer, own, inner]), other_edge)


def row_sum(yi, xi, ci, parts, after):
    return pl.pallas_call(
        row_sum_kernel,
        out_shape=[pltpu.VMEM((PIECE, 128), bf16)] * 4,
        in_specs=[SMEM] * 3 + [VMEM] * 4 + [ANY],
        out_specs=[VMEM] * 4,
        compiler_params=pltpu.CompilerParams(vmem_limit_bytes=LIMIT),
        name="row_sum",
    )(yi, xi, ci, *near_memory(parts), after)


def block_sum(zi, parts):
    return pl.pallas_call(
        block_sum_kernel,
        out_shape=pltpu.VMEM((PIECE, 128), bf16),
        in_specs=[SMEM] + [VMEM] * 4,
        out_specs=VMEM,
        compiler_params=pltpu.CompilerParams(vmem_limit_bytes=LIMIT),
        name="block_sum",
    )(zi, *near_memory(parts))


def piece_sum(zi, m):
    return pl.pallas_call(
        piece_sum_kernel,
        out_shape=pltpu.VMEM((8, 56, 128), bf16),
        in_specs=[SMEM, VMEM],
        out_specs=VMEM,
        compiler_params=pltpu.CompilerParams(vmem_limit_bytes=LIMIT),
        name="piece_sum",
    )(zi, *near_memory([m]))


def join(parts):
    return pl.pallas_call(
        join_kernel,
        out_shape=pltpu.VMEM((4, PIECE, 128), bf16),
        in_specs=[VMEM] * 4,
        out_specs=VMEM,
        compiler_params=pltpu.CompilerParams(vmem_limit_bytes=LIMIT),
        name="join",
    )(*near_memory(parts))


def squares_of(yi, xi, ci, pieces):
    return pl.pallas_call(
        squares_kernel,
        out_shape=pltpu.VMEM((8, 128), f32),
        in_specs=[SMEM] * 3 + [VMEM] * 7,
        out_specs=VMEM,
        compiler_params=pltpu.CompilerParams(vmem_limit_bytes=LIMIT),
        name="squares",
    )(yi, xi, ci, *near_memory(pieces))


def finish(yi, xi, ci, pieces, partial):
    return pl.pallas_call(
        final_kernel,
        out_shape=(shape(720, 2304), shape(36, 2304), shape(720), shape(36), shape(1, 128)),
        in_specs=[SMEM] * 3 + [VMEM] * 9,
        out_specs=(ANY, VMEM, VMEM, VMEM, VMEM),
        scratch_shapes=[
            pltpu.VMEM((ROWS_ALL, 2304), f32),
            pltpu.VMEM((32, 8, 128), f32),
            pltpu.VMEM((8, 896), f32),
            pltpu.SemaphoreType.DMA,
        ],
        compiler_params=pltpu.CompilerParams(vmem_limit_bytes=LIMIT),
        name="finish",
    )(yi, xi, ci, *near_memory([*pieces, partial]))


def swap(value):
    return lax.ppermute(value, "core", [(0, 1), (1, 0)])


def across(value):
    pairs = [(t, t + 1) for t in range(1, 31, 2)]
    return lax.ppermute(value, TILE_AXES, pairs + [(b, a) for a, b in pairs])


def along(value, k, first_axis):
    pairs = []
    for y in range(4):
        for c in range(2):
            for x in range(4):
                dx = k if (first_axis == "x") == (c == 0) else 0
                dy = k - dx
                pairs.append(((y * 2 + c) * 4 + x, (((y + dy) % 4) * 2 + c) * 4 + (x + dx) % 4))
    return lax.ppermute(value, ("y", "core", "x"), pairs)


def per_device(tower, cls_weight, cls_bias, box_weight, box_bias, labels, target_index, boxes):
    own = tower[0]
    outer = across(own)
    inner = swap(own)
    ci = lax.axis_index("core").reshape(1)
    yi = lax.axis_index("y").reshape(1)
    xi = lax.axis_index("x").reshape(1)
    zi = (lax.axis_index("zhi") * 4 + lax.axis_index("zlo")).reshape(1)
    first = (lax.axis_index(TILE_AXES) * 2).reshape(1)

    w = stage(cls_weight, box_weight)
    g, keep, send, edge = head(
        first, ci, outer, own, inner, w, cls_bias, box_bias, labels[0], target_index[0], boxes[0]
    )
    *parts, token = weight_terms(yi, xi, ci, keep, swap(send), outer, own, inner, swap(edge))

    mid, to_outer, to_inner, _ = tower_terms(ci, g, w, token)
    tower_grad, end_token = tower_end(ci, mid, across(to_outer), swap(to_inner))

    got = {k: along(parts[k], k, "y") for k in (2, 1, 3)}
    parts = [parts[0]] + [got[k] for k in (2, 1, 3)]
    parts = row_sum(yi, xi, ci, parts, end_token)
    got = {k: along(parts[k], k, "x") for k in (2, 1, 3)}
    parts = [parts[0]] + [got[k] for k in (2, 1, 3)]
    terms = lax.all_to_all(block_sum(zi, parts).reshape(8, 56, 128), ("zhi", "zlo"), 0, 0, tiled=True)
    copies = lax.all_to_all(piece_sum(zi, terms), ("zhi", "zlo"), 0, 0, tiled=True)
    block = copies.reshape(PIECE, 128)
    got = {k: along(block, k, "x") for k in (3, 1, 2)}
    row = join([block] + [got[k] for k in (3, 1, 2)])
    got = {k: along(row, k, "y") for k in (3, 1, 2)}
    mine = [row] + [got[k] for k in (1, 2, 3)]
    pieces = mine + [swap(v) for v in mine]
    partial = squares_of(yi, xi, ci, pieces[:LAST] + pieces[LAST + 1 :])
    cw_grad, bw_grad, cb_grad, bb_grad, loss = finish(yi, xi, ci, pieces, partial)
    return loss[0, 0], cw_grad, cb_grad, bw_grad, bb_grad, tower_grad


def solution(mesh):
    fine = Mesh(mesh.devices.reshape(4, 4, 2, 4, 2), ("zlo", "y", "core", "x", "zhi"))
    placed = (
        P(IMG_AXES, TILE_AXES, None, None),
        P(),
        P(),
        P(),
        P(),
        P(IMG_AXES, None, TILE_AXES, None),
        P(IMG_AXES, None, TILE_AXES, None),
        P(IMG_AXES, None, None),
    )
    return jax.shard_map(
        per_device,
        mesh=fine,
        in_specs=placed,
        out_specs=(P(), P(), P(), P(), P(), P(IMG_AXES, TILE_AXES, None, None)),
        check_vma=False,
    )
```

```python
import jax
import jax.numpy as jnp
from jax import lax
from jax.experimental import pallas as pl
from jax.experimental.pallas import tpu as pltpu
from jax.sharding import Mesh, PartitionSpec as P

CLASSES = 80
ANCHORS = 9
STRIDE = 8
FOCAL_ALPHA = 0.25
NORM_EPS = 1e-06

ROWS_ALL = 768
VALID = 756
HALF = 384
GROUP_ROWS = 96
BLOCK = 24
TILES = 56
PIECE = 448

LIMIT = 24 << 20

TILE_AXES = ("zlo", "y", "core")
IMG_AXES = ("x", "zhi")

f32 = jnp.float32
bf16 = jnp.bfloat16


def dot(a, b, dims):
    return lax.dot_general(a, b, (dims, ((), ())), preferred_element_type=f32)


def shifted(x, j):
    if j == 1:
        return x
    ids = lax.broadcasted_iota(jnp.int32, x.shape, 0)
    if j == 0:
        return jnp.where(ids == 0, 0.0, pltpu.roll(x, 1, 0))
    return jnp.where(ids == x.shape[0] - 1, 0.0, pltpu.roll(x, x.shape[0] - 1, 0))


def fill_patches(rows, p_ref, base):
    for e, row in enumerate(rows):
        x = row.astype(f32)
        for j in range(3):
            v = shifted(x, j).astype(bf16)
            for i in range(3):
                r = e - i
                if 0 <= r < 2:
                    p_ref[base + r * 128 : base + r * 128 + 128, (3 * i + j) * 256 : (3 * i + j) * 256 + 256] = v


def anchor_sizes(shape):
    ids = lax.broadcasted_iota(jnp.int32, shape, 0)
    w = jnp.ones(shape, f32)
    h = jnp.ones(shape, f32)
    for a in range(ANCHORS):
        base = 4.0 * STRIDE * 2.0 ** ((a // 3) / 3.0)
        ratio = a % 3 - 1
        w = jnp.where(ids == a, base * 2.0 ** (-ratio / 2.0), w)
        h = jnp.where(ids == a, base * 2.0 ** (ratio / 2.0), h)
    return w, h


def giou_terms(o0, o1, o2, o3, aw, ah, cx, cy, tl, tt, tr, tb):
    mx = cx + o0 * aw
    my = cy + o1 * ah
    pw = aw * jnp.exp(o2)
    ph = ah * jnp.exp(o3)
    left = mx - 0.5 * pw
    right = mx + 0.5 * pw
    top = my - 0.5 * ph
    bottom = my + 0.5 * ph
    iw = jnp.maximum(jnp.minimum(right, tr) - jnp.maximum(left, tl), 0.0)
    ih = jnp.maximum(jnp.minimum(bottom, tb) - jnp.maximum(top, tt), 0.0)
    inter = iw * ih
    union = pw * ph + (tr - tl) * (tb - tt) - inter
    ow = jnp.maximum(right, tr) - jnp.minimum(left, tl)
    oh = jnp.maximum(bottom, tb) - jnp.minimum(top, tt)
    outer = ow * oh
    return 1.0 - (inter / union - (outer - union) / outer)


def stage_kernel(cw, bw, w_ref, sem):
    copy = pltpu.make_async_copy(cw, w_ref.at[pl.ds(0, 720)], sem)
    copy.start()
    w_ref[752:768, :] = jnp.zeros((16, 2304), bf16)
    w_ref[720:756, :] = bw[...]
    copy.wait()


def head_kernel(first, ci, outer, own, inner, w, cb, bb, lab, idx, box, *refs):
    g_out, keep, send, edge = refs[0:4]
    p_ref, o_ref, b_ref, gb_ref, g_ref, row_ref, box_ref, lab_ref, idx_ref, ext_ref = refs[4:]
    c = ci[0]
    edge[0] = outer[1 - c]
    ext_ref[3 * c] = outer[1 - c]
    ext_ref[3 - 3 * c] = inner[c]
    fill_patches([ext_ref[0], own[0], own[1], ext_ref[3]], p_ref, 0)
    row_ref[0, 0:720] = cb[...]
    row_ref[8, 0:36] = bb[...]
    column = row_ref[0:8, :].T[:, 0:1]
    box_column = row_ref[8:16, 0:128].T[:, 0:1]
    box_ref[0:4, 0:100] = box[...]
    lab_ref[...] = jnp.full((32, 128), -2, jnp.int32)
    idx_ref[...] = jnp.zeros((32, 128), jnp.int32)
    for r in range(2):
        for a in range(ANCHORS):
            lab_ref[r * 16 + a : r * 16 + a + 1, :] = lab[a, r : r + 1, :]
            idx_ref[r * 16 + a : r * 16 + a + 1, :] = idx[a, r : r + 1, :]
    p = p_ref[...]
    out = dot(w[...], p, ((1,), (1,)))
    o_ref[...] = out[0:720] + column[0:720]
    small_out = out[720:756] + box_column[0:36]
    for r in range(2):
        b_ref[r * 64 + 32 : r * 64 + 64, :] = jnp.zeros((32, 128), f32)
        b_ref[r * 64 : r * 64 + 36, :] = small_out[:, r * 128 : r * 128 + 128]
    cls = lax.broadcasted_iota(jnp.int32, (CLASSES, 128), 0)

    def one_anchor(a, carry):
        sums = []
        at = pl.multiple_of(a * CLASSES, 16)
        for r in range(2):
            label = lab_ref[pl.ds(r * 16 + a, 1), :]
            x = o_ref[pl.ds(at, CLASSES), r * 128 : r * 128 + 128]
            hit = label == cls
            z = jnp.where(hit, -x, x)
            e = jnp.exp(-jnp.abs(z))
            soft = jnp.maximum(z, 0.0) + jnp.log1p(e)
            big = 1.0 / (1.0 + e)
            small = e * big
            up = z >= 0.0
            q = jnp.where(up, big, small)
            rest = jnp.where(up, small, big)
            counted = (label >= -1).astype(f32)
            w = jnp.where(hit, FOCAL_ALPHA, 1.0 - FOCAL_ALPHA) * counted
            wq = w * q * q
            dz = wq * (q + 2.0 * rest * soft)
            g_ref[pl.ds(at, CLASSES), r * 128 : r * 128 + 128] = jnp.where(hit, -dz, dz).astype(bf16)
            sums.append(carry[r] + jnp.sum(wq * soft, axis=0, keepdims=True))
        return tuple(sums)

    zero = jnp.zeros((1, 128), f32)
    focal = lax.fori_loop(0, ANCHORS, one_anchor, (zero, zero))

    aw, ah = anchor_sizes((16, 128))
    cx = (lax.broadcasted_iota(jnp.int32, (16, 128), 1).astype(f32) + 0.5) * STRIDE
    for r in range(2):
        cy = (jnp.full((16, 128), first[0] + r, jnp.int32).astype(f32) + 0.5) * STRIDE
        which = idx_ref[r * 16 : r * 16 + 16, :]
        corner = [
            jnp.take_along_axis(jnp.broadcast_to(box_ref[k : k + 1, :], (16, 128)), which, axis=1) for k in range(4)
        ]
        positive = lab_ref[r * 16 : r * 16 + 16, :] >= 0
        o = [b_ref[pl.ds(r * 64 + k, 16, stride=4), :] for k in range(4)]
        value, pull = jax.vjp(
            lambda o0, o1, o2, o3: giou_terms(o0, o1, o2, o3, aw, ah, cx, cy, *corner), *o
        )
        grads = pull(jnp.ones((16, 128), f32))
        for k in range(4):
            gb_ref[pl.ds(r * 64 + k, 16, stride=4), :] = jnp.where(positive, grads[k], 0.0)
        giou = jnp.sum(jnp.where(positive, value, 0.0), axis=0, keepdims=True)
        count = jnp.sum(positive.astype(f32), axis=0, keepdims=True)
        rows = []
        for v in (focal[r], giou):
            hi = v.astype(bf16).astype(f32)
            rows += [hi, v - hi]
        rows.append(count)
        for n, v in enumerate(rows):
            gb_ref[r * 64 + 36 + n : r * 64 + 37 + n, :] = v
        g_ref[720:768, r * 128 : r * 128 + 128] = gb_ref[r * 64 : r * 64 + 48, :].astype(bf16)
    g_out[...] = g_ref[...]
    keep[...] = g_ref[pl.ds(pl.multiple_of(ci[0] * HALF, 16), HALF), :]
    send[...] = g_ref[pl.ds(pl.multiple_of((1 - ci[0]) * HALF, 16), HALF), :]


def tower_kernel(ci, g, w_ref, unused, mid, outer, inner, token):
    token[...] = jnp.zeros((8, 128), f32)
    gt = g[...].astype(f32).T
    gj = []
    for j in range(3):
        gj.append(
            jnp.concatenate([shifted(gt[r * 128 : r * 128 + 128], 2 - j) for r in range(2)], axis=0).astype(bf16)
        )
    t = []
    for i in range(3):
        acc = jnp.zeros((256, 256), f32)
        for j in range(3):
            at = (3 * i + j) * 256
            acc = acc + dot(gj[j], w_ref[:, at : at + 256], ((1,), (0,)))
        t.append(acc)
    low = jnp.full((128, 256), ci[0], jnp.int32) == 0
    up = t[0][0:128]
    down = t[2][128:256]
    outer[0] = jnp.where(low, up, down).astype(bf16)
    inner[0] = jnp.where(low, down, up).astype(bf16)
    mid[0] = t[1][0:128] + t[0][128:256]
    mid[1] = t[1][128:256] + t[2][0:128]


def tower_end_kernel(ci, mid, outer, inner, t_ref, token):
    token[...] = jnp.zeros((8, 128), f32)
    c = ci[0]
    t_ref[0, c] = (mid[c] + outer[0].astype(f32)).astype(bf16)
    t_ref[0, 1 - c] = (mid[1 - c] + inner[0].astype(f32)).astype(bf16)


def weight_kernel(yi, xi, ci, keep, got, outer, own, inner, other_edge, *refs):
    outs = refs[0:4]
    token, t_ref, s_ref, g_ref, m_ref = refs[4:]
    token[...] = jnp.zeros((8, 128), f32)
    c = ci[0]
    t_ref[5 * c] = outer[1 - c]
    t_ref[5 - 5 * c] = other_edge[0]
    for r in range(2):
        t_ref[1 + 2 * c + r] = own[r]
        t_ref[3 - 2 * c + r] = inner[r]
    g_ref[c] = keep[...]
    g_ref[1 - c] = got[...]

    def shift(row, carry):
        x = t_ref[row].astype(f32)
        at = pl.multiple_of(row * 128, 128)
        for j in range(3):
            s_ref[j, pl.ds(at, 128), :] = shifted(x, j).astype(bf16)
        return carry

    lax.fori_loop(0, 6, shift, 0)
    lhs = jnp.concatenate([g_ref[0], g_ref[1]], axis=1)
    for tap in range(9):
        i, j = divmod(tap, 3)
        acc = dot(lhs, s_ref[j, i * 128 : i * 128 + 512, :], ((1,), (0,)))
        for m in range(16):
            for rb in range(3):
                row = m * BLOCK + rb * 8
                both = jnp.concatenate([acc[row : row + 8, 0:128], acc[row : row + 8, 128:256]], axis=0)
                v = (rb * 18 + 2 * tap) * 8
                m_ref[m, v : v + 16, :] = both.astype(bf16)
    bias = dot(jnp.ones((8, 512), bf16), lhs, ((1,), (1,)))
    for m in range(16):
        tile, off = divmod(m * BLOCK, 128)
        e = bias[:, tile * 128 : tile * 128 + 128]
        e = e if off == 0 else pltpu.roll(e, 128 - off, 1)
        if off + BLOCK > 128:
            past = pltpu.roll(bias[:, tile * 128 + 128 : tile * 128 + 256], 128 - off, 1)
            lane = lax.broadcasted_iota(jnp.int32, (8, 128), 1)
            e = jnp.where(lane < 128 - off, e, past)
        hi = e.astype(bf16).astype(f32)
        m_ref[m, 432:448, :] = jnp.concatenate([hi, e - hi], axis=0).astype(bf16)
    for k in range(4):
        for q in range(4):
            outs[k][q] = m_ref[jnp.where(c == 1, ((yi[0] + k) & 3) * 4 + q, q * 4 + ((xi[0] + k) & 3))]


def row_sum_kernel(yi, xi, ci, *refs):
    parts = refs[0:4]
    outs = refs[5:9]
    here = jnp.where(ci[0] == 1, xi[0], yi[0])
    for k in range(4):
        q = (here + k) & 3
        acc = parts[0][q].astype(f32)
        for n in range(1, 4):
            acc = acc + parts[n][q].astype(f32)
        e = acc[432:440] + acc[440:448]
        hi = e.astype(bf16).astype(f32)
        outs[k][0:432, :] = acc[0:432].astype(bf16)
        outs[k][432:448, :] = jnp.concatenate([hi, e - hi], axis=0).astype(bf16)


def block_sum_kernel(zi, a, b, c, d, s_ref):
    acc = (a[...].astype(f32) + b[...].astype(f32)) + (c[...].astype(f32) + d[...].astype(f32))
    e = acc[432:440] + acc[440:448]
    hi = e.astype(bf16).astype(f32)
    s_ref[0:432, :] = acc[0:432].astype(bf16)
    s_ref[432:448, :] = jnp.concatenate([hi, e - hi], axis=0).astype(bf16)


def piece_sum_kernel(zi, m_ref, c_ref):
    acc = m_ref[0].astype(f32)
    for m in range(1, 8):
        acc = acc + m_ref[m].astype(f32)
    last = jnp.full((8, 128), zi[0], jnp.int32) == 7
    e = acc[40:48] + acc[48:56]
    hi = e.astype(bf16).astype(f32)
    out = jnp.concatenate(
        [acc[0:40], jnp.where(last, hi, acc[40:48]), jnp.where(last, e - hi, acc[48:56])], axis=0
    ).astype(bf16)
    for z in range(8):
        c_ref[z] = out


def join_kernel(a, b, c, d, o_ref):
    for k, ref in enumerate((a, b, c, d)):
        o_ref[k] = ref[...]


LAST = 5


def block_of(yi, xi, ci, n, k):
    c = ci[0] if n < 4 else 1 - ci[0]
    far = n % 4
    y = (yi[0] - jnp.where(c == 1, far, k)) & 3
    x = (xi[0] - jnp.where(c == 1, k, far)) & 3
    return c * 16 + y * 4 + x


def squares(yi, xi, ci, n, src):
    srow = lax.broadcasted_iota(jnp.int32, (8, 128), 0)
    lane = lax.broadcasted_iota(jnp.int32, (8, 128), 1)

    def one(k, total):
        base = block_of(yi, xi, ci, n, k) * BLOCK
        for rb in range(3):
            acc = jnp.zeros((16, 128), f32)
            for t in range(9):
                v = src[k, (rb * 9 + t) * 16 : (rb * 9 + t) * 16 + 16, :].astype(f32)
                acc = acc + v * v
            ok = base + rb * 8 + srow < VALID
            total = total + jnp.where(ok, acc[0:8] + acc[8:16], 0.0)
        e = src[k, 432:448, :].astype(f32)
        e = e[0:8] + e[8:16]
        ok = (base + lane < VALID) & (lane < BLOCK) & (srow == 0)
        return total + jnp.where(ok, e * e, 0.0)

    return one


def squares_kernel(yi, xi, ci, *refs):
    total = jnp.zeros((8, 128), f32)
    for n, src in zip([n for n in range(8) if n != LAST], refs[:7]):
        total = lax.fori_loop(0, 4, squares(yi, xi, ci, n, src), total)
    refs[7][...] = total


def final_kernel(yi, xi, ci, *refs):
    sources = refs[0:8]
    partial, cw_out, bw_out, cb_out, bb_out, loss, w_ref, e_ref, row_ref, sem = refs[8:]
    srow = lax.broadcasted_iota(jnp.int32, (8, 128), 0)
    lane = lax.broadcasted_iota(jnp.int32, (8, 128), 1)
    total = lax.fori_loop(0, 4, squares(yi, xi, ci, LAST, sources[LAST]), partial[...])
    mean = jnp.sum(total) * (1.0 / (VALID * 2305))
    scale = lax.rsqrt(jnp.full((8, 128), mean + NORM_EPS, f32))

    def chunk(block):
        rows = pl.ds(pl.multiple_of(block * BLOCK, 8), BLOCK)
        return pltpu.make_async_copy(w_ref.at[rows], cw_out.at[rows], sem)

    def write(n):
        src = sources[n]

        def one(k, carry):
            block = block_of(yi, xi, ci, n, k)
            e = src[k, 432:448, :].astype(f32)
            e_ref[block] = e[0:8] + e[8:16]
            for rb in range(3):
                row = pl.multiple_of(block * BLOCK + rb * 8, 8)
                for t in range(9):
                    v = src[k, (rb * 9 + t) * 16 : (rb * 9 + t) * 16 + 16, :].astype(f32)
                    w_ref[pl.ds(row, 8), t * 256 : t * 256 + 128] = v[0:8] * scale
                    w_ref[pl.ds(row, 8), t * 256 + 128 : t * 256 + 256] = v[8:16] * scale

            @pl.when(block < 30)
            def _():
                chunk(block).start()

            return carry

        return one

    for n in range(8):
        lax.fori_loop(0, 4, write(n), 0)
    bw_out[...] = w_ref[720:756, :]
    row_ref[...] = jnp.zeros((8, 896), f32)
    for block in range(32):
        tile, off = divmod(block * BLOCK, 128)
        e = e_ref[block] * scale
        e = e if off == 0 else pltpu.roll(e, off, 1)
        here = (lane >= off) & (lane < off + BLOCK)
        row_ref[:, tile * 128 : tile * 128 + 128] = jnp.where(here, e, row_ref[:, tile * 128 : tile * 128 + 128])
        if off + BLOCK > 128:
            past = lane < off + BLOCK - 128
            row_ref[:, tile * 128 + 128 : tile * 128 + 256] = jnp.where(past, e, 0.0)
    cb_out[...] = row_ref[0, 0:720]
    bb_out[...] = pltpu.roll(row_ref[:, 640:768], 128 - 80, 1)[0, 0:36]
    e = jnp.where(srow == 0, e_ref[31], 0.0)
    sums = jnp.sum(jnp.where((lane >= 12) & (lane < 16), e, 0.0))
    count = jnp.sum(jnp.where(lane == 16, e, 0.0))
    loss[...] = jnp.full((1, 128), sums, f32) / jnp.full((1, 128), count, f32)

    def drain(k, carry):
        chunk(k).wait()
        return carry

    lax.fori_loop(0, 30, drain, 0)


VMEM = pl.BlockSpec(memory_space=pltpu.VMEM)
SMEM = pl.BlockSpec(memory_space=pltpu.SMEM)
ANY = pl.BlockSpec(memory_space=pl.ANY)


def near_memory(arrays):
    return [pltpu.with_memory_space_constraint(v, pltpu.VMEM) for v in arrays]


def far_memory(arrays):
    return [pltpu.with_memory_space_constraint(v, pltpu.HBM) for v in arrays]


def shape(*dims, dtype=f32):
    return jax.ShapeDtypeStruct(dims, dtype)


def stage(cw, bw):
    return pl.pallas_call(
        stage_kernel,
        out_shape=pltpu.VMEM((ROWS_ALL, 2304), bf16),
        in_specs=[ANY, VMEM],
        out_specs=VMEM,
        scratch_shapes=[pltpu.SemaphoreType.DMA],
        compiler_params=pltpu.CompilerParams(vmem_limit_bytes=LIMIT),
        name="stage",
    )(*far_memory([cw, bw]))


def head(first, ci, outer, own, inner, w, cb, bb, lab, idx, box):
    return pl.pallas_call(
        head_kernel,
        out_shape=[
            pltpu.HBM((ROWS_ALL, 256), bf16),
            pltpu.HBM((HALF, 256), bf16),
            pltpu.HBM((HALF, 256), bf16),
            pltpu.VMEM((1, 128, 256), bf16),
        ],
        in_specs=[SMEM] * 2 + [VMEM] * 9,
        out_specs=[VMEM] * 4,
        scratch_shapes=[
            pltpu.VMEM((256, 2304), bf16),
            pltpu.VMEM((720, 256), f32),
            pltpu.VMEM((128, 128), f32),
            pltpu.VMEM((128, 128), f32),
            pltpu.VMEM((ROWS_ALL, 256), bf16),
            pltpu.VMEM((16, 768), f32),
            pltpu.VMEM((8, 128), f32),
            pltpu.VMEM((32, 128), jnp.int32),
            pltpu.VMEM((32, 128), jnp.int32),
            pltpu.VMEM((4, 128, 256), bf16),
        ],
        compiler_params=pltpu.CompilerParams(vmem_limit_bytes=LIMIT),
        name="head",
    )(first, ci, *far_memory([outer, own, inner]), *near_memory([w]), *far_memory([cb, bb, lab, idx, box]))


def tower_terms(ci, g, w, after):
    return pl.pallas_call(
        tower_kernel,
        out_shape=(
            pltpu.HBM((2, 128, 256), f32),
            pltpu.VMEM((1, 128, 256), bf16),
            pltpu.VMEM((1, 128, 256), bf16),
            shape(8, 128),
        ),
        in_specs=[SMEM, VMEM, VMEM, ANY],
        out_specs=(VMEM, VMEM, VMEM, VMEM),
        compiler_params=pltpu.CompilerParams(vmem_limit_bytes=LIMIT),
        name="tower_terms",
        cost_estimate=pl.CostEstimate(flops=2 * 756 * 2304 * 256, transcendentals=0, bytes_accessed=4500000),
    )(ci, *far_memory([g]), *near_memory([w]), after)


def tower_end(ci, mid, outer, inner):
    return pl.pallas_call(
        tower_end_kernel,
        out_shape=(shape(1, 2, 128, 256, dtype=bf16), shape(8, 128)),
        in_specs=[SMEM] + [VMEM] * 3,
        out_specs=(VMEM, VMEM),
        compiler_params=pltpu.CompilerParams(vmem_limit_bytes=LIMIT),
        name="tower_end",
    )(ci, *far_memory([mid]), outer, inner)


def weight_terms(yi, xi, ci, keep, got, outer, own, inner, other_edge):
    return pl.pallas_call(
        weight_kernel,
        out_shape=[pltpu.VMEM((4, PIECE, 128), bf16)] * 4 + [shape(8, 128)],
        in_specs=[SMEM] * 3 + [VMEM] * 6,
        out_specs=[VMEM] * 5,
        scratch_shapes=[
            pltpu.VMEM((6, 128, 256), bf16),
            pltpu.VMEM((3, 768, 256), bf16),
            pltpu.VMEM((2, HALF, 256), bf16),
            pltpu.VMEM((16, PIECE, 128), bf16),
        ],
        compiler_params=pltpu.CompilerParams(vmem_limit_bytes=LIMIT),
        name="weight_terms",
    )(yi, xi, ci, *far_memory([keep, got, outer, own, inner]), other_edge)


def row_sum(yi, xi, ci, parts, after):
    return pl.pallas_call(
        row_sum_kernel,
        out_shape=[pltpu.VMEM((PIECE, 128), bf16)] * 4,
        in_specs=[SMEM] * 3 + [VMEM] * 4 + [ANY],
        out_specs=[VMEM] * 4,
        compiler_params=pltpu.CompilerParams(vmem_limit_bytes=LIMIT),
        name="row_sum",
    )(yi, xi, ci, *near_memory(parts), after)


def block_sum(zi, parts):
    return pl.pallas_call(
        block_sum_kernel,
        out_shape=pltpu.VMEM((PIECE, 128), bf16),
        in_specs=[SMEM] + [VMEM] * 4,
        out_specs=VMEM,
        compiler_params=pltpu.CompilerParams(vmem_limit_bytes=LIMIT),
        name="block_sum",
    )(zi, *near_memory(parts))


def piece_sum(zi, m):
    return pl.pallas_call(
        piece_sum_kernel,
        out_shape=pltpu.VMEM((8, 56, 128), bf16),
        in_specs=[SMEM, VMEM],
        out_specs=VMEM,
        compiler_params=pltpu.CompilerParams(vmem_limit_bytes=LIMIT),
        name="piece_sum",
    )(zi, *near_memory([m]))


def join(parts):
    return pl.pallas_call(
        join_kernel,
        out_shape=pltpu.VMEM((4, PIECE, 128), bf16),
        in_specs=[VMEM] * 4,
        out_specs=VMEM,
        compiler_params=pltpu.CompilerParams(vmem_limit_bytes=LIMIT),
        name="join",
    )(*near_memory(parts))


def squares_of(yi, xi, ci, pieces):
    return pl.pallas_call(
        squares_kernel,
        out_shape=pltpu.VMEM((8, 128), f32),
        in_specs=[SMEM] * 3 + [VMEM] * 7,
        out_specs=VMEM,
        compiler_params=pltpu.CompilerParams(vmem_limit_bytes=LIMIT),
        name="squares",
    )(yi, xi, ci, *near_memory(pieces))


def finish(yi, xi, ci, pieces, partial):
    return pl.pallas_call(
        final_kernel,
        out_shape=(shape(720, 2304), shape(36, 2304), shape(720), shape(36), shape(1, 128)),
        in_specs=[SMEM] * 3 + [VMEM] * 9,
        out_specs=(ANY, VMEM, VMEM, VMEM, VMEM),
        scratch_shapes=[
            pltpu.VMEM((ROWS_ALL, 2304), f32),
            pltpu.VMEM((32, 8, 128), f32),
            pltpu.VMEM((8, 896), f32),
            pltpu.SemaphoreType.DMA,
        ],
        compiler_params=pltpu.CompilerParams(vmem_limit_bytes=LIMIT),
        name="finish",
    )(yi, xi, ci, *near_memory([*pieces, partial]))


def swap(value):
    return lax.ppermute(value, "core", [(0, 1), (1, 0)])


def across(value):
    pairs = [(t, t + 1) for t in range(1, 31, 2)]
    return lax.ppermute(value, TILE_AXES, pairs + [(b, a) for a, b in pairs])


def along(value, k, first_axis):
    pairs = []
    for y in range(4):
        for c in range(2):
            for x in range(4):
                dx = k if (first_axis == "x") == (c == 1) else 0
                dy = k - dx
                pairs.append(((y * 2 + c) * 4 + x, (((y + dy) % 4) * 2 + c) * 4 + (x + dx) % 4))
    return lax.ppermute(value, ("y", "core", "x"), pairs)


def per_device(tower, cls_weight, cls_bias, box_weight, box_bias, labels, target_index, boxes):
    own = tower[0]
    outer = across(own)
    inner = swap(own)
    ci = lax.axis_index("core").reshape(1)
    yi = lax.axis_index("y").reshape(1)
    xi = lax.axis_index("x").reshape(1)
    zi = (lax.axis_index("zhi") * 4 + lax.axis_index("zlo")).reshape(1)
    first = (lax.axis_index(TILE_AXES) * 2).reshape(1)

    w = stage(cls_weight, box_weight)
    g, keep, send, edge = head(
        first, ci, outer, own, inner, w, cls_bias, box_bias, labels[0], target_index[0], boxes[0]
    )
    *parts, token = weight_terms(yi, xi, ci, keep, swap(send), outer, own, inner, swap(edge))

    mid, to_outer, to_inner, _ = tower_terms(ci, g, w, token)
    tower_grad, end_token = tower_end(ci, mid, across(to_outer), swap(to_inner))

    parts = [parts[0]] + [along(parts[k], k, "y") for k in (1, 2, 3)]
    parts = row_sum(yi, xi, ci, parts, end_token)
    parts = [parts[0]] + [along(parts[k], k, "x") for k in (1, 2, 3)]
    terms = lax.all_to_all(block_sum(zi, parts).reshape(8, 56, 128), ("zhi", "zlo"), 0, 0, tiled=True)
    copies = lax.all_to_all(piece_sum(zi, terms), ("zhi", "zlo"), 0, 0, tiled=True)
    block = copies.reshape(PIECE, 128)
    row = join([block] + [along(block, k, "x") for k in (1, 2, 3)])
    mine = [row] + [along(row, k, "y") for k in (1, 2, 3)]
    pieces = mine + [swap(v) for v in mine]
    partial = squares_of(yi, xi, ci, pieces[:LAST] + pieces[LAST + 1 :])
    cw_grad, bw_grad, cb_grad, bb_grad, loss = finish(yi, xi, ci, pieces, partial)
    return loss[0, 0], cw_grad, cb_grad, bw_grad, bb_grad, tower_grad


def solution(mesh):
    fine = Mesh(mesh.devices.reshape(4, 4, 2, 4, 2), ("zlo", "y", "core", "x", "zhi"))
    placed = (
        P(IMG_AXES, TILE_AXES, None, None),
        P(),
        P(),
        P(),
        P(),
        P(IMG_AXES, None, TILE_AXES, None),
        P(IMG_AXES, None, TILE_AXES, None),
        P(IMG_AXES, None, None),
    )
    return jax.shard_map(
        per_device,
        mesh=fine,
        in_specs=placed,
        out_specs=(P(), P(), P(), P(), P(), P(IMG_AXES, TILE_AXES, None, None)),
        check_vma=False,
    )
```
